32 devices in a mesh: tok: 8 (over z, y), head: 4 (over x, core).
Axes of the slice: x: 2, y: 2, z: 4, core: 2. Of those that a mesh axis runs over, the one named last changes fastest.
Arguments:
- tokens: bfloat16 [37632, 1024], P(('tok', 'head')), may hold values from -6 to 6
- target_prenorm: bfloat16 [1024], P('tok'), may hold values from 0.25 to 1.75
- target_project: bfloat16 [1024, 3072], P('tok'), may hold values from -0.1875 to 0.1875
- target_outward: bfloat16 [1024, 1024], P('tok'), may hold values from -1.5 to 1.5
- target_midnorm: bfloat16 [1024], P('tok'), may hold values from 0.25 to 1.75
- target_expand: bfloat16 [1024, 4096], P('tok'), may hold values from -0.1875 to 0.1875
- target_shrink: bfloat16 [4096, 1024], P('tok'), may hold values from -0.09375 to 0.09375
- context_prenorm: bfloat16 [1024], P('tok'), may hold values from 0.25 to 1.75
- context_project: bfloat16 [1024, 3072], P('tok'), may hold values from -0.1875 to 0.1875
- context_outward: bfloat16 [1024, 1024], P('tok'), may hold values from -1.5 to 1.5
- context_midnorm: bfloat16 [1024], P('tok'), may hold values from 0.25 to 1.75
- context_expand: bfloat16 [1024, 4096], P('tok'), may hold values from -0.1875 to 0.1875
- context_shrink: bfloat16 [4096, 1024], P('tok'), may hold values from -0.09375 to 0.09375
- predict_entry: bfloat16 [1024, 384], replicated, may hold values from -0.1875 to 0.1875
- mask_token: bfloat16 [384], replicated, may hold values from -6 to 6
- predict_prenorm: bfloat16 [384], replicated, may hold values from 0.25 to 1.75
- predict_project: bfloat16 [384, 1152], replicated, may hold values from -0.3125 to 0.3125
- predict_outward: bfloat16 [384, 384], replicated, may hold values from -1.75 to 1.75
- predict_midnorm: bfloat16 [384], replicated, may hold values from 0.25 to 1.75
- predict_expand: bfloat16 [384, 1536], replicated, may hold values from -0.3125 to 0.3125
- predict_shrink: bfloat16 [1536, 384], replicated, may hold values from -0.15625 to 0.15625
- predict_endnorm: bfloat16 [384], replicated, may hold values from 0.25 to 1.75
- predict_exit: bfloat16 [384, 1024], replicated, may hold values from -0.3125 to 0.3125
- clip_order: int32 [32, 1176], P(('tok', 'head')), may hold values from 0 to 1175, as said below
- visible_count: int32 [32], replicated, may hold values from 128 to 464, as said below
Outputs:
- clip_loss: float32 [32], P(('tok', 'head'))
- tokens_grad: float32 [37632, 1024], P(('tok', 'head'))
- context_prenorm_grad: float32 [1024], P('tok')
- context_project_grad: float32 [1024, 3072], P('tok')
- context_outward_grad: float32 [1024, 1024], P('tok')
- context_midnorm_grad: float32 [1024], P('tok')
- context_expand_grad: float32 [1024, 4096], P('tok')
- context_shrink_grad: float32 [4096, 1024], P('tok')
- predict_entry_grad: float32 [1024, 384], replicated
- mask_token_grad: float32 [384], replicated
- predict_prenorm_grad: float32 [384], replicated
- predict_project_grad: float32 [384, 1152], replicated
- predict_outward_grad: float32 [384, 384], replicated
- predict_midnorm_grad: float32 [384], replicated
- predict_expand_grad: float32 [384, 1536], replicated
- predict_shrink_grad: float32 [1536, 384], replicated
- predict_endnorm_grad: float32 [384], replicated
- predict_exit_grad: float32 [384, 1024], replicated
The draws below stay inside these ranges and needn't reach their ends.
Inputs may be any that keep to these rules, and one draw needn't show every extreme that they name: visible_count[c] is the number of visible tokens of clip c. For every h, the clips c with (c) % 4 == h hold 2368 visible tokens together, and one of them holds exactly 464. `clip_order`: each row is a permutation of the clip's positions: its first visible_count[c] entries are the visible positions in ascending order, the others the hidden positions in ascending order.
All inputs are finite; a program needn't handle non-finite values.
Results may differ from the reference program's by a relative error of at most 0.014.
Values may be sent and summed in bfloat16 or wider, within the bound.
A program may use at most 256 MiB of HBM per device.

```python
import jax
import jax.numpy as jnp
from jax import lax

D = 1024
H = 16
FF = 4096
PD = 384
PH = 12
PFF = 1536
VMOST = 464
MEANV = 296
CLIP_DEV = 1
CLIP = 1176
CLIPS = 32
TOKENS = 37632
N_TOK = 8
N_HEAD = 4


def visible_counts(key):
    folded = jax.random.fold_in(key, 17)
    pair_key, shuffle_key = jax.random.split(folded)
    per_lane = N_TOK * CLIP_DEV
    spread = VMOST - MEANV
    offsets = jax.random.randint(pair_key, (N_HEAD, per_lane // 2), -spread, spread + 1)
    offsets = offsets.at[:, 0].set(spread)
    paired = jnp.stack([MEANV + offsets, MEANV - offsets], axis=2).reshape(N_HEAD, per_lane)
    lane_keys = jax.random.split(shuffle_key, N_HEAD)
    shuffles = jax.vmap(lambda lane_key: jax.random.permutation(lane_key, per_lane))(lane_keys)
    lane_counts = jnp.take_along_axis(paired, shuffles, axis=1)
    return lane_counts.reshape(N_HEAD, N_TOK, CLIP_DEV).transpose(1, 0, 2).reshape(CLIPS).astype(jnp.int32)


def draw_visible_count(key, part):
    return visible_counts(key)


def draw_clip_order(key, part):
    counts = visible_counts(key)
    order_key = jax.random.fold_in(key, 29)

    def one_clip(clip_key, clip_count):
        shuffled = jax.random.permutation(clip_key, CLIP)
        position_rank = jnp.argsort(shuffled)
        places = jnp.arange(CLIP, dtype=jnp.int32)
        sort_keys = jnp.where(position_rank < clip_count, places, CLIP + places)
        return jnp.argsort(sort_keys)
    return jax.vmap(one_clip)(jax.random.split(order_key, CLIPS), counts).astype(jnp.int32)


def levels(key, extent, shards, smallest, largest):
    def one(axis_at, blocks):
        steps = jax.random.uniform(jax.random.fold_in(jax.random.fold_in(key, 6), axis_at), (blocks,), jnp.float32, smallest / len(shards), largest / len(shards))
        return jnp.repeat(jnp.exp(steps), extent[axis_at] // blocks).reshape((-1,) + (1,) * (len(extent) - axis_at - 1))

    gain = one(*shards[0])
    for cut in shards[1:]:
        gain = gain * one(*cut)
    return gain


def scatter_about(key, extent, deviation, limit, pieces=(), kind=jnp.bfloat16):
    array = deviation * jax.random.normal(key, extent, jnp.float32)
    if pieces:
        array = array * levels(key, extent, pieces, -0.22, 0.18)
    return jnp.clip(array, -limit, limit).astype(kind)


def setup_inputs(seed: int = 0) -> dict:
    streams_of = jax.random.split(jax.random.key(seed), 26)
    return {
        "tokens": scatter_about(streams_of[0], (TOKENS, D), 1.0, 6.0, ((0, 32),)),
        "target_prenorm": jnp.clip(1.0 + 0.15 * jax.random.normal(streams_of[1], (D,), jnp.float32), 0.25, 1.75).astype(jnp.bfloat16),
        "target_project": scatter_about(streams_of[2], (D, 3 * D), D ** -0.5, 0.1875, ((0, 8),)),
        "target_outward": scatter_about(streams_of[3], (D, D), (D // 64) ** -0.5, 1.5, ((0, 8),)),
        "target_midnorm": jnp.clip(1.0 + 0.15 * jax.random.normal(streams_of[4], (D,), jnp.float32), 0.25, 1.75).astype(jnp.bfloat16),
        "target_expand": scatter_about(streams_of[5], (D, FF), D ** -0.5, 0.1875, ((0, 8),)),
        "target_shrink": scatter_about(streams_of[6], (FF, D), FF ** -0.5, 0.09375, ((0, 8),)),
        "context_prenorm": jnp.clip(1.0 + 0.15 * jax.random.normal(streams_of[7], (D,), jnp.float32), 0.25, 1.75).astype(jnp.bfloat16),
        "context_project": scatter_about(streams_of[8], (D, 3 * D), D ** -0.5, 0.1875, ((0, 8),)),
        "context_outward": scatter_about(streams_of[9], (D, D), (D // 64) ** -0.5, 1.5, ((0, 8),)),
        "context_midnorm": jnp.clip(1.0 + 0.15 * jax.random.normal(streams_of[10], (D,), jnp.float32), 0.25, 1.75).astype(jnp.bfloat16),
        "context_expand": scatter_about(streams_of[11], (D, FF), D ** -0.5, 0.1875, ((0, 8),)),
        "context_shrink": scatter_about(streams_of[12], (FF, D), FF ** -0.5, 0.09375, ((0, 8),)),
        "predict_entry": scatter_about(streams_of[13], (D, PD), D ** -0.5, 0.1875),
        "mask_token": scatter_about(streams_of[14], (PD,), 1.0, 6.0),
        "predict_prenorm": jnp.clip(1.0 + 0.15 * jax.random.normal(streams_of[15], (PD,), jnp.float32), 0.25, 1.75).astype(jnp.bfloat16),
        "predict_project": scatter_about(streams_of[16], (PD, 3 * PD), PD ** -0.5, 0.3125),
        "predict_outward": scatter_about(streams_of[17], (PD, PD), (PD // 32) ** -0.5, 1.75),
        "predict_midnorm": jnp.clip(1.0 + 0.15 * jax.random.normal(streams_of[18], (PD,), jnp.float32), 0.25, 1.75).astype(jnp.bfloat16),
        "predict_expand": scatter_about(streams_of[19], (PD, PFF), PD ** -0.5, 0.3125),
        "predict_shrink": scatter_about(streams_of[20], (PFF, PD), PFF ** -0.5, 0.15625),
        "predict_endnorm": jnp.clip(1.0 + 0.15 * jax.random.normal(streams_of[21], (PD,), jnp.float32), 0.25, 1.75).astype(jnp.bfloat16),
        "predict_exit": scatter_about(streams_of[22], (PD, D), PD ** -0.5, 0.3125),
        "clip_order": draw_clip_order(jax.random.fold_in(streams_of[25], 71), 0),
        "visible_count": draw_visible_count(jax.random.fold_in(streams_of[25], 71), 0),
    }


@jax.custom_vjp
def low(v):
    return lax.optimization_barrier(v.astype(jnp.bfloat16)).astype(jnp.float32)

@jax.custom_vjp
def low_back(v):
    return v

def low_keep(v):
    return (low(v), None)

def low_pass(kept, grad):
    return (grad,)

def back_keep(v):
    return (v, None)

def back_low(kept, grad):
    return (low(grad),)
low.defvjp(low_keep, low_pass)
low_back.defvjp(back_keep, back_low)
EPSILON = 1e-06
HUBER = 0.25
HIGHEST = lax.Precision.HIGHEST

def layer_norm(values, gains):
    center = values - lax.optimization_barrier(jnp.mean(values, axis=-1, keepdims=True))
    spread = lax.optimization_barrier(jnp.mean(center * center, axis=-1, keepdims=True))
    return center * lax.rsqrt(spread + EPSILON) * gains

def plain_norm(values):
    center = values - lax.optimization_barrier(jnp.mean(values, axis=-1, keepdims=True))
    spread = lax.optimization_barrier(jnp.mean(center * center, axis=-1, keepdims=True))
    return center * lax.rsqrt(spread + EPSILON)

def matmul(former, latter):
    return jnp.dot(former, latter, precision=HIGHEST)

def both_ways(values):
    return low_back(low(values))

def smooth_error(differ):
    magnitude = jnp.abs(differ)
    return jnp.where(magnitude < HUBER, 0.5 * differ * differ / HUBER, magnitude - 0.5 * HUBER)

def positions(length, breadth):
    half_width = breadth // 2
    places = jnp.arange(length, dtype=jnp.float32)[:, None]
    freqs = jnp.exp(-jnp.log(10000.0) * jnp.arange(half_width, dtype=jnp.float32) / half_width)
    angles = places * freqs[None, :]
    return jnp.concatenate([jnp.sin(angles), jnp.cos(angles)], axis=1)

def attention(mixed, head_count, usable):
    length = mixed.shape[0]
    column_span = mixed.shape[1] // 3
    head_size = column_span // head_count
    queries = mixed[:, :column_span].reshape(length, head_count, head_size)
    key_rows = mixed[:, column_span:2 * column_span].reshape(length, head_count, head_size)
    value_rows = mixed[:, 2 * column_span:].reshape(length, head_count, head_size)
    scores = low_back(jnp.einsum('qhd,khd->hqk', queries, key_rows, precision=HIGHEST) * head_size ** (-0.5))
    if usable is not None:
        scores = jnp.where(usable[None, None, :], scores, -1e+30)
    shares = low(jax.nn.softmax(scores, axis=-1))
    return jnp.einsum('hqk,khd->qhd', shares, value_rows, precision=HIGHEST).reshape(length, column_span)

def target_layer(clip_tokens, weights):
    prenorm, project, outward, midnorm, expand, shrink = weights
    normed = low(layer_norm(clip_tokens, prenorm))
    mixed = low(matmul(normed, project))
    attended = low(attention(mixed, H, None))
    middle = clip_tokens + matmul(attended, outward)
    active = low(jax.nn.gelu(matmul(low(layer_norm(middle, midnorm)), expand)))
    return plain_norm(middle + matmul(active, shrink))

def clip_forward(clip_tokens, clip_rows, clip_count, clip_target, params):
    context_prenorm, context_project, context_outward, context_midnorm, context_expand, context_shrink, predict_entry, mask_token, predict_prenorm, predict_project, predict_outward, predict_midnorm, predict_expand, predict_shrink, predict_endnorm, predict_exit = params
    slot_index = jnp.arange(VMOST, dtype=jnp.int32)
    live_slots = slot_index < clip_count
    seen = clip_tokens[clip_rows[:VMOST]]
    normed = low(layer_norm(seen, context_prenorm))
    mixed = both_ways(matmul(normed, context_project))
    attended = both_ways(attention(mixed, H, live_slots))
    middle = both_ways(seen + low_back(matmul(attended, context_outward)))
    raised = low_back(matmul(low(layer_norm(middle, context_midnorm)), context_expand))
    active = low(jax.nn.gelu(raised))
    context_out = both_ways(middle + low_back(matmul(active, context_shrink)))
    entry = low_back(matmul(context_out, predict_entry))
    order_rank = jnp.argsort(clip_rows).astype(jnp.int32)
    visible = order_rank < clip_count
    placed = entry[jnp.minimum(order_rank, VMOST - 1)]
    start = jnp.where(visible[:, None], placed, mask_token[None, :]) + positions(CLIP, PD)
    predict_in = low(layer_norm(start, predict_prenorm))
    predict_mixed = both_ways(matmul(predict_in, predict_project))
    predict_attn = both_ways(attention(predict_mixed, PH, None))
    branch = start + low_back(matmul(predict_attn, predict_outward))
    predict_raised = low_back(matmul(low(layer_norm(branch, predict_midnorm)), predict_expand))
    predict_active = low(jax.nn.gelu(predict_raised))
    final = branch + low_back(matmul(predict_active, predict_shrink))
    final_in = low(layer_norm(final, predict_endnorm))
    predicted = low_back(matmul(final_in, predict_exit))
    row_error = lax.optimization_barrier(jnp.mean(smooth_error(predicted - clip_target), axis=-1))
    clip_sum = jnp.sum(jnp.where(visible, 0.0, row_error))
    return (clip_sum, clip_sum / (CLIP - clip_count).astype(jnp.float32))

def reference(tokens, target_prenorm, target_project, target_outward, target_midnorm, target_expand, target_shrink, context_prenorm, context_project, context_outward, context_midnorm, context_expand, context_shrink, predict_entry, mask_token, predict_prenorm, predict_project, predict_outward, predict_midnorm, predict_expand, predict_shrink, predict_endnorm, predict_exit, clip_order, visible_count):
    token_clips = tokens.astype(jnp.float32).reshape(CLIPS, CLIP, D)
    target_weights = tuple((weight.astype(jnp.float32) for weight in (target_prenorm, target_project, target_outward, target_midnorm, target_expand, target_shrink)))
    targets = lax.map(lambda clip_tokens: target_layer(clip_tokens, target_weights), token_clips)
    params = tuple((weight.astype(jnp.float32) for weight in (context_prenorm, context_project, context_outward, context_midnorm, context_expand, context_shrink, predict_entry, mask_token, predict_prenorm, predict_project, predict_outward, predict_midnorm, predict_expand, predict_shrink, predict_endnorm, predict_exit)))

    def objective(clip_values, weights):

        def one_clip(member):
            clip_tokens, clip_rows, clip_count, clip_target = member
            return jax.checkpoint(clip_forward)(clip_tokens, clip_rows, clip_count, clip_target, weights)
        clip_sums, clip_losses = lax.map(one_clip, (clip_values, clip_order, visible_count, targets))
        return (jnp.sum(clip_sums), clip_losses)
    unused, pullback, clip_losses = jax.vjp(objective, token_clips, params, has_aux=True)
    token_grads, param_grads = pullback(jnp.ones((), jnp.float32))
    return (clip_losses, token_grads.reshape(TOKENS, D), param_grads[0], param_grads[1], param_grads[2], param_grads[3], param_grads[4], param_grads[5], param_grads[6], param_grads[7], param_grads[8], param_grads[9], param_grads[10], param_grads[11], param_grads[12], param_grads[13], param_grads[14], param_grads[15])
```

```python
import functools

import jax
import jax.numpy as jnp
from jax import lax
from jax.experimental import pallas as pl
from jax.experimental.pallas import tpu as pltpu
from jax.sharding import PartitionSpec as P

H = 16
PD = 384
PH = 12
VMOST = 464


EPSILON = 1e-06
HUBER = 0.25


def layer_norm(values, gains):
    center = values - jnp.mean(values, axis=-1, keepdims=True)
    spread = jnp.mean(center * center, axis=-1, keepdims=True)
    return center * lax.rsqrt(spread + EPSILON) * gains


def plain_norm(values):
    center = values - jnp.mean(values, axis=-1, keepdims=True)
    spread = jnp.mean(center * center, axis=-1, keepdims=True)
    return center * lax.rsqrt(spread + EPSILON)


def smooth_error(differ):
    magnitude = jnp.abs(differ)
    return jnp.where(magnitude < HUBER, 0.5 * differ * differ / HUBER, magnitude - 0.5 * HUBER)


def positions(length, breadth):
    half_width = breadth // 2
    places = jnp.arange(length, dtype=jnp.float32)[:, None]
    freqs = jnp.exp(-jnp.log(10000.0) * jnp.arange(half_width, dtype=jnp.float32) / half_width)
    angles = places * freqs[None, :]
    return jnp.concatenate([jnp.sin(angles), jnp.cos(angles)], axis=1)


def product(former, latter):
    return jnp.dot(former, latter, preferred_element_type=jnp.float32)


def inner_rows(former, latter):
    return lax.dot_general(
        former, latter, (((0,), (0,)), ((), ())), preferred_element_type=jnp.float32
    )


def inner_cols(former, latter):
    return lax.dot_general(
        former, latter, (((1,), (1,)), ((), ())), preferred_element_type=jnp.float32
    )


BF=jnp.bfloat16; F32=jnp.float32
LOG2E=1.4426950408889634
NT=(((1,),(1,)),((),())); NN=(((1,),(0,)),((),()))
def dot(a,b,dims=NN): return lax.dot_general(a,b,dims,preferred_element_type=F32)
def chunks(n,step):
    return [(i,min(step,n-i)) for i in range(0,n,step)]
def lane_mask(rows,h,e):
    lane=lax.broadcasted_iota(jnp.int32,(rows,128),1)
    return (lane>=h*e)&(lane<(h+1)*e)
def head_rows(values,h,e):
    return jnp.where(lane_mask(values.shape[0],h,e),values,jnp.zeros_like(values))

def fwd_kernel(e,step,masked,want_lse,*refs):
    refs=list(refs)
    count=refs.pop(0) if masked else None
    q_ref,k_ref,v_ref,o_ref=refs[:4]
    lse_ref=refs[4] if want_lse else None
    L=q_ref.shape[0]; per=128//e; c=e**-0.5*LOG2E
    k=k_ref[...]
    vt=v_ref[...].T
    live=None
    if masked:
        live=lax.broadcasted_iota(jnp.int32,(L,1),0)<count[0]
    for (s0,n) in chunks(L,step):
        outs=[]; lses=[]
        for h in range(per):
            q=head_rows(q_ref[s0:s0+n,:],h,e)
            st=dot(k,q,NT)
            if masked: st=jnp.where(live,st,-1e30)
            m=jnp.max(st,axis=0,keepdims=True)
            p=jnp.exp2((st-m)*c)
            l=jnp.sum(p,axis=0,keepdims=True)
            o=dot(vt[h*e:(h+1)*e,:],p.astype(BF))
            outs.append(o*(1.0/l))
            if want_lse: lses.append(m*c+jnp.log2(l))
        o_ref[s0:s0+n,:]=jnp.concatenate(outs,axis=0).T.astype(BF)
        if want_lse: lse_ref[0,:,s0:s0+n]=jnp.concatenate(lses,axis=0)

def attn_fwd(mixed,heads,count=None,step=1280,want_lse=True):
    L,w3=mixed.shape; Dm=w3//3; e=Dm//heads; G=Dm//128; per=128//e
    masked=count is not None
    spec=lambda off: pl.BlockSpec((L,128),lambda g,*_:(0,off+g))
    out_shape=[jax.ShapeDtypeStruct((L,Dm),BF)]; out_specs=[pl.BlockSpec((L,128),lambda g,*_:(0,g))]
    if want_lse:
        out_shape.append(jax.ShapeDtypeStruct((G,per,L),F32)); out_specs.append(pl.BlockSpec((1,per,L),lambda g,*_:(g,0,0)))
    gs=pltpu.PrefetchScalarGridSpec(num_scalar_prefetch=1 if masked else 0,grid=(G,),in_specs=[spec(0),spec(G),spec(2*G)],out_specs=out_specs)
    flops=4*heads*L*L*e
    f=pl.pallas_call(functools.partial(fwd_kernel,e,step,masked,want_lse),grid_spec=gs,out_shape=out_shape,
        compiler_params=pltpu.CompilerParams(vmem_limit_bytes=56<<20),
        cost_estimate=pl.CostEstimate(flops=flops,bytes_accessed=L*Dm*8,transcendentals=heads*L*L),name="attn_fwd")
    return f(*((count,) if masked else ()),mixed,mixed,mixed)

def bwd_kernel(e,step,masked,*refs):
    refs=list(refs)
    count=refs.pop(0) if masked else None
    q_ref,k_ref,v_ref,o_ref,do_ref,lse_ref,g_ref,dk_ref,dv_ref=refs
    L=q_ref.shape[0]; per=128//e; c=e**-0.5*LOG2E; f=e**-0.5
    g=pl.program_id(0); G=pl.num_programs(0)
    k=k_ref[...]; v=v_ref[...]
    kt=k.T
    live=None
    if masked:
        live=lax.broadcasted_iota(jnp.int32,(L,1),0)<count[0]
    dk_ref[...]=jnp.zeros_like(dk_ref); dv_ref[...]=jnp.zeros_like(dv_ref)
    cols=lambda part: pl.ds(pl.multiple_of((part*G+g)*128,128),128)
    for (s0,n) in chunks(L,step):
        do_all=do_ref[s0:s0+n,:]; q_all=q_ref[s0:s0+n,:]
        prod=(do_all.astype(F32)*o_ref[s0:s0+n,:].astype(F32)).T
        dqs=[]
        for h in range(per):
            q=head_rows(q_all,h,e); do=head_rows(do_all,h,e)
            delta=jnp.sum(prod[h*e:(h+1)*e,:],axis=0,keepdims=True)
            st=dot(k,q,NT)
            p=jnp.exp2(st*c-lse_ref[0,h:h+1,s0:s0+n])
            if masked: p=jnp.where(live,p,0.0)
            dp=dot(v,do,NT)
            ds=(p*(dp-delta)).astype(BF)
            dv_ref[...]+=dot(p.astype(BF),do)
            dk_ref[...]+=dot(ds,q)
            dqs.append(dot(kt[h*e:(h+1)*e,:],ds))
        g_ref[s0:s0+n,cols(0)]=(jnp.concatenate(dqs,axis=0)*f).T.astype(BF)
    g_ref[:,cols(1)]=(dk_ref[...]*f).astype(BF)
    g_ref[:,cols(2)]=dv_ref[...].astype(BF)

def attn_bwd(mixed,o,lse,do,heads,count=None,step=256):
    L,w3=mixed.shape; Dm=w3//3; e=Dm//heads; G=Dm//128; per=128//e
    masked=count is not None
    spec=lambda off: pl.BlockSpec((L,128),lambda g,*_:(0,off+g))
    gs=pltpu.PrefetchScalarGridSpec(num_scalar_prefetch=1 if masked else 0,grid=(G,),
        in_specs=[spec(0),spec(G),spec(2*G),spec(0),spec(0),pl.BlockSpec((1,per,L),lambda g,*_:(g,0,0))],
        out_specs=pl.BlockSpec((L,w3),lambda g,*_:(0,0)),
        scratch_shapes=[pltpu.VMEM((L,128),F32)]*2)
    return pl.pallas_call(functools.partial(bwd_kernel,e,step,masked),grid_spec=gs,out_shape=jax.ShapeDtypeStruct((L,w3),BF),
        compiler_params=pltpu.CompilerParams(vmem_limit_bytes=56<<20),
        cost_estimate=pl.CostEstimate(flops=10*heads*L*L*e,bytes_accessed=L*Dm*16,transcendentals=heads*L*L),name="attn_bwd")(*((count,) if masked else ()),mixed,mixed,mixed,o,do,lse)


def feed_forward(mid_rows, midnorm, expand, shrink):
    mid_wide = mid_rows.astype(jnp.float32)
    normed = layer_norm(mid_wide, midnorm).astype(jnp.bfloat16)
    raised = product(normed, expand)
    active = jax.nn.gelu(raised).astype(jnp.bfloat16)
    output = (mid_wide + product(active, shrink)).astype(jnp.bfloat16)
    return (output, (mid_wide, normed, raised, active))


def feed_forward_back(grad_rows, saved, midnorm, expand, shrink):
    mid_wide, normed, raised, active = saved
    grad_shrink = inner_rows(active, grad_rows)
    grad_active = inner_cols(grad_rows, shrink)
    unused, gelu_pullback = jax.vjp(jax.nn.gelu, raised)
    grad_raised = gelu_pullback(grad_active)[0].astype(jnp.bfloat16)
    grad_expand = inner_rows(normed, grad_raised)
    grad_normed = inner_cols(grad_raised, expand)
    unused, norm_pullback = jax.vjp(layer_norm, mid_wide, midnorm)
    grad_mid, grad_midnorm = norm_pullback(grad_normed)
    grad_total = (grad_rows.astype(jnp.float32) + grad_mid).astype(jnp.bfloat16)
    return (grad_total, (grad_midnorm, grad_expand, grad_shrink))


def shards(
    tokens,
    target_prenorm,
    target_project,
    target_outward,
    target_midnorm,
    target_expand,
    target_shrink,
    context_prenorm,
    context_project,
    context_outward,
    context_midnorm,
    context_expand,
    context_shrink,
    predict_entry,
    mask_token,
    predict_prenorm,
    predict_project,
    predict_outward,
    predict_midnorm,
    predict_expand,
    predict_shrink,
    predict_endnorm,
    predict_exit,
    clip_order,
    visible_count,
):
    clips_here = clip_order.shape[0]
    clip_len = clip_order.shape[1]
    model_width = tokens.shape[1]
    head_devices = lax.axis_size("head")
    lane_index = lax.axis_index("tok")
    head_index = lax.axis_index("head")
    device_index = lane_index * head_devices + head_index
    counts_here = lax.dynamic_slice_in_dim(visible_count, device_index * clips_here, clips_here)
    gathered = (
        lax.all_gather(target_prenorm, "tok", axis=0, tiled=True),
        lax.all_gather(target_project, "tok", axis=0, tiled=True),
        lax.all_gather(target_outward, "tok", axis=0, tiled=True),
        lax.all_gather(target_midnorm, "tok", axis=0, tiled=True),
        lax.all_gather(target_expand, "tok", axis=0, tiled=True),
        lax.all_gather(target_shrink, "tok", axis=0, tiled=True),
        lax.all_gather(context_prenorm, "tok", axis=0, tiled=True),
        lax.all_gather(context_project, "tok", axis=0, tiled=True),
        lax.all_gather(context_outward, "tok", axis=0, tiled=True),
        lax.all_gather(context_midnorm, "tok", axis=0, tiled=True),
        lax.all_gather(context_expand, "tok", axis=0, tiled=True),
        lax.all_gather(context_shrink, "tok", axis=0, tiled=True),
    )
    (
        tgt_prenorm_full,
        tgt_project_full,
        tgt_outward_full,
        tgt_midnorm_full,
        tgt_expand_full,
        tgt_shrink_full,
    ) = gathered[:6]
    (
        ctx_prenorm_full,
        ctx_project_full,
        ctx_outward_full,
        ctx_midnorm_full,
        ctx_expand_full,
        ctx_shrink_full,
    ) = gathered[6:]
    tokens_wide = tokens.astype(jnp.float32)
    target_in = layer_norm(tokens_wide, tgt_prenorm_full.astype(jnp.float32)).astype(jnp.bfloat16)
    target_mixed = product(target_in, tgt_project_full).astype(jnp.bfloat16)
    target_attn = attn_fwd(target_mixed, H, want_lse=False)[0]
    target_mid = tokens_wide + product(target_attn, tgt_outward_full)
    target_normed = layer_norm(target_mid, tgt_midnorm_full.astype(jnp.float32)).astype(
        jnp.bfloat16
    )
    target_active = jax.nn.gelu(product(target_normed, tgt_expand_full)).astype(jnp.bfloat16)
    target_out = plain_norm(target_mid + product(target_active, tgt_shrink_full))
    order_rank = jnp.argsort(clip_order, axis=1)
    visible = order_rank < counts_here[:, None]
    visible_pos = clip_order[:, :VMOST]
    slot_live = jnp.arange(VMOST, dtype=jnp.int32)[None, :] < counts_here[:, None]
    token_grid = tokens.reshape(clips_here, clip_len, model_width)
    seen_rows = jnp.take_along_axis(token_grid, visible_pos[:, :, None], axis=1)
    seen_rows = seen_rows.reshape(clips_here * VMOST, model_width).astype(jnp.float32)
    ctx_prenorm_wide = ctx_prenorm_full.astype(jnp.float32)
    ctx_midnorm_wide = ctx_midnorm_full.astype(jnp.float32)
    context_in = layer_norm(seen_rows, ctx_prenorm_wide).astype(jnp.bfloat16)
    context_mixed = product(context_in, ctx_project_full).astype(jnp.bfloat16)
    context_attn, context_lse = attn_fwd(context_mixed, H, counts_here)
    context_mid = (seen_rows + product(context_attn, ctx_outward_full)).astype(jnp.bfloat16)
    context_out, ffn_saved = feed_forward(
        context_mid, ctx_midnorm_wide, ctx_expand_full, ctx_shrink_full
    )
    entry_rows = product(context_out, predict_entry).reshape(clips_here, VMOST, -1)
    placed = jnp.take_along_axis(entry_rows, jnp.minimum(order_rank, VMOST - 1)[:, :, None], axis=1)
    start_rows = jnp.where(
        visible[:, :, None], placed, mask_token.astype(jnp.float32)[None, None, :]
    )
    start_rows = (start_rows + positions(clip_len, PD)[None]).reshape(clips_here * clip_len, PD)
    pred_prenorm_wide = predict_prenorm.astype(jnp.float32)
    pred_midnorm_wide = predict_midnorm.astype(jnp.float32)
    pred_endnorm_wide = predict_endnorm.astype(jnp.float32)
    predict_in = layer_norm(start_rows, pred_prenorm_wide).astype(jnp.bfloat16)
    predict_mixed = product(predict_in, predict_project).astype(jnp.bfloat16)
    predict_attn, predict_lse = attn_fwd(predict_mixed, PH)
    branch_rows = start_rows + product(predict_attn, predict_outward)
    predict_normed = layer_norm(branch_rows, pred_midnorm_wide).astype(jnp.bfloat16)
    predict_raised = product(predict_normed, predict_expand)
    predict_active = jax.nn.gelu(predict_raised).astype(jnp.bfloat16)
    final_rows = branch_rows + product(predict_active, predict_shrink)
    final_in = layer_norm(final_rows, pred_endnorm_wide).astype(jnp.bfloat16)
    predicted = product(final_in, predict_exit)
    differ = predicted - target_out
    hidden_rows = jnp.logical_not(visible).reshape(-1)
    row_error = jnp.mean(smooth_error(differ), axis=1)
    clip_sums = jnp.sum(
        jnp.where(hidden_rows, row_error, 0.0).reshape(clips_here, clip_len), axis=1
    )
    clip_loss = clip_sums / (clip_len - counts_here).astype(jnp.float32)
    slope = jnp.clip(differ / HUBER, -1.0, 1.0)
    grad_predicted = (jnp.where(hidden_rows[:, None], slope, 0.0) / model_width).astype(
        jnp.bfloat16
    )
    grad_exit = inner_rows(final_in, grad_predicted)
    grad_final_in = inner_cols(grad_predicted, predict_exit)
    unused, norm_pullback = jax.vjp(layer_norm, final_rows, pred_endnorm_wide)
    grad_final, grad_endnorm = norm_pullback(grad_final_in)
    grad_second = grad_final.astype(jnp.bfloat16)
    grad_pred_shrink = inner_rows(predict_active, grad_second)
    grad_pred_active = inner_cols(grad_second, predict_shrink)
    unused, gelu_pullback = jax.vjp(jax.nn.gelu, predict_raised)
    grad_pred_raised = gelu_pullback(grad_pred_active)[0].astype(jnp.bfloat16)
    grad_pred_expand = inner_rows(predict_normed, grad_pred_raised)
    grad_pred_normed = inner_cols(grad_pred_raised, predict_expand)
    unused, norm_pullback = jax.vjp(layer_norm, branch_rows, pred_midnorm_wide)
    grad_branch_norm, grad_pred_midnorm = norm_pullback(grad_pred_normed)
    grad_branch = grad_final + grad_branch_norm
    grad_first = grad_branch.astype(jnp.bfloat16)
    grad_pred_outward = inner_rows(predict_attn, grad_first)
    grad_pred_attn = inner_cols(grad_first, predict_outward).astype(jnp.bfloat16)
    grad_pred_mixed = attn_bwd(predict_mixed, predict_attn, predict_lse, grad_pred_attn, PH)
    grad_pred_project = inner_rows(predict_in, grad_pred_mixed)
    grad_pred_in = inner_cols(grad_pred_mixed, predict_project)
    unused, norm_pullback = jax.vjp(layer_norm, start_rows, pred_prenorm_wide)
    grad_start_norm, grad_pred_prenorm = norm_pullback(grad_pred_in)
    grad_start = (grad_branch + grad_start_norm).reshape(clips_here, clip_len, PD)
    grad_mask = jnp.sum(jnp.where(visible[:, :, None], 0.0, grad_start), axis=(0, 1))
    grad_entry_rows = jnp.take_along_axis(grad_start, visible_pos[:, :, None], axis=1)
    grad_entry_rows = jnp.where(slot_live[:, :, None], grad_entry_rows, 0.0)
    grad_entry_rows = grad_entry_rows.reshape(clips_here * VMOST, PD).astype(jnp.bfloat16)
    grad_entry = inner_rows(context_out, grad_entry_rows)
    grad_context_out = inner_cols(grad_entry_rows, predict_entry).astype(jnp.bfloat16)
    refetched = (
        lax.all_gather(context_prenorm, "tok", axis=0, tiled=True),
        lax.all_gather(context_project, "tok", axis=0, tiled=True),
        lax.all_gather(context_outward, "tok", axis=0, tiled=True),
        lax.all_gather(context_midnorm, "tok", axis=0, tiled=True),
        lax.all_gather(context_expand, "tok", axis=0, tiled=True),
        lax.all_gather(context_shrink, "tok", axis=0, tiled=True),
    )
    back_prenorm, back_project, back_outward, back_midnorm, back_expand, back_shrink = refetched
    back_prenorm_wide = back_prenorm.astype(jnp.float32)
    back_midnorm_wide = back_midnorm.astype(jnp.float32)
    grad_mid, ffn_grads = feed_forward_back(
        grad_context_out, ffn_saved, back_midnorm_wide, back_expand, back_shrink
    )
    grad_ctx_outward = inner_rows(context_attn, grad_mid)
    grad_ctx_attn = inner_cols(grad_mid, back_outward).astype(jnp.bfloat16)
    grad_ctx_mixed = attn_bwd(
        context_mixed, context_attn, context_lse, grad_ctx_attn, H, counts_here
    )
    grad_ctx_project = inner_rows(context_in, grad_ctx_mixed)
    grad_ctx_in = inner_cols(grad_ctx_mixed, back_project)
    unused, norm_pullback = jax.vjp(layer_norm, seen_rows, back_prenorm_wide)
    grad_seen_norm, grad_ctx_prenorm = norm_pullback(grad_ctx_in)
    grad_seen = (grad_mid.astype(jnp.float32) + grad_seen_norm).reshape(
        clips_here, VMOST, model_width
    )
    grad_grid = jnp.take_along_axis(
        grad_seen, jnp.minimum(order_rank, VMOST - 1)[:, :, None], axis=1
    )
    tokens_grad = jnp.where(visible[:, :, None], grad_grid, 0.0).reshape(
        clips_here * clip_len, model_width
    )
    lane_parts = (
        lax.psum_scatter(grad_ctx_prenorm, "tok", scatter_dimension=0, tiled=True),
        lax.psum_scatter(grad_ctx_project, "tok", scatter_dimension=0, tiled=True),
        lax.psum_scatter(grad_ctx_outward, "tok", scatter_dimension=0, tiled=True),
        lax.psum_scatter(ffn_grads[0], "tok", scatter_dimension=0, tiled=True),
        lax.psum_scatter(ffn_grads[1], "tok", scatter_dimension=0, tiled=True),
        lax.psum_scatter(ffn_grads[2], "tok", scatter_dimension=0, tiled=True),
    )
    context_sums = (
        lax.psum(lane_parts[0].astype(jnp.bfloat16), "head").astype(jnp.float32),
        lax.psum(lane_parts[1].astype(jnp.bfloat16), "head").astype(jnp.float32),
        lax.psum(lane_parts[2].astype(jnp.bfloat16), "head").astype(jnp.float32),
        lax.psum(lane_parts[3].astype(jnp.bfloat16), "head").astype(jnp.float32),
        lax.psum(lane_parts[4].astype(jnp.bfloat16), "head").astype(jnp.float32),
        lax.psum(lane_parts[5].astype(jnp.bfloat16), "head").astype(jnp.float32),
    )
    predict_sums = lax.psum(
        (
            grad_entry,
            grad_mask,
            grad_pred_prenorm,
            grad_pred_project,
            grad_pred_outward,
            grad_pred_midnorm,
            grad_pred_expand,
            grad_pred_shrink,
            grad_endnorm,
            grad_exit,
        ),
        ("tok", "head"),
    )
    return (
        clip_loss,
        tokens_grad,
        context_sums[0],
        context_sums[1],
        context_sums[2],
        context_sums[3],
        context_sums[4],
        context_sums[5],
        predict_sums[0],
        predict_sums[1],
        predict_sums[2],
        predict_sums[3],
        predict_sums[4],
        predict_sums[5],
        predict_sums[6],
        predict_sums[7],
        predict_sums[8],
        predict_sums[9],
    )


def solution(mesh):
    return jax.shard_map(
        shards,
        mesh=mesh,
        in_specs=(
            P(("tok", "head"), None),
            P("tok"),
            P("tok", None),
            P("tok", None),
            P("tok"),
            P("tok", None),
            P("tok", None),
            P("tok"),
            P("tok", None),
            P("tok", None),
            P("tok"),
            P("tok", None),
            P("tok", None),
            P(),
            P(),
            P(),
            P(),
            P(),
            P(),
            P(),
            P(),
            P(),
            P(),
            P(("tok", "head"), None),
            P(),
        ),
        out_specs=(
            P(("tok", "head")),
            P(("tok", "head"), None),
            P("tok"),
            P("tok", None),
            P("tok", None),
            P("tok"),
            P("tok", None),
            P("tok", None),
            P(),
            P(),
            P(),
            P(),
            P(),
            P(),
            P(),
            P(),
            P(),
            P(),
        ),
        check_vma=False,
    )
```

```python
import functools

import jax
import jax.numpy as jnp
from jax import lax
from jax.experimental import pallas as pl
from jax.experimental.pallas import tpu as pltpu
from jax.sharding import PartitionSpec as P

H = 16
PD = 384
PH = 12
VMOST = 464


EPSILON = 1e-06
HUBER = 0.25


def layer_norm(values, gains):
    center = values - jnp.mean(values, axis=-1, keepdims=True)
    spread = jnp.mean(center * center, axis=-1, keepdims=True)
    return center * lax.rsqrt(spread + EPSILON) * gains


def plain_norm(values):
    center = values - jnp.mean(values, axis=-1, keepdims=True)
    spread = jnp.mean(center * center, axis=-1, keepdims=True)
    return center * lax.rsqrt(spread + EPSILON)


def smooth_error(differ):
    magnitude = jnp.abs(differ)
    return jnp.where(magnitude < HUBER, 0.5 * differ * differ / HUBER, magnitude - 0.5 * HUBER)


def positions(length, breadth):
    half_width = breadth // 2
    places = jnp.arange(length, dtype=jnp.float32)[:, None]
    freqs = jnp.exp(-jnp.log(10000.0) * jnp.arange(half_width, dtype=jnp.float32) / half_width)
    angles = places * freqs[None, :]
    return jnp.concatenate([jnp.sin(angles), jnp.cos(angles)], axis=1)


def product(former, latter):
    return jnp.dot(former, latter, preferred_element_type=jnp.float32)


def inner_rows(former, latter):
    return lax.dot_general(
        former, latter, (((0,), (0,)), ((), ())), preferred_element_type=jnp.float32
    )


def inner_cols(former, latter):
    return lax.dot_general(
        former, latter, (((1,), (1,)), ((), ())), preferred_element_type=jnp.float32
    )


BF=jnp.bfloat16; F32=jnp.float32
LOG2E=1.4426950408889634
NT=(((1,),(1,)),((),())); NN=(((1,),(0,)),((),()))
def dot(a,b,dims=NN): return lax.dot_general(a,b,dims,preferred_element_type=F32)
def chunks(n,step):
    return [(i,min(step,n-i)) for i in range(0,n,step)]
def lane_mask(rows,h,e):
    lane=lax.broadcasted_iota(jnp.int32,(rows,128),1)
    return (lane>=h*e)&(lane<(h+1)*e)
def head_rows(values,h,e):
    return jnp.where(lane_mask(values.shape[0],h,e),values,jnp.zeros_like(values))

def fwd_kernel(e,step,masked,want_lse,*refs):
    refs=list(refs)
    count=refs.pop(0) if masked else None
    q_ref,k_ref,v_ref,o_ref=refs[:4]
    lse_ref=refs[4] if want_lse else None
    L=q_ref.shape[0]; per=128//e; c=e**-0.5*LOG2E
    k=k_ref[...]
    vt=v_ref[...].T
    live=None
    if masked:
        live=lax.broadcasted_iota(jnp.int32,(L,1),0)<count[0]
    for (s0,n) in chunks(L,step):
        outs=[]; lses=[]
        for h in range(per):
            q=head_rows(q_ref[s0:s0+n,:],h,e)
            st=dot(k,q,NT)
            if masked: st=jnp.where(live,st,-1e30)
            m=jnp.max(st,axis=0,keepdims=True)
            p=jnp.exp2((st-m)*c)
            l=jnp.sum(p,axis=0,keepdims=True)
            o=dot(vt[h*e:(h+1)*e,:],p.astype(BF))
            outs.append(o*(1.0/l))
            if want_lse: lses.append(m*c+jnp.log2(l))
        o_ref[s0:s0+n,:]=jnp.concatenate(outs,axis=0).T.astype(BF)
        if want_lse: lse_ref[0,:,s0:s0+n]=jnp.concatenate(lses,axis=0)

def attn_fwd(mixed,heads,count=None,step=1280,want_lse=True):
    L,w3=mixed.shape; Dm=w3//3; e=Dm//heads; G=Dm//128; per=128//e
    masked=count is not None
    spec=lambda off: pl.BlockSpec((L,128),lambda g,*_:(0,off+g))
    out_shape=[jax.ShapeDtypeStruct((L,Dm),BF)]; out_specs=[pl.BlockSpec((L,128),lambda g,*_:(0,g))]
    if want_lse:
        out_shape.append(jax.ShapeDtypeStruct((G,per,L),F32)); out_specs.append(pl.BlockSpec((1,per,L),lambda g,*_:(g,0,0)))
    gs=pltpu.PrefetchScalarGridSpec(num_scalar_prefetch=1 if masked else 0,grid=(G,),in_specs=[spec(0),spec(G),spec(2*G)],out_specs=out_specs)
    flops=4*heads*L*L*e
    f=pl.pallas_call(functools.partial(fwd_kernel,e,step,masked,want_lse),grid_spec=gs,out_shape=out_shape,
        compiler_params=pltpu.CompilerParams(vmem_limit_bytes=56<<20),
        cost_estimate=pl.CostEstimate(flops=flops,bytes_accessed=L*Dm*8,transcendentals=heads*L*L),name="attn_fwd")
    return f(*((count,) if masked else ()),mixed,mixed,mixed)

def bwd_kernel(e,step,masked,*refs):
    refs=list(refs)
    count=refs.pop(0) if masked else None
    q_ref,k_ref,v_ref,o_ref,do_ref,lse_ref,g_ref,dk_ref,dv_ref=refs
    L=q_ref.shape[0]; per=128//e; c=e**-0.5*LOG2E; f=e**-0.5
    g=pl.program_id(0); G=pl.num_programs(0)
    k=k_ref[...]; v=v_ref[...]
    kt=k.T
    live=None
    if masked:
        live=lax.broadcasted_iota(jnp.int32,(L,1),0)<count[0]
    dk_ref[...]=jnp.zeros_like(dk_ref); dv_ref[...]=jnp.zeros_like(dv_ref)
    cols=lambda part: pl.ds(pl.multiple_of((part*G+g)*128,128),128)
    for (s0,n) in chunks(L,step):
        do_all=do_ref[s0:s0+n,:]; q_all=q_ref[s0:s0+n,:]
        prod=(do_all.astype(F32)*o_ref[s0:s0+n,:].astype(F32)).T
        dqs=[]
        for h in range(per):
            q=head_rows(q_all,h,e); do=head_rows(do_all,h,e)
            delta=jnp.sum(prod[h*e:(h+1)*e,:],axis=0,keepdims=True)
            st=dot(k,q,NT)
            p=jnp.exp2(st*c-lse_ref[0,h:h+1,s0:s0+n])
            if masked: p=jnp.where(live,p,0.0)
            dp=dot(v,do,NT)
            ds=(p*(dp-delta)).astype(BF)
            dv_ref[...]+=dot(p.astype(BF),do)
            dk_ref[...]+=dot(ds,q)
            dqs.append(dot(kt[h*e:(h+1)*e,:],ds))
        g_ref[s0:s0+n,cols(0)]=(jnp.concatenate(dqs,axis=0)*f).T.astype(BF)
    g_ref[:,cols(1)]=(dk_ref[...]*f).astype(BF)
    g_ref[:,cols(2)]=dv_ref[...].astype(BF)

def attn_bwd(mixed,o,lse,do,heads,count=None,step=256):
    L,w3=mixed.shape; Dm=w3//3; e=Dm//heads; G=Dm//128; per=128//e
    masked=count is not None
    spec=lambda off: pl.BlockSpec((L,128),lambda g,*_:(0,off+g))
    gs=pltpu.PrefetchScalarGridSpec(num_scalar_prefetch=1 if masked else 0,grid=(G,),
        in_specs=[spec(0),spec(G),spec(2*G),spec(0),spec(0),pl.BlockSpec((1,per,L),lambda g,*_:(g,0,0))],
        out_specs=pl.BlockSpec((L,w3),lambda g,*_:(0,0)),
        scratch_shapes=[pltpu.VMEM((L,128),F32)]*2)
    return pl.pallas_call(functools.partial(bwd_kernel,e,step,masked),grid_spec=gs,out_shape=jax.ShapeDtypeStruct((L,w3),BF),
        compiler_params=pltpu.CompilerParams(vmem_limit_bytes=56<<20),
        cost_estimate=pl.CostEstimate(flops=10*heads*L*L*e,bytes_accessed=L*Dm*16,transcendentals=heads*L*L),name="attn_bwd")(*((count,) if masked else ()),mixed,mixed,mixed,o,do,lse)


MESH = pl.DeviceIdType.MESH
ANY = pl.BlockSpec(memory_space=pl.ANY)

def place():
    tok=lax.axis_index("tok"); head=lax.axis_index("head")
    return tok//2, tok%2, head//2, head%2

def peer(z,y,x,c): return (z*2+y, x*2+c)

def greet(barrier_peers):
    barrier=pltpu.get_barrier_semaphore()
    for p in barrier_peers:
        pl.semaphore_signal(barrier,inc=1,device_id=p,device_id_type=MESH)
    pl.semaphore_wait(barrier,len(barrier_peers))

def gather_steps(shard, full, own, cut, quarter, local, send, recv):
    z,y,x,c=place()
    xs = x if quarter else slice(None)
    rows, cols = cut
    def rcopy(i,src,dst,dev):
        return pltpu.make_async_remote_copy(src_ref=src,dst_ref=dst,send_sem=send.at[i],recv_sem=recv.at[i],device_id=dev,device_id_type=MESH)
    mine=shard.at[xs,c,rows,cols]
    def load(): return pltpu.make_async_copy(mine,own,local.at[0])
    def put(): return pltpu.make_async_copy(own,full.at[z,y,xs,c,rows,cols],local.at[1])
    def zc(k,out):
        dst=full.at[z,y,xs,c,rows,cols] if out else full.at[(z+4-k)%4,y,xs,c,rows,cols]
        return rcopy(k-1,mine,dst,peer((z+k)%4,y,x,c))
    def yc(out):
        yy=y if out else 1-y
        return rcopy(3,full.at[:,y,xs,c,rows,cols],full.at[:,yy,xs,c,rows,cols],peer(z,1-y,x,c))
    def xc(out):
        xx=x if out else 1-x
        return rcopy(4,full.at[:,:,x,c,rows,cols],full.at[:,:,xx,c,rows,cols],peer(z,y,1-x,c))
    def cc(out):
        cz=c if out else 1-c
        return rcopy(5,full.at[:,:,:,c,rows,cols],full.at[:,:,:,cz,rows,cols],peer(z,y,x,1-c))
    def s0():
        load().start()
        for k in (2,1,3): zc(k,True).start()
    def s1():
        load().wait(); put().start()
        for k in (1,2,3): zc(k,False).wait_recv()
        put().wait()
        yc(True).start()
    def s2():
        yc(False).wait_recv()
        if quarter: xc(True).start()
        else: cc(True).start()
    def s3():
        if quarter:
            xc(False).wait_recv(); cc(True).start()
    def s4():
        cc(False).wait_recv()
        for k in (1,2,3): zc(k,True).wait_send()
        yc(True).wait_send()
        if quarter: xc(True).wait_send()
        cc(True).wait_send()
    return [s0,s1,s2,s3,s4]

def gains_steps(src,out,send,recv):
    z,y,x,c=place()
    def cp(k,outgoing):
        dz,dy=k//2,k%2
        t=z*2+y
        pz=(z+dz)%4; py=(y+dy)%2
        sz=(z+4-dz)%4; sy=(y+2-dy)%2
        dst=out.at[t] if outgoing else out.at[sz*2+sy]
        return pltpu.make_async_remote_copy(src_ref=src,dst_ref=dst,send_sem=send.at[k-1],recv_sem=recv.at[k-1],device_id=peer(pz,py,x,c),device_id_type=MESH)
    def start():
        for k in range(1,8): cp(k,True).start()
    def finish():
        for k in range(1,8): cp(k,False).wait_recv()
        for k in range(1,8): cp(k,True).wait_send()
    return start,finish

def everyone_on_tok():
    z,y,x,c=place()
    peers=[peer((z+k//2)%4,(y+k%2)%2,x,c) for k in range(1,8)]
    return peers+[peer(z,y,1-x,c),peer(z,y,x,1-c)]

def interleave(chunks):
    n=len(chunks); depth=len(chunks[0])
    order=[]
    for t in range(n+depth-1):
        for s in range(depth):
            i=t-s
            if 0<=i<n: order.append(chunks[i][s])
    return order

def ag_kernel(plan,n,*refs):
    shards=refs[:n]; gain=refs[n]; fulls=refs[n+1:2*n+1]; gout=refs[2*n+1]
    rest=refs[2*n+2:]
    owns=rest[:len(plan)]; gown,local,send,recv,gsend,grecv,glocal=rest[len(plan):]
    z,y,x,c=place()
    greet(everyone_on_tok())
    gs,gf=gains_steps(gain,gout,gsend,grecv)
    gs()
    g0=pltpu.make_async_copy(gain,gown,glocal.at[0]); g0.start()
    steps=[]
    for i,(w,r0,rn,c0,cn,quarter) in enumerate(plan):
        steps.append(gather_steps(shards[w],fulls[w],owns[i],(pl.ds(r0,rn),pl.ds(c0,cn)),quarter,local.at[i],send.at[i],recv.at[i]))
    for f in interleave(steps): f()
    g0.wait()
    g1=pltpu.make_async_copy(gown,gout.at[z*2+y],glocal.at[1]); g1.start(); g1.wait()
    gf()

def gather_weights(shards, gains, plan, cid):
    n=len(shards)
    views=[s.reshape(2,2,s.shape[0]//4,s.shape[1]) for s in shards]
    outs=[jax.ShapeDtypeStruct((4,2,2,2,s.shape[0]//4,s.shape[1]),s.dtype) for s in shards]
    outs.append(jax.ShapeDtypeStruct((8,)+gains.shape,gains.dtype))
    owns=[pltpu.VMEM(((rn,cn) if q else (2,rn,cn)),jnp.bfloat16) for (w,r0,rn,c0,cn,q) in plan]
    k=len(plan)
    res=pl.pallas_call(functools.partial(ag_kernel,plan,n),out_shape=outs,in_specs=[ANY]*(n+1),out_specs=[ANY]*(n+1),
        scratch_shapes=owns+[pltpu.VMEM(gains.shape,gains.dtype),pltpu.SemaphoreType.DMA((k,2)),pltpu.SemaphoreType.DMA((k,6)),pltpu.SemaphoreType.DMA((k,6)),
            pltpu.SemaphoreType.DMA((7,)),pltpu.SemaphoreType.DMA((7,)),pltpu.SemaphoreType.DMA((2,))],
        compiler_params=pltpu.CompilerParams(collective_id=cid,has_side_effects=True),name="gather_weights")(*views,gains)
    return [o.reshape(8*s.shape[0],s.shape[1]) for o,s in zip(res[:n],shards)],res[n]


def reduce_steps(grad, out, rn, rows, bufs, order, everywhere, local, send, recv):
    z,y,x,c=place()
    M,C,A,B,Z,T=bufs
    def rcopy(i,src,dst,dev):
        return pltpu.make_async_remote_copy(src_ref=src,dst_ref=dst,send_sem=send.at[i],recv_sem=recv.at[i],device_id=dev,device_id_type=MESH)
    xfirst=order=="xy"
    side={"x":peer(z,y,1-x,c),"y":peer(z,1-y,x,c)}
    first,second=order
    load=lambda: pltpu.make_async_copy(grad.at[:,:,:,c,rows],M,local.at[0])
    cc=lambda: rcopy(0,grad.at[:,:,:,1-c,rows],C,side_c)
    side_c=peer(z,y,x,1-c)
    ac=lambda: rcopy(1,M.at[:,:,1-x] if xfirst else M.at[:,1-y],A,side[first])
    bc=lambda: rcopy(2,M.at[:,1-y,x] if xfirst else M.at[:,y,1-x],B,side[second])
    zc=lambda k: rcopy(2+k,M.at[(z+k)%4,y,x],Z.at[k-1],peer((z+k)%4,y,x,c))
    def add(target,source):
        target[...]=(target[...].astype(F32)+source[...].astype(F32)).astype(BF)
    def s0():
        cc().start(); load().start()
    def s1():
        load().wait(); cc().wait_recv()
        @pl.loop(0,16)
        def _(i):
            at=(i//4,(i//2)%2,i%2)
            add(M.at[at],C.at[at])
        ac().start()
    def s2():
        ac().wait_recv()
        @pl.loop(0,8)
        def _(i):
            if xfirst: add(M.at[i//2,i%2,x],A.at[i//2,i%2])
            else: add(M.at[i//2,y,i%2],A.at[i//2,i%2])
        bc().start()
    def s3():
        bc().wait_recv()
        @pl.loop(0,4)
        def _(i):
            add(M.at[i,y,x],B.at[i])
        for k in (2,1,3): zc(k).start()
    if everywhere:
        home=out.at[z,y,x,c,rows]
        spread=[]
        for k in (1,2,3):
            spread.append((5+k,lambda o,k=k:(T,out.at[z,y,x,c,rows] if o else out.at[(z+4-k)%4,y,x,c,rows],peer((z+k)%4,y,x,c))))
        sy=(9,lambda o:(out.at[:,y,x,c,rows],out.at[:,y if o else 1-y,x,c,rows],side["y"]))
        sx=(10,lambda o:(out.at[:,:,x,c,rows],out.at[:,:,x if o else 1-x,c,rows],side["x"]))
        if xfirst: stages=[spread,[sy],[sx]]
        else:
            sx=(9,lambda o:(out.at[:,y,x,c,rows],out.at[:,y,x if o else 1-x,c,rows],side["x"]))
            sy=(10,lambda o:(out.at[:,y,:,c,rows],out.at[:,y if o else 1-y,:,c,rows],side["y"]))
            stages=[spread,[sx],[sy]]
        stages.append([(11,lambda o:(out.at[:,:,:,c,rows],out.at[:,:,:,c if o else 1-c,rows],side_c))])
    else:
        home=out.at[x,c,rows]
        stages=[[(6,lambda o:(T,out.at[x if o else 1-x,c,rows],side["x"]))],[(7,lambda o:(out.at[:,c,rows],out.at[:,c if o else 1-c,rows],side_c))]]
    def run(entry,o):
        i,f=entry; src,dst,dev=f(o); return rcopy(i,src,dst,dev)
    put=lambda: pltpu.make_async_copy(T,home,local.at[1])
    def s4():
        for k in (1,2,3): zc(k).wait_recv()
        T[...]=(M[z,y,x].astype(F32)+Z[0].astype(F32)+Z[1].astype(F32)+Z[2].astype(F32)).astype(BF)
        put().start()
        for e in stages[0]: run(e,True).start()
    def later(n):
        def s():
            if n==1: put().wait()
            for e in stages[n-1]: run(e,False).wait_recv()
            for e in stages[n]: run(e,True).start()
        return s
    def last():
        for e in stages[-1]: run(e,False).wait_recv()
        cc().wait_send(); ac().wait_send(); bc().wait_send()
        for k in (1,2,3): zc(k).wait_send()
        for st in stages:
            for e in st: run(e,True).wait_send()
    mids=[later(n) for n in range(1,len(stages))]
    if not everywhere: mids=mids+[lambda:None]*2
    return [s0,s1,s2,s3,s4]+mids+[last]

def vector_steps(src,out,bufs,local,send,recv):
    z,y,x,c=place()
    V,R=bufs
    dev=[peer(z,y,x,1-c),peer(z,y,1-x,c),peer(z,1-y,x,c)]+[peer((z+k)%4,y,x,c) for k in (1,2,3)]
    def rc(i): return pltpu.make_async_remote_copy(src_ref=V.at[min(i,3)],dst_ref=R.at[i],send_sem=send.at[i],recv_sem=recv.at[i],device_id=dev[i],device_id_type=MESH)
    load=lambda: pltpu.make_async_copy(src,V.at[0],local.at[0])
    def s0():
        load().start(); load().wait(); rc(0).start()
    def mid(n):
        def s():
            rc(n-1).wait_recv()
            V[n]=V[n-1]+R[n-1]
            if n<3: rc(n).start()
            else:
                for i in (3,4,5): rc(i).start()
        return s
    def fin():
        for i in (3,4,5): rc(i).wait_recv()
        V[4]=V[3]+R[3]+R[4]+R[5]
        cp=pltpu.make_async_copy(V.at[4],out,local.at[1]); cp.start(); cp.wait()
        for i in range(6): rc(i).wait_send()
    nothing=lambda:None
    return [s0,mid(1),mid(2),mid(3),fin,nothing,nothing,nothing,nothing]

def rs_kernel(plan,n,*refs):
    grads=refs[:n]; vec=refs[n]; outs=refs[n+1:2*n+1]; vout=refs[2*n+1]; rest=refs[2*n+2:]
    k=len(plan)
    bufs=[rest[6*i:6*i+6] for i in range(k)]
    V,R,local,send,recv,vlocal,vsend,vrecv=rest[6*k:]
    z,y,x,c=place()
    greet([peer((z+j)%4,y,x,c) for j in (1,2,3)]+[peer(z,1-y,x,c),peer(z,y,1-x,c),peer(z,y,x,1-c)])
    steps=[reduce_steps(grads[w],outs[w],rn,pl.ds(r0,rn),bufs[i],order,ev,local.at[i],send.at[i],recv.at[i]) for i,(w,r0,rn,order,ev) in enumerate(plan)]
    steps.append(vector_steps(vec,vout,(V,R),vlocal,vsend,vrecv))
    for st in steps: st[0]()
    for f in interleave([st[1:] for st in steps]): f()

def reduce_grads(grads, vec, plan, cid):
    n=len(grads)
    every={w:ev for w,_,_,_,ev in plan}
    views=[g.reshape(4,2,2,2,g.shape[0]//32,g.shape[1]) for g in grads]
    outs=[jax.ShapeDtypeStruct(v.shape if every[w] else v.shape[2:],BF) for w,v in enumerate(views)]
    outs.append(jax.ShapeDtypeStruct(vec.shape,F32))
    scratch=[]
    for (w,r0,rn,order,ev) in plan:
        N=grads[w].shape[1]
        scratch+=[pltpu.VMEM((4,2,2,rn,N),BF),pltpu.VMEM((4,2,2,rn,N),BF),pltpu.VMEM((4,2,rn,N),BF),pltpu.VMEM((4,rn,N),BF),pltpu.VMEM((3,rn,N),BF),pltpu.VMEM((rn,N),BF)]
    k=len(plan)
    S=pltpu.SemaphoreType.DMA
    scratch+=[pltpu.VMEM((5,)+vec.shape,F32),pltpu.VMEM((6,)+vec.shape,F32),S((k,2)),S((k,12)),S((k,12)),S((2,)),S((6,)),S((6,))]
    res=pl.pallas_call(functools.partial(rs_kernel,plan,n),out_shape=outs,in_specs=[ANY]*(n+1),out_specs=[ANY]*(n+1),scratch_shapes=scratch,
        compiler_params=pltpu.CompilerParams(collective_id=cid,has_side_effects=True,vmem_limit_bytes=60<<20),name="reduce_grads")(*views,vec)
    flat=[]
    for w,r in enumerate(res[:n]):
        rows=grads[w].shape[0]
        flat.append(r.reshape(rows if every[w] else rows//8,grads[w].shape[1]))
    return flat,res[n]


def gather_plan(shards):
    quarter = lambda w: shards[w].shape[0] // 4
    wide = lambda w: shards[w].shape[1]
    plan = [(1, 0, quarter(1), 0, wide(1), True)]
    for w, sliced in ((0, True), (4, True), (2, True), (6, False), (3, True), (7, False)):
        half = quarter(w) // 2
        plan += [(w, part * half, half, 0, wide(w), sliced) for part in (0, 1)]
    return plan + [(5, 0, quarter(5), 0, wide(5), True)]


def every_weight(tuned, gains, shards):
    if not tuned:
        return tuple(lax.all_gather(v, "tok", axis=0, tiled=True) for v in gains + shards)
    packed = jnp.pad(jnp.stack(gains), ((0, 12), (0, 0)))
    full, norms = gather_weights(list(shards), packed, gather_plan(shards), 1)
    return tuple(norms[:, i, :].reshape(-1) for i in range(4)) + tuple(full)


def every_grad(tuned, context, predict):
    if not tuned:
        parts = [lax.psum_scatter(v, "tok", scatter_dimension=0, tiled=True) for v in context]
        return (
            tuple(lax.psum(v.astype(jnp.bfloat16), "head").astype(jnp.float32) for v in parts),
            lax.psum(predict, ("tok", "head")),
        )
    entry, mask, prenorm, project, outward, midnorm, expand, shrink, endnorm, leave = predict
    model_width, width = entry.shape
    wide = jnp.concatenate([project, outward, expand, leave], axis=1).astype(BF)
    blocks = wide.shape[1] // model_width
    wide = jnp.concatenate(
        [wide[:, i * model_width : (i + 1) * model_width] for i in range(blocks)], axis=0
    )
    tall = jnp.concatenate([entry, shrink], axis=0).astype(BF)
    small = (mask, prenorm, midnorm, endnorm, context[0], context[3])
    line = jnp.concatenate(small)
    vector = jnp.pad(line, (0, -line.shape[0] % 1024)).reshape(-1, 128)
    grads = [context[1], context[2], context[4], context[5]]
    grads = [v.astype(BF) for v in grads] + [wide, tall]
    piece = [v.shape[0] // 32 for v in grads]
    plan = [
        (4, 0, piece[4], "yx", True),
        (5, 0, piece[5], "xy", True),
        (3, 0, piece[3] // 2, "xy", False),
        (3, piece[3] // 2, piece[3] // 2, "yx", False),
        (2, 0, piece[2] // 2, "xy", False),
        (2, piece[2] // 2, piece[2] // 2, "yx", False),
        (1, 0, piece[1], "xy", False),
        (0, 0, piece[0] // 2, "yx", False),
        (0, piece[0] // 2, piece[0] // 2, "xy", False),
    ]
    sums, vector = reduce_grads(grads, vector, plan, 2)
    sums = [v.astype(F32) for v in sums]
    line = vector.reshape(-1)
    lines = []
    for v in small:
        lines.append(line[: v.shape[0]])
        line = line[v.shape[0] :]
    share = model_width // lax.axis_size("tok")
    mine = lambda v: lax.dynamic_slice_in_dim(v, lax.axis_index("tok") * share, share)
    wide = jnp.concatenate(
        [sums[4][i * width : (i + 1) * width] for i in range(blocks)], axis=1
    )
    cuts = [0]
    for v in (project, outward, expand, leave):
        cuts.append(cuts[-1] + v.shape[1])
    project, outward, expand, leave = (wide[:, a:b] for a, b in zip(cuts, cuts[1:]))
    return (
        (mine(lines[4]), sums[0], sums[1], mine(lines[5]), sums[2], sums[3]),
        (
            sums[5][:model_width],
            lines[0],
            lines[1],
            project,
            outward,
            lines[2],
            expand,
            sums[5][model_width:],
            lines[3],
            leave,
        ),
    )


def feed_forward(mid_rows, midnorm, expand, shrink):
    mid_wide = mid_rows.astype(jnp.float32)
    normed = layer_norm(mid_wide, midnorm).astype(jnp.bfloat16)
    raised = product(normed, expand)
    active = jax.nn.gelu(raised).astype(jnp.bfloat16)
    output = (mid_wide + product(active, shrink)).astype(jnp.bfloat16)
    return (output, (mid_wide, normed, raised, active))


def feed_forward_back(grad_rows, saved, midnorm, expand, shrink):
    mid_wide, normed, raised, active = saved
    grad_shrink = inner_rows(active, grad_rows)
    grad_active = inner_cols(grad_rows, shrink)
    unused, gelu_pullback = jax.vjp(jax.nn.gelu, raised)
    grad_raised = gelu_pullback(grad_active)[0].astype(jnp.bfloat16)
    grad_expand = inner_rows(normed, grad_raised)
    grad_normed = inner_cols(grad_raised, expand)
    unused, norm_pullback = jax.vjp(layer_norm, mid_wide, midnorm)
    grad_mid, grad_midnorm = norm_pullback(grad_normed)
    grad_total = (grad_rows.astype(jnp.float32) + grad_mid).astype(jnp.bfloat16)
    return (grad_total, (grad_midnorm, grad_expand, grad_shrink))


def shards(
    tokens,
    target_prenorm,
    target_project,
    target_outward,
    target_midnorm,
    target_expand,
    target_shrink,
    context_prenorm,
    context_project,
    context_outward,
    context_midnorm,
    context_expand,
    context_shrink,
    predict_entry,
    mask_token,
    predict_prenorm,
    predict_project,
    predict_outward,
    predict_midnorm,
    predict_expand,
    predict_shrink,
    predict_endnorm,
    predict_exit,
    clip_order,
    visible_count,
):
    clips_here = clip_order.shape[0]
    clip_len = clip_order.shape[1]
    model_width = tokens.shape[1]
    head_devices = lax.axis_size("head")
    lane_index = lax.axis_index("tok")
    head_index = lax.axis_index("head")
    device_index = lane_index * head_devices + head_index
    counts_here = lax.dynamic_slice_in_dim(visible_count, device_index * clips_here, clips_here)
    tuned = lax.axis_size("tok") == 8 and head_devices == 4
    (
        tgt_prenorm_full,
        tgt_midnorm_full,
        ctx_prenorm_full,
        ctx_midnorm_full,
        tgt_project_full,
        tgt_outward_full,
        tgt_expand_full,
        tgt_shrink_full,
        ctx_project_full,
        ctx_outward_full,
        ctx_expand_full,
        ctx_shrink_full,
    ) = every_weight(
        tuned,
        (target_prenorm, target_midnorm, context_prenorm, context_midnorm),
        (
            target_project,
            target_outward,
            target_expand,
            target_shrink,
            context_project,
            context_outward,
            context_expand,
            context_shrink,
        ),
    )
    tokens_wide = tokens.astype(jnp.float32)
    target_in = layer_norm(tokens_wide, tgt_prenorm_full.astype(jnp.float32)).astype(jnp.bfloat16)
    target_mixed = product(target_in, tgt_project_full).astype(jnp.bfloat16)
    target_attn = attn_fwd(target_mixed, H, want_lse=False)[0]
    target_mid = tokens_wide + product(target_attn, tgt_outward_full)
    target_normed = layer_norm(target_mid, tgt_midnorm_full.astype(jnp.float32)).astype(
        jnp.bfloat16
    )
    target_active = jax.nn.gelu(product(target_normed, tgt_expand_full)).astype(jnp.bfloat16)
    target_out = plain_norm(target_mid + product(target_active, tgt_shrink_full))
    order_rank = jnp.argsort(clip_order, axis=1)
    visible = order_rank < counts_here[:, None]
    visible_pos = clip_order[:, :VMOST]
    slot_live = jnp.arange(VMOST, dtype=jnp.int32)[None, :] < counts_here[:, None]
    token_grid = tokens.reshape(clips_here, clip_len, model_width)
    seen_rows = jnp.take_along_axis(token_grid, visible_pos[:, :, None], axis=1)
    seen_rows = seen_rows.reshape(clips_here * VMOST, model_width).astype(jnp.float32)
    ctx_prenorm_wide = ctx_prenorm_full.astype(jnp.float32)
    ctx_midnorm_wide = ctx_midnorm_full.astype(jnp.float32)
    context_in = layer_norm(seen_rows, ctx_prenorm_wide).astype(jnp.bfloat16)
    context_mixed = product(context_in, ctx_project_full).astype(jnp.bfloat16)
    context_attn, context_lse = attn_fwd(context_mixed, H, counts_here)
    context_mid = (seen_rows + product(context_attn, ctx_outward_full)).astype(jnp.bfloat16)
    context_out, ffn_saved = feed_forward(
        context_mid, ctx_midnorm_wide, ctx_expand_full, ctx_shrink_full
    )
    entry_rows = product(context_out, predict_entry).reshape(clips_here, VMOST, -1)
    placed = jnp.take_along_axis(entry_rows, jnp.minimum(order_rank, VMOST - 1)[:, :, None], axis=1)
    start_rows = jnp.where(
        visible[:, :, None], placed, mask_token.astype(jnp.float32)[None, None, :]
    )
    start_rows = (start_rows + positions(clip_len, PD)[None]).reshape(clips_here * clip_len, PD)
    pred_prenorm_wide = predict_prenorm.astype(jnp.float32)
    pred_midnorm_wide = predict_midnorm.astype(jnp.float32)
    pred_endnorm_wide = predict_endnorm.astype(jnp.float32)
    predict_in = layer_norm(start_rows, pred_prenorm_wide).astype(jnp.bfloat16)
    predict_mixed = product(predict_in, predict_project).astype(jnp.bfloat16)
    predict_attn, predict_lse = attn_fwd(predict_mixed, PH)
    branch_rows = start_rows + product(predict_attn, predict_outward)
    predict_normed = layer_norm(branch_rows, pred_midnorm_wide).astype(jnp.bfloat16)
    predict_raised = product(predict_normed, predict_expand)
    predict_active = jax.nn.gelu(predict_raised).astype(jnp.bfloat16)
    final_rows = branch_rows + product(predict_active, predict_shrink)
    final_in = layer_norm(final_rows, pred_endnorm_wide).astype(jnp.bfloat16)
    predicted = product(final_in, predict_exit)
    differ = predicted - target_out
    hidden_rows = jnp.logical_not(visible).reshape(-1)
    row_error = jnp.mean(smooth_error(differ), axis=1)
    clip_sums = jnp.sum(
        jnp.where(hidden_rows, row_error, 0.0).reshape(clips_here, clip_len), axis=1
    )
    clip_loss = clip_sums / (clip_len - counts_here).astype(jnp.float32)
    slope = jnp.clip(differ / HUBER, -1.0, 1.0)
    grad_predicted = (jnp.where(hidden_rows[:, None], slope, 0.0) / model_width).astype(
        jnp.bfloat16
    )
    grad_exit = inner_rows(final_in, grad_predicted)
    grad_final_in = inner_cols(grad_predicted, predict_exit)
    unused, norm_pullback = jax.vjp(layer_norm, final_rows, pred_endnorm_wide)
    grad_final, grad_endnorm = norm_pullback(grad_final_in)
    grad_second = grad_final.astype(jnp.bfloat16)
    grad_pred_shrink = inner_rows(predict_active, grad_second)
    grad_pred_active = inner_cols(grad_second, predict_shrink)
    unused, gelu_pullback = jax.vjp(jax.nn.gelu, predict_raised)
    grad_pred_raised = gelu_pullback(grad_pred_active)[0].astype(jnp.bfloat16)
    grad_pred_expand = inner_rows(predict_normed, grad_pred_raised)
    grad_pred_normed = inner_cols(grad_pred_raised, predict_expand)
    unused, norm_pullback = jax.vjp(layer_norm, branch_rows, pred_midnorm_wide)
    grad_branch_norm, grad_pred_midnorm = norm_pullback(grad_pred_normed)
    grad_branch = grad_final + grad_branch_norm
    grad_first = grad_branch.astype(jnp.bfloat16)
    grad_pred_outward = inner_rows(predict_attn, grad_first)
    grad_pred_attn = inner_cols(grad_first, predict_outward).astype(jnp.bfloat16)
    grad_pred_mixed = attn_bwd(predict_mixed, predict_attn, predict_lse, grad_pred_attn, PH)
    grad_pred_project = inner_rows(predict_in, grad_pred_mixed)
    grad_pred_in = inner_cols(grad_pred_mixed, predict_project)
    unused, norm_pullback = jax.vjp(layer_norm, start_rows, pred_prenorm_wide)
    grad_start_norm, grad_pred_prenorm = norm_pullback(grad_pred_in)
    grad_start = (grad_branch + grad_start_norm).reshape(clips_here, clip_len, PD)
    grad_mask = jnp.sum(jnp.where(visible[:, :, None], 0.0, grad_start), axis=(0, 1))
    grad_entry_rows = jnp.take_along_axis(grad_start, visible_pos[:, :, None], axis=1)
    grad_entry_rows = jnp.where(slot_live[:, :, None], grad_entry_rows, 0.0)
    grad_entry_rows = grad_entry_rows.reshape(clips_here * VMOST, PD).astype(jnp.bfloat16)
    grad_entry = inner_rows(context_out, grad_entry_rows)
    grad_context_out = inner_cols(grad_entry_rows, predict_entry).astype(jnp.bfloat16)
    back_project, back_outward = ctx_project_full, ctx_outward_full
    back_expand, back_shrink = ctx_expand_full, ctx_shrink_full
    back_prenorm_wide, back_midnorm_wide = ctx_prenorm_wide, ctx_midnorm_wide
    grad_mid, ffn_grads = feed_forward_back(
        grad_context_out, ffn_saved, back_midnorm_wide, back_expand, back_shrink
    )
    grad_ctx_outward = inner_rows(context_attn, grad_mid)
    grad_ctx_attn = inner_cols(grad_mid, back_outward).astype(jnp.bfloat16)
    grad_ctx_mixed = attn_bwd(
        context_mixed, context_attn, context_lse, grad_ctx_attn, H, counts_here
    )
    grad_ctx_project = inner_rows(context_in, grad_ctx_mixed)
    grad_ctx_in = inner_cols(grad_ctx_mixed, back_project)
    unused, norm_pullback = jax.vjp(layer_norm, seen_rows, back_prenorm_wide)
    grad_seen_norm, grad_ctx_prenorm = norm_pullback(grad_ctx_in)
    grad_seen = (grad_mid.astype(jnp.float32) + grad_seen_norm).reshape(
        clips_here, VMOST, model_width
    )
    grad_grid = jnp.take_along_axis(
        grad_seen, jnp.minimum(order_rank, VMOST - 1)[:, :, None], axis=1
    )
    tokens_grad = jnp.where(visible[:, :, None], grad_grid, 0.0).reshape(
        clips_here * clip_len, model_width
    )
    context_sums, predict_sums = every_grad(
        tuned,
        (
            grad_ctx_prenorm,
            grad_ctx_project,
            grad_ctx_outward,
            ffn_grads[0],
            ffn_grads[1],
            ffn_grads[2],
        ),
        (
            grad_entry,
            grad_mask,
            grad_pred_prenorm,
            grad_pred_project,
            grad_pred_outward,
            grad_pred_midnorm,
            grad_pred_expand,
            grad_pred_shrink,
            grad_endnorm,
            grad_exit,
        ),
    )
    return (
        clip_loss,
        tokens_grad,
        context_sums[0],
        context_sums[1],
        context_sums[2],
        context_sums[3],
        context_sums[4],
        context_sums[5],
        predict_sums[0],
        predict_sums[1],
        predict_sums[2],
        predict_sums[3],
        predict_sums[4],
        predict_sums[5],
        predict_sums[6],
        predict_sums[7],
        predict_sums[8],
        predict_sums[9],
    )


def solution(mesh):
    return jax.shard_map(
        shards,
        mesh=mesh,
        in_specs=(
            P(("tok", "head"), None),
            P("tok"),
            P("tok", None),
            P("tok", None),
            P("tok"),
            P("tok", None),
            P("tok", None),
            P("tok"),
            P("tok", None),
            P("tok", None),
            P("tok"),
            P("tok", None),
            P("tok", None),
            P(),
            P(),
            P(),
            P(),
            P(),
            P(),
            P(),
            P(),
            P(),
            P(),
            P(("tok", "head"), None),
            P(),
        ),
        out_specs=(
            P(("tok", "head")),
            P(("tok", "head"), None),
            P("tok"),
            P("tok", None),
            P("tok", None),
            P("tok"),
            P("tok", None),
            P("tok", None),
            P(),
            P(),
            P(),
            P(),
            P(),
            P(),
            P(),
            P(),
            P(),
            P(),
        ),
        check_vma=False,
    )
```

```python
import functools

import jax
import jax.numpy as jnp
from jax import lax
from jax.experimental import pallas as pl
from jax.experimental.pallas import tpu as pltpu
from jax.sharding import PartitionSpec as P

H = 16
PD = 384
PH = 12
VMOST = 464


EPSILON = 1e-06
HUBER = 0.25


def layer_norm(values, gains):
    center = values - jnp.mean(values, axis=-1, keepdims=True)
    spread = jnp.mean(center * center, axis=-1, keepdims=True)
    return center * lax.rsqrt(spread + EPSILON) * gains


def plain_norm(values):
    center = values - jnp.mean(values, axis=-1, keepdims=True)
    spread = jnp.mean(center * center, axis=-1, keepdims=True)
    return center * lax.rsqrt(spread + EPSILON)


def smooth_error(differ):
    magnitude = jnp.abs(differ)
    return jnp.where(magnitude < HUBER, 0.5 * differ * differ / HUBER, magnitude - 0.5 * HUBER)


def positions(length, breadth, block=32):
    half_width = breadth // 2
    freqs = jnp.exp(-jnp.log(10000.0) * jnp.arange(half_width, dtype=jnp.float32) / half_width)
    coarse = jnp.arange(0, length, block, dtype=jnp.float32)[:, None, None] * freqs
    fine = jnp.arange(block, dtype=jnp.float32)[None, :, None] * freqs
    sines = lax.optimization_barrier((jnp.sin(coarse), jnp.cos(coarse), jnp.sin(fine), jnp.cos(fine)))
    sin_far, cos_far, sin_near, cos_near = sines
    table = jnp.concatenate(
        [sin_far * cos_near + cos_far * sin_near, cos_far * cos_near - sin_far * sin_near], axis=2
    )
    return table.reshape(-1, breadth)[:length]


def product(former, latter):
    return jnp.dot(former, latter, preferred_element_type=jnp.float32)


def inner_rows(former, latter):
    return lax.dot_general(
        former, latter, (((0,), (0,)), ((), ())), preferred_element_type=jnp.float32
    )


def inner_cols(former, latter):
    return lax.dot_general(
        former, latter, (((1,), (1,)), ((), ())), preferred_element_type=jnp.float32
    )


BF=jnp.bfloat16; F32=jnp.float32
LOG2E=1.4426950408889634
NT=(((1,),(1,)),((),())); NN=(((1,),(0,)),((),()))
def dot(a,b,dims=NN): return lax.dot_general(a,b,dims,preferred_element_type=F32)
def chunks(n,step):
    return [(i,min(step,n-i)) for i in range(0,n,step)]
def lane_mask(rows,h,e):
    lane=lax.broadcasted_iota(jnp.int32,(rows,128),1)
    return (lane>=h*e)&(lane<(h+1)*e)
def head_rows(values,h,e):
    return jnp.where(lane_mask(values.shape[0],h,e),values,jnp.zeros_like(values))

def fwd_kernel(e,step,masked,want_lse,*refs):
    refs=list(refs)
    count=refs.pop(0) if masked else None
    q_ref,k_ref,v_ref,o_ref=refs[:4]
    lse_ref=refs[4] if want_lse else None
    L=q_ref.shape[0]; per=128//e; c=e**-0.5*LOG2E
    k=k_ref[...]
    vt=v_ref[...].T
    live=None
    if masked:
        live=lax.broadcasted_iota(jnp.int32,(L,1),0)<count[0]
    for (s0,n) in chunks(L,step):
        outs=[]; lses=[]
        for h in range(per):
            q=head_rows(q_ref[s0:s0+n,:],h,e)
            st=dot(k,q,NT)
            if masked: st=jnp.where(live,st,-1e30)
            m=jnp.max(st,axis=0,keepdims=True)
            p=jnp.exp2((st-m)*c)
            l=jnp.sum(p,axis=0,keepdims=True)
            o=dot(vt[h*e:(h+1)*e,:],p.astype(BF))
            outs.append(o*(1.0/l))
            if want_lse: lses.append(m*c+jnp.log2(l))
        o_ref[s0:s0+n,:]=jnp.concatenate(outs,axis=0).T.astype(BF)
        if want_lse: lse_ref[0,:,s0:s0+n]=jnp.concatenate(lses,axis=0)

def attn_fwd(mixed,heads,count=None,step=1280,want_lse=True):
    L,w3=mixed.shape; Dm=w3//3; e=Dm//heads; G=Dm//128; per=128//e
    masked=count is not None
    spec=lambda off: pl.BlockSpec((L,128),lambda g,*_:(0,off+g))
    out_shape=[jax.ShapeDtypeStruct((L,Dm),BF)]; out_specs=[pl.BlockSpec((L,128),lambda g,*_:(0,g))]
    if want_lse:
        out_shape.append(jax.ShapeDtypeStruct((G,per,L),F32)); out_specs.append(pl.BlockSpec((1,per,L),lambda g,*_:(g,0,0)))
    gs=pltpu.PrefetchScalarGridSpec(num_scalar_prefetch=1 if masked else 0,grid=(G,),in_specs=[spec(0),spec(G),spec(2*G)],out_specs=out_specs)
    flops=4*heads*L*L*e
    f=pl.pallas_call(functools.partial(fwd_kernel,e,step,masked,want_lse),grid_spec=gs,out_shape=out_shape,
        compiler_params=pltpu.CompilerParams(vmem_limit_bytes=56<<20),
        cost_estimate=pl.CostEstimate(flops=flops,bytes_accessed=L*Dm*8,transcendentals=heads*L*L),name="attn_fwd")
    return f(*((count,) if masked else ()),mixed,mixed,mixed)

def bwd_kernel(e,step,masked,*refs):
    refs=list(refs)
    count=refs.pop(0) if masked else None
    q_ref,k_ref,v_ref,o_ref,do_ref,lse_ref,g_ref,dk_ref,dv_ref=refs
    L=q_ref.shape[0]; per=128//e; c=e**-0.5*LOG2E; f=e**-0.5
    g=pl.program_id(0); G=pl.num_programs(0)
    k=k_ref[...]; v=v_ref[...]
    kt=k.T
    live=None
    if masked:
        live=lax.broadcasted_iota(jnp.int32,(L,1),0)<count[0]
    dk_ref[...]=jnp.zeros_like(dk_ref); dv_ref[...]=jnp.zeros_like(dv_ref)
    cols=lambda part: pl.ds(pl.multiple_of((part*G+g)*128,128),128)
    for (s0,n) in chunks(L,step):
        do_all=do_ref[s0:s0+n,:]; q_all=q_ref[s0:s0+n,:]
        prod=(do_all.astype(F32)*o_ref[s0:s0+n,:].astype(F32)).T
        dqs=[]
        for h in range(per):
            q=head_rows(q_all,h,e); do=head_rows(do_all,h,e)
            delta=jnp.sum(prod[h*e:(h+1)*e,:],axis=0,keepdims=True)
            st=dot(k,q,NT)
            p=jnp.exp2(st*c-lse_ref[0,h:h+1,s0:s0+n])
            if masked: p=jnp.where(live,p,0.0)
            dp=dot(v,do,NT)
            ds=(p*(dp-delta)).astype(BF)
            dv_ref[...]+=dot(p.astype(BF),do)
            dk_ref[...]+=dot(ds,q)
            dqs.append(dot(kt[h*e:(h+1)*e,:],ds))
        g_ref[s0:s0+n,cols(0)]=(jnp.concatenate(dqs,axis=0)*f).T.astype(BF)
    g_ref[:,cols(1)]=(dk_ref[...]*f).astype(BF)
    g_ref[:,cols(2)]=dv_ref[...].astype(BF)

def attn_bwd(mixed,o,lse,do,heads,count=None,step=256):
    L,w3=mixed.shape; Dm=w3//3; e=Dm//heads; G=Dm//128; per=128//e
    masked=count is not None
    spec=lambda off: pl.BlockSpec((L,128),lambda g,*_:(0,off+g))
    gs=pltpu.PrefetchScalarGridSpec(num_scalar_prefetch=1 if masked else 0,grid=(G,),
        in_specs=[spec(0),spec(G),spec(2*G),spec(0),spec(0),pl.BlockSpec((1,per,L),lambda g,*_:(g,0,0))],
        out_specs=pl.BlockSpec((L,w3),lambda g,*_:(0,0)),
        scratch_shapes=[pltpu.VMEM((L,128),F32)]*2)
    return pl.pallas_call(functools.partial(bwd_kernel,e,step,masked),grid_spec=gs,out_shape=jax.ShapeDtypeStruct((L,w3),BF),
        compiler_params=pltpu.CompilerParams(vmem_limit_bytes=56<<20),
        cost_estimate=pl.CostEstimate(flops=10*heads*L*L*e,bytes_accessed=L*Dm*16,transcendentals=heads*L*L),name="attn_bwd")(*((count,) if masked else ()),mixed,mixed,mixed,o,do,lse)


MESH = pl.DeviceIdType.MESH
ANY = pl.BlockSpec(memory_space=pl.ANY)

def place():
    tok=lax.axis_index("tok"); head=lax.axis_index("head")
    return tok//2, tok%2, head//2, head%2

def peer(z,y,x,c): return (z*2+y, x*2+c)

def greet(barrier_peers):
    barrier=pltpu.get_barrier_semaphore()
    for p in barrier_peers:
        pl.semaphore_signal(barrier,inc=1,device_id=p,device_id_type=MESH)
    pl.semaphore_wait(barrier,len(barrier_peers))

def gather_steps(shard, full, own, cut, quarter, local, send, recv):
    z,y,x,c=place()
    xs = x if quarter else slice(None)
    rows, cols = cut
    def rcopy(i,src,dst,dev):
        return pltpu.make_async_remote_copy(src_ref=src,dst_ref=dst,send_sem=send.at[i],recv_sem=recv.at[i],device_id=dev,device_id_type=MESH)
    mine=shard.at[xs,c,rows,cols]
    def load(): return pltpu.make_async_copy(mine,own,local.at[0])
    def put(): return pltpu.make_async_copy(own,full.at[z,y,xs,c,rows,cols],local.at[1])
    def zc(k,out):
        dst=full.at[z,y,xs,c,rows,cols] if out else full.at[(z+4-k)%4,y,xs,c,rows,cols]
        return rcopy(k-1,mine,dst,peer((z+k)%4,y,x,c))
    def yc(out):
        yy=y if out else 1-y
        return rcopy(3,full.at[:,y,xs,c,rows,cols],full.at[:,yy,xs,c,rows,cols],peer(z,1-y,x,c))
    def xc(out):
        xx=x if out else 1-x
        return rcopy(4,full.at[:,:,x,c,rows,cols],full.at[:,:,xx,c,rows,cols],peer(z,y,1-x,c))
    def cc(out):
        cz=c if out else 1-c
        return rcopy(5,full.at[:,:,:,c,rows,cols],full.at[:,:,:,cz,rows,cols],peer(z,y,x,1-c))
    def s0():
        load().start()
        for k in (2,1,3): zc(k,True).start()
    def s1():
        load().wait(); put().start()
        for k in (1,2,3): zc(k,False).wait_recv()
        put().wait()
        yc(True).start()
    def s2():
        yc(False).wait_recv()
        if quarter: xc(True).start()
        else: cc(True).start()
    def s3():
        if quarter:
            xc(False).wait_recv(); cc(True).start()
    def s4():
        cc(False).wait_recv()
        for k in (1,2,3): zc(k,True).wait_send()
        yc(True).wait_send()
        if quarter: xc(True).wait_send()
        cc(True).wait_send()
    return [s0,s1,s2,s3,s4]

def gains_steps(src,out,send,recv):
    z,y,x,c=place()
    def cp(k,outgoing):
        dz,dy=k//2,k%2
        t=z*2+y
        pz=(z+dz)%4; py=(y+dy)%2
        sz=(z+4-dz)%4; sy=(y+2-dy)%2
        dst=out.at[t] if outgoing else out.at[sz*2+sy]
        return pltpu.make_async_remote_copy(src_ref=src,dst_ref=dst,send_sem=send.at[k-1],recv_sem=recv.at[k-1],device_id=peer(pz,py,x,c),device_id_type=MESH)
    def start():
        for k in range(1,8): cp(k,True).start()
    def finish():
        for k in range(1,8): cp(k,False).wait_recv()
        for k in range(1,8): cp(k,True).wait_send()
    return start,finish

def everyone_on_tok():
    z,y,x,c=place()
    peers=[peer((z+k//2)%4,(y+k%2)%2,x,c) for k in range(1,8)]
    return peers+[peer(z,y,1-x,c),peer(z,y,x,1-c)]

def together(members):
    def stage(s):
        def run():
            for m in members: m[s]()
        return run
    return [stage(s) for s in range(len(members[0]))]

def interleave(chunks):
    n=len(chunks); depth=len(chunks[0])
    order=[]
    for t in range(n+depth-1):
        for s in range(depth):
            i=t-s
            if 0<=i<n: order.append(chunks[i][s])
    return order

def ag_kernel(plan,n,*refs):
    shards=refs[:n]; gain=refs[n]; fulls=refs[n+1:2*n+1]; gout=refs[2*n+1]
    rest=refs[2*n+2:]
    owns=rest[:len(plan)]; gown,local,send,recv,gsend,grecv,glocal=rest[len(plan):]
    z,y,x,c=place()
    greet(everyone_on_tok())
    gs,gf=gains_steps(gain,gout,gsend,grecv)
    gs()
    g0=pltpu.make_async_copy(gain,gown,glocal.at[0]); g0.start()
    steps=[]
    for i,(w,r0,rn,c0,cn,quarter) in enumerate(plan):
        steps.append(gather_steps(shards[w],fulls[w],owns[i],(pl.ds(r0,rn),pl.ds(c0,cn)),quarter,local.at[i],send.at[i],recv.at[i]))
    groups={}
    for st,entry in zip(steps,plan): groups.setdefault(entry[:3],[]).append(st)
    for f in interleave([together(m) for m in groups.values()]): f()
    g0.wait()
    g1=pltpu.make_async_copy(gown,gout.at[z*2+y],glocal.at[1]); g1.start(); g1.wait()
    gf()

def gather_weights(shards, gains, plan, cid):
    n=len(shards)
    views=[s.reshape(2,2,s.shape[0]//4,s.shape[1]) for s in shards]
    outs=[jax.ShapeDtypeStruct((4,2,2,2,s.shape[0]//4,s.shape[1]),s.dtype) for s in shards]
    outs.append(jax.ShapeDtypeStruct((8,)+gains.shape,gains.dtype))
    owns=[pltpu.VMEM(((rn,cn) if q else (2,rn,cn)),jnp.bfloat16) for (w,r0,rn,c0,cn,q) in plan]
    k=len(plan)
    res=pl.pallas_call(functools.partial(ag_kernel,plan,n),out_shape=outs,in_specs=[ANY]*(n+1),out_specs=[ANY]*(n+1),
        scratch_shapes=owns+[pltpu.VMEM(gains.shape,gains.dtype),pltpu.SemaphoreType.DMA((k,2)),pltpu.SemaphoreType.DMA((k,6)),pltpu.SemaphoreType.DMA((k,6)),
            pltpu.SemaphoreType.DMA((7,)),pltpu.SemaphoreType.DMA((7,)),pltpu.SemaphoreType.DMA((2,))],
        compiler_params=pltpu.CompilerParams(collective_id=cid,has_side_effects=True),name="gather_weights")(*views,gains)
    return [o.reshape(8*s.shape[0],s.shape[1]) for o,s in zip(res[:n],shards)],res[n]


def reduce_steps(grad, out, rn, rows, bufs, order, everywhere, local, send, recv):
    z,y,x,c=place()
    M,C,A,B,Z,T=bufs
    def rcopy(i,src,dst,dev):
        return pltpu.make_async_remote_copy(src_ref=src,dst_ref=dst,send_sem=send.at[i],recv_sem=recv.at[i],device_id=dev,device_id_type=MESH)
    xfirst=order=="xy"
    side={"x":peer(z,y,1-x,c),"y":peer(z,1-y,x,c)}
    first,second=order
    load=lambda: pltpu.make_async_copy(grad.at[:,:,:,c,rows],M,local.at[0])
    cc=lambda: rcopy(0,grad.at[:,:,:,1-c,rows],C,side_c)
    side_c=peer(z,y,x,1-c)
    ac=lambda: rcopy(1,M.at[:,:,1-x] if xfirst else M.at[:,1-y],A,side[first])
    bc=lambda: rcopy(2,M.at[:,1-y,x] if xfirst else M.at[:,y,1-x],B,side[second])
    zc=lambda k: rcopy(2+k,M.at[(z+k)%4,y,x],Z.at[k-1],peer((z+k)%4,y,x,c))
    def add(target,source):
        target[...]=(target[...].astype(F32)+source[...].astype(F32)).astype(BF)
    def s0():
        cc().start(); load().start()
    def s1():
        load().wait(); cc().wait_recv()
        @pl.loop(0,16)
        def _(i):
            at=(i//4,(i//2)%2,i%2)
            add(M.at[at],C.at[at])
        ac().start()
    def s2():
        ac().wait_recv()
        @pl.loop(0,8)
        def _(i):
            if xfirst: add(M.at[i//2,i%2,x],A.at[i//2,i%2])
            else: add(M.at[i//2,y,i%2],A.at[i//2,i%2])
        bc().start()
    def s3():
        bc().wait_recv()
        @pl.loop(0,4)
        def _(i):
            add(M.at[i,y,x],B.at[i])
        for k in (2,1,3): zc(k).start()
    if everywhere:
        home=out.at[z,y,x,c,rows]
        spread=[]
        for k in (1,2,3):
            spread.append((5+k,lambda o,k=k:(T,out.at[z,y,x,c,rows] if o else out.at[(z+4-k)%4,y,x,c,rows],peer((z+k)%4,y,x,c))))
        sy=(9,lambda o:(out.at[:,y,x,c,rows],out.at[:,y if o else 1-y,x,c,rows],side["y"]))
        sx=(10,lambda o:(out.at[:,:,x,c,rows],out.at[:,:,x if o else 1-x,c,rows],side["x"]))
        if xfirst: stages=[spread,[sy],[sx]]
        else:
            sx=(9,lambda o:(out.at[:,y,x,c,rows],out.at[:,y,x if o else 1-x,c,rows],side["x"]))
            sy=(10,lambda o:(out.at[:,y,:,c,rows],out.at[:,y if o else 1-y,:,c,rows],side["y"]))
            stages=[spread,[sx],[sy]]
        stages.append([(11,lambda o:(out.at[:,:,:,c,rows],out.at[:,:,:,c if o else 1-c,rows],side_c))])
    else:
        home=out.at[x,c,rows]
        stages=[[(6,lambda o:(T,out.at[x if o else 1-x,c,rows],side["x"]))],[(7,lambda o:(out.at[:,c,rows],out.at[:,c if o else 1-c,rows],side_c))]]
    def run(entry,o):
        i,f=entry; src,dst,dev=f(o); return rcopy(i,src,dst,dev)
    put=lambda: pltpu.make_async_copy(T,home,local.at[1])
    def s4():
        for k in (1,2,3): zc(k).wait_recv()
        T[...]=(M[z,y,x].astype(F32)+Z[0].astype(F32)+Z[1].astype(F32)+Z[2].astype(F32)).astype(BF)
        put().start()
        for e in stages[0]: run(e,True).start()
    def later(n):
        def s():
            if n==1: put().wait()
            for e in stages[n-1]: run(e,False).wait_recv()
            for e in stages[n]: run(e,True).start()
        return s
    def last():
        for e in stages[-1]: run(e,False).wait_recv()
        cc().wait_send(); ac().wait_send(); bc().wait_send()
        for k in (1,2,3): zc(k).wait_send()
        for st in stages:
            for e in st: run(e,True).wait_send()
    mids=[later(n) for n in range(1,len(stages))]
    if not everywhere: mids=mids+[lambda:None]*2
    return [s0,s1,s2,s3,s4]+mids+[last]

def vector_steps(src,out,bufs,local,send,recv):
    z,y,x,c=place()
    V,R=bufs
    dev=[peer(z,y,x,1-c),peer(z,y,1-x,c),peer(z,1-y,x,c)]+[peer((z+k)%4,y,x,c) for k in (1,2,3)]
    def rc(i): return pltpu.make_async_remote_copy(src_ref=V.at[min(i,3)],dst_ref=R.at[i],send_sem=send.at[i],recv_sem=recv.at[i],device_id=dev[i],device_id_type=MESH)
    load=lambda: pltpu.make_async_copy(src,V.at[0],local.at[0])
    def s0():
        load().start(); load().wait(); rc(0).start()
    def mid(n):
        def s():
            rc(n-1).wait_recv()
            V[n]=V[n-1]+R[n-1]
            if n<3: rc(n).start()
            else:
                for i in (3,4,5): rc(i).start()
        return s
    def fin():
        for i in (3,4,5): rc(i).wait_recv()
        V[4]=V[3]+R[3]+R[4]+R[5]
        cp=pltpu.make_async_copy(V.at[4],out,local.at[1]); cp.start(); cp.wait()
        for i in range(6): rc(i).wait_send()
    nothing=lambda:None
    return [s0,mid(1),mid(2),mid(3),fin,nothing,nothing,nothing,nothing]

def rs_kernel(plan,n,*refs):
    grads=refs[:n]; vec=refs[n]; outs=refs[n+1:2*n+1]; vout=refs[2*n+1]; rest=refs[2*n+2:]
    k=len(plan)
    bufs=[rest[6*i:6*i+6] for i in range(k)]
    V,R,local,send,recv,vlocal,vsend,vrecv=rest[6*k:]
    z,y,x,c=place()
    greet([peer((z+j)%4,y,x,c) for j in (1,2,3)]+[peer(z,1-y,x,c),peer(z,y,1-x,c),peer(z,y,x,1-c)])
    steps=[reduce_steps(grads[w],outs[w],rn,pl.ds(r0,rn),bufs[i],order,ev,local.at[i],send.at[i],recv.at[i]) for i,(w,r0,rn,order,ev,_) in enumerate(plan)]
    steps.append(vector_steps(vec,vout,(V,R),vlocal,vsend,vrecv))
    groups={}
    for st,entry in zip(steps,plan): groups.setdefault(entry[5],[]).append(st)
    groups[plan[0][5]].append(steps[-1])
    groups=[together(m) for m in groups.values()]
    for st in groups: st[0]()
    for f in interleave([st[1:] for st in groups]): f()

def reduce_grads(grads, vec, plan, cid):
    n=len(grads)
    every={w:ev for w,_,_,_,ev,_ in plan}
    views=[g.reshape(4,2,2,2,g.shape[0]//32,g.shape[1]) for g in grads]
    outs=[jax.ShapeDtypeStruct(v.shape if every[w] else v.shape[2:],BF) for w,v in enumerate(views)]
    outs.append(jax.ShapeDtypeStruct(vec.shape,F32))
    scratch=[]
    for (w,r0,rn,order,ev,_) in plan:
        N=grads[w].shape[1]
        scratch+=[pltpu.VMEM((4,2,2,rn,N),BF),pltpu.VMEM((4,2,2,rn,N),BF),pltpu.VMEM((4,2,rn,N),BF),pltpu.VMEM((4,rn,N),BF),pltpu.VMEM((3,rn,N),BF),pltpu.VMEM((rn,N),BF)]
    k=len(plan)
    S=pltpu.SemaphoreType.DMA
    scratch+=[pltpu.VMEM((5,)+vec.shape,F32),pltpu.VMEM((6,)+vec.shape,F32),S((k,2)),S((k,12)),S((k,12)),S((2,)),S((6,)),S((6,))]
    res=pl.pallas_call(functools.partial(rs_kernel,plan,n),out_shape=outs,in_specs=[ANY]*(n+1),out_specs=[ANY]*(n+1),scratch_shapes=scratch,
        compiler_params=pltpu.CompilerParams(collective_id=cid,has_side_effects=True,vmem_limit_bytes=60<<20),name="reduce_grads")(*views,vec)
    flat=[]
    for w,r in enumerate(res[:n]):
        rows=grads[w].shape[0]
        flat.append(r.reshape(rows if every[w] else rows//8,grads[w].shape[1]))
    return flat,res[n]


def gather_plan(shards):
    plan = []
    for w in (1, 0, 2, 3, 4, 6, 7, 5):
        rows, wide = shards[w].shape[0] // 4, shards[w].shape[1]
        rest = (wide // 3 + 64) // 128 * 128
        parts = 1 if wide == shards[w].shape[0] * 8 else 2
        for part in range(parts):
            r0, rn = part * rows // parts, rows // parts
            plan.append((w, r0, rn, 0, wide - rest, True))
            plan.append((w, r0, rn, wide - rest, rest, False))
    return plan


def every_weight(tuned, gains, shards):
    if not tuned:
        return tuple(lax.all_gather(v, "tok", axis=0, tiled=True) for v in gains + shards)
    packed = jnp.pad(jnp.stack(gains), ((0, 12), (0, 0)))
    full, norms = gather_weights(list(shards), packed, gather_plan(shards), 1)
    return tuple(norms[:, i, :].reshape(-1) for i in range(4)) + tuple(full)


def every_grad(tuned, context, predict):
    if not tuned:
        parts = [lax.psum_scatter(v, "tok", scatter_dimension=0, tiled=True) for v in context]
        return (
            tuple(lax.psum(v.astype(jnp.bfloat16), "head").astype(jnp.float32) for v in parts),
            lax.psum(predict, ("tok", "head")),
        )
    entry, mask, prenorm, project, outward, midnorm, expand, shrink, endnorm, leave = predict
    model_width, width = entry.shape
    wide = jnp.concatenate([project, outward, expand, leave], axis=1).astype(BF)
    blocks = wide.shape[1] // model_width
    wide = jnp.concatenate(
        [wide[:, i * model_width : (i + 1) * model_width] for i in range(blocks)], axis=0
    )
    tall = jnp.concatenate([entry, shrink], axis=0).astype(BF)
    small = (mask, prenorm, midnorm, endnorm, context[0], context[3])
    line = jnp.concatenate(small)
    vector = jnp.pad(line, (0, -line.shape[0] % 1024)).reshape(-1, 128)
    grads = [context[1], context[2], context[4], context[5]]
    grads = [v.astype(BF) for v in grads] + [wide, tall]
    piece = [v.shape[0] // 32 for v in grads]
    plan = [(4, 0, piece[4], "yx", True, 4), (5, 0, piece[5], "xy", True, 4)]
    for w in (1, 0, 2, 3):
        half = piece[w] // 2
        plan += [(w, 0, half, "xy", False, w), (w, half, half, "yx", False, w)]
    sums, vector = reduce_grads(grads, vector, plan, 2)
    sums = [v.astype(F32) for v in sums]
    line = vector.reshape(-1)
    lines = []
    for v in small:
        lines.append(line[: v.shape[0]])
        line = line[v.shape[0] :]
    share = model_width // lax.axis_size("tok")
    mine = lambda v: lax.dynamic_slice_in_dim(v, lax.axis_index("tok") * share, share)
    wide = jnp.concatenate(
        [sums[4][i * width : (i + 1) * width] for i in range(blocks)], axis=1
    )
    cuts = [0]
    for v in (project, outward, expand, leave):
        cuts.append(cuts[-1] + v.shape[1])
    project, outward, expand, leave = (wide[:, a:b] for a, b in zip(cuts, cuts[1:]))
    return (
        (mine(lines[4]), sums[0], sums[1], mine(lines[5]), sums[2], sums[3]),
        (
            sums[5][:model_width],
            lines[0],
            lines[1],
            project,
            outward,
            lines[2],
            expand,
            sums[5][model_width:],
            lines[3],
            leave,
        ),
    )


def ffn_kernel(mid_ref, gain_ref, expand_ref, shrink_ref, out_ref, normed_ref, sum_ref):
    step = pl.program_id(0)

    @pl.when(step == 0)
    def _():
        normed_ref[...] = layer_norm(mid_ref[...], gain_ref[...]).astype(BF)
        sum_ref[...] = mid_ref[...]

    active = jax.nn.gelu(dot(normed_ref[...], expand_ref[...])).astype(BF)
    sum_ref[...] += dot(active, shrink_ref[...])

    @pl.when(step == pl.num_programs(0) - 1)
    def _():
        out_ref[...] = plain_norm(sum_ref[...])


def target_ffn(mid_rows, gain, expand, shrink, block=1024):
    length, width = mid_rows.shape
    hidden = expand.shape[1]
    whole = pl.BlockSpec((length, width), lambda j: (0, 0))
    return pl.pallas_call(
        ffn_kernel,
        grid=(hidden // block,),
        in_specs=[
            whole,
            pl.BlockSpec((1, width), lambda j: (0, 0)),
            pl.BlockSpec((width, block), lambda j: (0, j)),
            pl.BlockSpec((block, width), lambda j: (j, 0)),
        ],
        out_specs=whole,
        out_shape=jax.ShapeDtypeStruct((length, width), F32),
        scratch_shapes=[pltpu.VMEM((length, width), BF), pltpu.VMEM((length, width), F32)],
        compiler_params=pltpu.CompilerParams(vmem_limit_bytes=60 << 20),
        cost_estimate=pl.CostEstimate(
            flops=4 * length * width * hidden,
            bytes_accessed=8 * length * width + 4 * width * hidden,
            transcendentals=length * hidden,
        ),
        name="target_ffn",
    )(mid_rows, gain.reshape(1, -1), expand, shrink)


def feed_forward(mid_rows, midnorm, expand, shrink):
    mid_wide = mid_rows.astype(jnp.float32)
    normed = layer_norm(mid_wide, midnorm).astype(jnp.bfloat16)
    raised = product(normed, expand)
    active = jax.nn.gelu(raised).astype(jnp.bfloat16)
    output = (mid_wide + product(active, shrink)).astype(jnp.bfloat16)
    return (output, (mid_wide, normed, raised, active))


def feed_forward_back(grad_rows, saved, midnorm, expand, shrink):
    mid_wide, normed, raised, active = saved
    grad_shrink = inner_rows(active, grad_rows)
    grad_active = inner_cols(grad_rows, shrink)
    unused, gelu_pullback = jax.vjp(jax.nn.gelu, raised)
    grad_raised = gelu_pullback(grad_active)[0].astype(jnp.bfloat16)
    grad_expand = inner_rows(normed, grad_raised)
    grad_normed = inner_cols(grad_raised, expand)
    unused, norm_pullback = jax.vjp(layer_norm, mid_wide, midnorm)
    grad_mid, grad_midnorm = norm_pullback(grad_normed)
    grad_total = (grad_rows.astype(jnp.float32) + grad_mid).astype(jnp.bfloat16)
    return (grad_total, (grad_midnorm, grad_expand, grad_shrink))


def shards(
    tokens,
    target_prenorm,
    target_project,
    target_outward,
    target_midnorm,
    target_expand,
    target_shrink,
    context_prenorm,
    context_project,
    context_outward,
    context_midnorm,
    context_expand,
    context_shrink,
    predict_entry,
    mask_token,
    predict_prenorm,
    predict_project,
    predict_outward,
    predict_midnorm,
    predict_expand,
    predict_shrink,
    predict_endnorm,
    predict_exit,
    clip_order,
    visible_count,
):
    clips_here = clip_order.shape[0]
    clip_len = clip_order.shape[1]
    model_width = tokens.shape[1]
    head_devices = lax.axis_size("head")
    lane_index = lax.axis_index("tok")
    head_index = lax.axis_index("head")
    device_index = lane_index * head_devices + head_index
    counts_here = lax.dynamic_slice_in_dim(visible_count, device_index * clips_here, clips_here)
    tuned = lax.axis_size("tok") == 8 and head_devices == 4
    (
        tgt_prenorm_full,
        tgt_midnorm_full,
        ctx_prenorm_full,
        ctx_midnorm_full,
        tgt_project_full,
        tgt_outward_full,
        tgt_expand_full,
        tgt_shrink_full,
        ctx_project_full,
        ctx_outward_full,
        ctx_expand_full,
        ctx_shrink_full,
    ) = every_weight(
        tuned,
        (target_prenorm, target_midnorm, context_prenorm, context_midnorm),
        (
            target_project,
            target_outward,
            target_expand,
            target_shrink,
            context_project,
            context_outward,
            context_expand,
            context_shrink,
        ),
    )
    tokens_wide = tokens.astype(jnp.float32)
    target_in = layer_norm(tokens_wide, tgt_prenorm_full.astype(jnp.float32)).astype(jnp.bfloat16)
    target_mixed = product(target_in, tgt_project_full).astype(jnp.bfloat16)
    target_attn = attn_fwd(target_mixed, H, want_lse=False)[0]
    target_mid = tokens_wide + product(target_attn, tgt_outward_full)
    target_out = target_ffn(
        target_mid, tgt_midnorm_full.astype(jnp.float32), tgt_expand_full, tgt_shrink_full
    )
    visible_pos = clip_order[:, :VMOST]
    slot_live = jnp.arange(VMOST, dtype=jnp.int32)[None, :] < counts_here[:, None]
    holds = visible_pos[:, :, None] == jnp.arange(clip_len, dtype=jnp.int32)[None, None, :]
    holds = jnp.logical_and(holds, slot_live[:, :, None])
    visible = jnp.any(holds, axis=1)
    slot = jnp.arange(VMOST, dtype=jnp.int32)[None, :, None]
    order_rank = jnp.sum(jnp.where(holds, slot, 0), axis=1)
    token_grid = tokens.reshape(clips_here, clip_len, model_width)
    seen_rows = jnp.einsum(
        "csl,cld->csd", holds.astype(BF), token_grid, preferred_element_type=jnp.float32
    )
    seen_rows = seen_rows.reshape(clips_here * VMOST, model_width)
    ctx_prenorm_wide = ctx_prenorm_full.astype(jnp.float32)
    ctx_midnorm_wide = ctx_midnorm_full.astype(jnp.float32)
    context_in = layer_norm(seen_rows, ctx_prenorm_wide).astype(jnp.bfloat16)
    context_mixed = product(context_in, ctx_project_full).astype(jnp.bfloat16)
    context_attn, context_lse = attn_fwd(context_mixed, H, counts_here)
    context_mid = (seen_rows + product(context_attn, ctx_outward_full)).astype(jnp.bfloat16)
    context_out, ffn_saved = feed_forward(
        context_mid, ctx_midnorm_wide, ctx_expand_full, ctx_shrink_full
    )
    entry_rows = product(context_out, predict_entry).reshape(clips_here, VMOST, -1)
    placed = jnp.take_along_axis(entry_rows, order_rank[:, :, None], axis=1)
    start_rows = jnp.where(
        visible[:, :, None], placed, mask_token.astype(jnp.float32)[None, None, :]
    )
    start_rows = (start_rows + positions(clip_len, PD)[None]).reshape(clips_here * clip_len, PD)
    pred_prenorm_wide = predict_prenorm.astype(jnp.float32)
    pred_midnorm_wide = predict_midnorm.astype(jnp.float32)
    pred_endnorm_wide = predict_endnorm.astype(jnp.float32)
    predict_in = layer_norm(start_rows, pred_prenorm_wide).astype(jnp.bfloat16)
    predict_mixed = product(predict_in, predict_project).astype(jnp.bfloat16)
    predict_attn, predict_lse = attn_fwd(predict_mixed, PH)
    branch_rows = start_rows + product(predict_attn, predict_outward)
    predict_normed = layer_norm(branch_rows, pred_midnorm_wide).astype(jnp.bfloat16)
    predict_raised = product(predict_normed, predict_expand)
    predict_active = jax.nn.gelu(predict_raised).astype(jnp.bfloat16)
    final_rows = branch_rows + product(predict_active, predict_shrink)
    final_in = layer_norm(final_rows, pred_endnorm_wide).astype(jnp.bfloat16)
    predicted = product(final_in, predict_exit)
    differ = predicted - target_out
    hidden_rows = jnp.logical_not(visible).reshape(-1)
    row_error = jnp.mean(smooth_error(differ), axis=1)
    clip_sums = jnp.sum(
        jnp.where(hidden_rows, row_error, 0.0).reshape(clips_here, clip_len), axis=1
    )
    clip_loss = clip_sums / (clip_len - counts_here).astype(jnp.float32)
    slope = jnp.clip(differ / HUBER, -1.0, 1.0)
    grad_predicted = (jnp.where(hidden_rows[:, None], slope, 0.0) / model_width).astype(
        jnp.bfloat16
    )
    grad_exit = inner_rows(final_in, grad_predicted)
    grad_final_in = inner_cols(grad_predicted, predict_exit)
    unused, norm_pullback = jax.vjp(layer_norm, final_rows, pred_endnorm_wide)
    grad_final, grad_endnorm = norm_pullback(grad_final_in)
    grad_second = grad_final.astype(jnp.bfloat16)
    grad_pred_shrink = inner_rows(predict_active, grad_second)
    grad_pred_active = inner_cols(grad_second, predict_shrink)
    unused, gelu_pullback = jax.vjp(jax.nn.gelu, predict_raised)
    grad_pred_raised = gelu_pullback(grad_pred_active)[0].astype(jnp.bfloat16)
    grad_pred_expand = inner_rows(predict_normed, grad_pred_raised)
    grad_pred_normed = inner_cols(grad_pred_raised, predict_expand)
    unused, norm_pullback = jax.vjp(layer_norm, branch_rows, pred_midnorm_wide)
    grad_branch_norm, grad_pred_midnorm = norm_pullback(grad_pred_normed)
    grad_branch = grad_final + grad_branch_norm
    grad_first = grad_branch.astype(jnp.bfloat16)
    grad_pred_outward = inner_rows(predict_attn, grad_first)
    grad_pred_attn = inner_cols(grad_first, predict_outward).astype(jnp.bfloat16)
    grad_pred_mixed = attn_bwd(predict_mixed, predict_attn, predict_lse, grad_pred_attn, PH)
    grad_pred_project = inner_rows(predict_in, grad_pred_mixed)
    grad_pred_in = inner_cols(grad_pred_mixed, predict_project)
    unused, norm_pullback = jax.vjp(layer_norm, start_rows, pred_prenorm_wide)
    grad_start_norm, grad_pred_prenorm = norm_pullback(grad_pred_in)
    grad_start = (grad_branch + grad_start_norm).reshape(clips_here, clip_len, PD)
    grad_mask = jnp.sum(jnp.where(visible[:, :, None], 0.0, grad_start), axis=(0, 1))
    grad_entry_rows = jnp.take_along_axis(grad_start, visible_pos[:, :, None], axis=1)
    grad_entry_rows = jnp.where(slot_live[:, :, None], grad_entry_rows, 0.0)
    grad_entry_rows = grad_entry_rows.reshape(clips_here * VMOST, PD).astype(jnp.bfloat16)
    grad_entry = inner_rows(context_out, grad_entry_rows)
    grad_context_out = inner_cols(grad_entry_rows, predict_entry).astype(jnp.bfloat16)
    back_project, back_outward = ctx_project_full, ctx_outward_full
    back_expand, back_shrink = ctx_expand_full, ctx_shrink_full
    back_prenorm_wide, back_midnorm_wide = ctx_prenorm_wide, ctx_midnorm_wide
    grad_mid, ffn_grads = feed_forward_back(
        grad_context_out, ffn_saved, back_midnorm_wide, back_expand, back_shrink
    )
    grad_ctx_outward = inner_rows(context_attn, grad_mid)
    grad_ctx_attn = inner_cols(grad_mid, back_outward).astype(jnp.bfloat16)
    grad_ctx_mixed = attn_bwd(
        context_mixed, context_attn, context_lse, grad_ctx_attn, H, counts_here
    )
    grad_ctx_project = inner_rows(context_in, grad_ctx_mixed)
    grad_ctx_in = inner_cols(grad_ctx_mixed, back_project)
    unused, norm_pullback = jax.vjp(layer_norm, seen_rows, back_prenorm_wide)
    grad_seen_norm, grad_ctx_prenorm = norm_pullback(grad_ctx_in)
    grad_seen = (grad_mid.astype(jnp.float32) + grad_seen_norm).reshape(
        clips_here, VMOST, model_width
    )
    grad_grid = jnp.take_along_axis(
        grad_seen, order_rank[:, :, None], axis=1
    )
    tokens_grad = jnp.where(visible[:, :, None], grad_grid, 0.0).reshape(
        clips_here * clip_len, model_width
    )
    context_sums, predict_sums = every_grad(
        tuned,
        (
            grad_ctx_prenorm,
            grad_ctx_project,
            grad_ctx_outward,
            ffn_grads[0],
            ffn_grads[1],
            ffn_grads[2],
        ),
        (
            grad_entry,
            grad_mask,
            grad_pred_prenorm,
            grad_pred_project,
            grad_pred_outward,
            grad_pred_midnorm,
            grad_pred_expand,
            grad_pred_shrink,
            grad_endnorm,
            grad_exit,
        ),
    )
    return (
        clip_loss,
        tokens_grad,
        context_sums[0],
        context_sums[1],
        context_sums[2],
        context_sums[3],
        context_sums[4],
        context_sums[5],
        predict_sums[0],
        predict_sums[1],
        predict_sums[2],
        predict_sums[3],
        predict_sums[4],
        predict_sums[5],
        predict_sums[6],
        predict_sums[7],
        predict_sums[8],
        predict_sums[9],
    )


def solution(mesh):
    return jax.shard_map(
        shards,
        mesh=mesh,
        in_specs=(
            P(("tok", "head"), None),
            P("tok"),
            P("tok", None),
            P("tok", None),
            P("tok"),
            P("tok", None),
            P("tok", None),
            P("tok"),
            P("tok", None),
            P("tok", None),
            P("tok"),
            P("tok", None),
            P("tok", None),
            P(),
            P(),
            P(),
            P(),
            P(),
            P(),
            P(),
            P(),
            P(),
            P(),
            P(("tok", "head"), None),
            P(),
        ),
        out_specs=(
            P(("tok", "head")),
            P(("tok", "head"), None),
            P("tok"),
            P("tok", None),
            P("tok", None),
            P("tok"),
            P("tok", None),
            P("tok", None),
            P(),
            P(),
            P(),
            P(),
            P(),
            P(),
            P(),
            P(),
            P(),
            P(),
        ),
        check_vma=False,
    )
```

```python
import functools

import jax
import jax.numpy as jnp
from jax import lax
from jax.experimental import pallas as pl
from jax.experimental.pallas import tpu as pltpu
from jax.sharding import PartitionSpec as P

H = 16
PD = 384
PH = 12
VMOST = 464


EPSILON = 1e-06
HUBER = 0.25


def layer_norm(values, gains):
    center = values - jnp.mean(values, axis=-1, keepdims=True)
    spread = jnp.mean(center * center, axis=-1, keepdims=True)
    return center * lax.rsqrt(spread + EPSILON) * gains


def plain_norm(values):
    center = values - jnp.mean(values, axis=-1, keepdims=True)
    spread = jnp.mean(center * center, axis=-1, keepdims=True)
    return center * lax.rsqrt(spread + EPSILON)


def smooth_error(differ):
    magnitude = jnp.abs(differ)
    return jnp.where(magnitude < HUBER, 0.5 * differ * differ / HUBER, magnitude - 0.5 * HUBER)


def positions(length, breadth, block=32):
    half_width = breadth // 2
    freqs = jnp.exp(-jnp.log(10000.0) * jnp.arange(half_width, dtype=jnp.float32) / half_width)
    coarse = jnp.arange(0, length, block, dtype=jnp.float32)[:, None, None] * freqs
    fine = jnp.arange(block, dtype=jnp.float32)[None, :, None] * freqs
    sines = lax.optimization_barrier((jnp.sin(coarse), jnp.cos(coarse), jnp.sin(fine), jnp.cos(fine)))
    sin_far, cos_far, sin_near, cos_near = sines
    table = jnp.concatenate(
        [sin_far * cos_near + cos_far * sin_near, cos_far * cos_near - sin_far * sin_near], axis=2
    )
    return table.reshape(-1, breadth)[:length]


def product(former, latter):
    return jnp.dot(former, latter, preferred_element_type=jnp.float32)


def inner_rows(former, latter):
    return lax.dot_general(
        former, latter, (((0,), (0,)), ((), ())), preferred_element_type=jnp.float32
    )


def inner_cols(former, latter):
    return lax.dot_general(
        former, latter, (((1,), (1,)), ((), ())), preferred_element_type=jnp.float32
    )


BF=jnp.bfloat16; F32=jnp.float32
LOG2E=1.4426950408889634
NT=(((1,),(1,)),((),())); NN=(((1,),(0,)),((),()))
def dot(a,b,dims=NN): return lax.dot_general(a,b,dims,preferred_element_type=F32)
def chunks(n,step):
    return [(i,min(step,n-i)) for i in range(0,n,step)]
def lane_mask(rows,h,e):
    lane=lax.broadcasted_iota(jnp.int32,(rows,128),1)
    return (lane>=h*e)&(lane<(h+1)*e)
def head_rows(values,h,e):
    return jnp.where(lane_mask(values.shape[0],h,e),values,jnp.zeros_like(values))

def attend_group(q_all,k,v,e,live,step):
    L=q_all.shape[0]; per=128//e; c=e**-0.5*LOG2E
    vt=v.T
    results=[]; sums=[]
    for (s0,n) in chunks(L,step):
        outs=[]; lses=[]
        for h in range(per):
            q=head_rows(q_all[s0:s0+n,:],h,e)
            st=dot(k,q,NT)
            if live is not None: st=jnp.where(live,st,-1e30)
            m=jnp.max(st,axis=0,keepdims=True)
            p=jnp.exp2((st-m)*c)
            l=jnp.sum(p,axis=0,keepdims=True)
            outs.append(dot(vt[h*e:(h+1)*e,:],p.astype(BF))*(1.0/l))
            lses.append(m*c+jnp.log2(l))
        results.append(jnp.concatenate(outs,axis=0).T.astype(BF))
        sums.append(jnp.concatenate(lses,axis=0))
    if len(results)==1: return results[0],sums[0]
    return jnp.concatenate(results,axis=0),jnp.concatenate(sums,axis=1)

def fwd_kernel(e,step,masked,want_lse,*refs):
    refs=list(refs)
    count=refs.pop(0) if masked else None
    q_ref,k_ref,v_ref,o_ref=refs[:4]
    L=q_ref.shape[0]
    live=lax.broadcasted_iota(jnp.int32,(L,1),0)<count[0] if masked else None
    o_ref[...],lse=attend_group(q_ref[...],k_ref[...],v_ref[...],e,live,step)
    if want_lse: refs[4][0]=lse

def attn_fwd(mixed,heads,count=None,step=1280,want_lse=True):
    L,w3=mixed.shape; Dm=w3//3; e=Dm//heads; G=Dm//128; per=128//e
    masked=count is not None
    spec=lambda off: pl.BlockSpec((L,128),lambda g,*_:(0,off+g))
    out_shape=[jax.ShapeDtypeStruct((L,Dm),BF)]; out_specs=[pl.BlockSpec((L,128),lambda g,*_:(0,g))]
    if want_lse:
        out_shape.append(jax.ShapeDtypeStruct((G,per,L),F32)); out_specs.append(pl.BlockSpec((1,per,L),lambda g,*_:(g,0,0)))
    gs=pltpu.PrefetchScalarGridSpec(num_scalar_prefetch=1 if masked else 0,grid=(G,),in_specs=[spec(0),spec(G),spec(2*G)],out_specs=out_specs)
    flops=4*heads*L*L*e
    f=pl.pallas_call(functools.partial(fwd_kernel,e,step,masked,want_lse),grid_spec=gs,out_shape=out_shape,
        compiler_params=pltpu.CompilerParams(vmem_limit_bytes=56<<20),
        cost_estimate=pl.CostEstimate(flops=flops,bytes_accessed=L*Dm*8,transcendentals=heads*L*L),name="attn_fwd")
    return f(*((count,) if masked else ()),mixed,mixed,mixed)

def bwd_kernel(e,step,masked,*refs):
    refs=list(refs)
    count=refs.pop(0) if masked else None
    q_ref,k_ref,v_ref,o_ref,do_ref,lse_ref,g_ref,dk_ref,dv_ref=refs
    L=q_ref.shape[0]; per=128//e; c=e**-0.5*LOG2E; f=e**-0.5
    g=pl.program_id(0); G=pl.num_programs(0)
    k=k_ref[...]; v=v_ref[...]
    kt=k.T
    live=None
    if masked:
        live=lax.broadcasted_iota(jnp.int32,(L,1),0)<count[0]
    dk_ref[...]=jnp.zeros_like(dk_ref); dv_ref[...]=jnp.zeros_like(dv_ref)
    cols=lambda part: pl.ds(pl.multiple_of((part*G+g)*128,128),128)
    for (s0,n) in chunks(L,step):
        do_all=do_ref[s0:s0+n,:]; q_all=q_ref[s0:s0+n,:]
        prod=(do_all.astype(F32)*o_ref[s0:s0+n,:].astype(F32)).T
        dqs=[]
        for h in range(per):
            q=head_rows(q_all,h,e); do=head_rows(do_all,h,e)
            delta=jnp.sum(prod[h*e:(h+1)*e,:],axis=0,keepdims=True)
            st=dot(k,q,NT)
            p=jnp.exp2(st*c-lse_ref[0,h:h+1,s0:s0+n])
            if masked: p=jnp.where(live,p,0.0)
            dp=dot(v,do,NT)
            ds=(p*(dp-delta)).astype(BF)
            dv_ref[...]+=dot(p.astype(BF),do)
            dk_ref[...]+=dot(ds,q)
            dqs.append(dot(kt[h*e:(h+1)*e,:],ds))
        g_ref[s0:s0+n,cols(0)]=(jnp.concatenate(dqs,axis=0)*f).T.astype(BF)
    g_ref[:,cols(1)]=(dk_ref[...]*f).astype(BF)
    g_ref[:,cols(2)]=dv_ref[...].astype(BF)

def attn_bwd(mixed,o,lse,do,heads,count=None,step=256):
    L,w3=mixed.shape; Dm=w3//3; e=Dm//heads; G=Dm//128; per=128//e
    masked=count is not None
    spec=lambda off: pl.BlockSpec((L,128),lambda g,*_:(0,off+g))
    gs=pltpu.PrefetchScalarGridSpec(num_scalar_prefetch=1 if masked else 0,grid=(G,),
        in_specs=[spec(0),spec(G),spec(2*G),spec(0),spec(0),pl.BlockSpec((1,per,L),lambda g,*_:(g,0,0))],
        out_specs=pl.BlockSpec((L,w3),lambda g,*_:(0,0)),
        scratch_shapes=[pltpu.VMEM((L,128),F32)]*2)
    return pl.pallas_call(functools.partial(bwd_kernel,e,step,masked),grid_spec=gs,out_shape=jax.ShapeDtypeStruct((L,w3),BF),
        compiler_params=pltpu.CompilerParams(vmem_limit_bytes=56<<20),
        cost_estimate=pl.CostEstimate(flops=10*heads*L*L*e,bytes_accessed=L*Dm*16,transcendentals=heads*L*L),name="attn_bwd")(*((count,) if masked else ()),mixed,mixed,mixed,o,do,lse)


MESH = pl.DeviceIdType.MESH
ANY = pl.BlockSpec(memory_space=pl.ANY)

def place():
    tok=lax.axis_index("tok"); head=lax.axis_index("head")
    return tok//2, tok%2, head//2, head%2

def peer(z,y,x,c): return (z*2+y, x*2+c)

def greet(barrier_peers):
    barrier=pltpu.get_barrier_semaphore()
    for p in barrier_peers:
        pl.semaphore_signal(barrier,inc=1,device_id=p,device_id_type=MESH)
    pl.semaphore_wait(barrier,len(barrier_peers))

def gather_steps(shard, full, own, cut, quarter, local, send, recv):
    z,y,x,c=place()
    xs = x if quarter else slice(None)
    rows, cols = cut
    def rcopy(i,src,dst,dev):
        return pltpu.make_async_remote_copy(src_ref=src,dst_ref=dst,send_sem=send.at[i],recv_sem=recv.at[i],device_id=dev,device_id_type=MESH)
    mine=shard.at[xs,c,rows,cols]
    def load(): return pltpu.make_async_copy(mine,own,local.at[0])
    def put(): return pltpu.make_async_copy(own,full.at[z,y,xs,c,rows,cols],local.at[1])
    def zc(k,out):
        dst=full.at[z,y,xs,c,rows,cols] if out else full.at[(z+4-k)%4,y,xs,c,rows,cols]
        return rcopy(k-1,mine,dst,peer((z+k)%4,y,x,c))
    def yc(out):
        yy=y if out else 1-y
        return rcopy(3,full.at[:,y,xs,c,rows,cols],full.at[:,yy,xs,c,rows,cols],peer(z,1-y,x,c))
    def xc(out):
        xx=x if out else 1-x
        return rcopy(4,full.at[:,:,x,c,rows,cols],full.at[:,:,xx,c,rows,cols],peer(z,y,1-x,c))
    def cc(out):
        cz=c if out else 1-c
        return rcopy(5,full.at[:,:,:,c,rows,cols],full.at[:,:,:,cz,rows,cols],peer(z,y,x,1-c))
    def s0():
        load().start()
        for k in (2,1,3): zc(k,True).start()
    def s1():
        load().wait(); put().start()
        for k in (1,2,3): zc(k,False).wait_recv()
        put().wait()
        yc(True).start()
    def s2():
        yc(False).wait_recv()
        if quarter: xc(True).start()
        else: cc(True).start()
    def s3():
        if quarter:
            xc(False).wait_recv(); cc(True).start()
    def s4():
        cc(False).wait_recv()
        for k in (1,2,3): zc(k,True).wait_send()
        yc(True).wait_send()
        if quarter: xc(True).wait_send()
        cc(True).wait_send()
    return [s0,s1,s2,s3,s4]

def gains_steps(src,out,send,recv):
    z,y,x,c=place()
    def cp(k,outgoing):
        dz,dy=k//2,k%2
        t=z*2+y
        pz=(z+dz)%4; py=(y+dy)%2
        sz=(z+4-dz)%4; sy=(y+2-dy)%2
        dst=out.at[t] if outgoing else out.at[sz*2+sy]
        return pltpu.make_async_remote_copy(src_ref=src,dst_ref=dst,send_sem=send.at[k-1],recv_sem=recv.at[k-1],device_id=peer(pz,py,x,c),device_id_type=MESH)
    def start():
        for k in range(1,8): cp(k,True).start()
    def finish():
        for k in range(1,8): cp(k,False).wait_recv()
        for k in range(1,8): cp(k,True).wait_send()
    return start,finish

def everyone_on_tok():
    z,y,x,c=place()
    peers=[peer((z+k//2)%4,(y+k%2)%2,x,c) for k in range(1,8)]
    return peers+[peer(z,y,1-x,c),peer(z,y,x,1-c)]

def together(members):
    def stage(s):
        def run():
            for m in members: m[s]()
        return run
    return [stage(s) for s in range(len(members[0]))]

def interleave(chunks):
    n=len(chunks); depth=len(chunks[0])
    order=[]
    for t in range(n+depth-1):
        for s in range(depth):
            i=t-s
            if 0<=i<n: order.append(chunks[i][s])
    return order

def by_turn(chunks):
    turns=[[] for _ in range(len(chunks)+len(chunks[0])-1)]
    for i,chunk in enumerate(chunks):
        for s,stage in enumerate(chunk): turns[i+s].append((s,stage))
    return [[stage for _,stage in sorted(t,key=lambda p:p[0])] for t in turns]

def scaled_norm(values,gain_blocks,row,out_ref):
    normed=plain_norm(values.astype(F32))
    for t in range(gain_blocks.shape[0]):
        cols=slice(t*128,(t+1)*128)
        out_ref[:,cols]=(normed[:,cols]*gain_blocks[t,row:row+1,:].astype(F32)).astype(BF)

def ag_kernel(plan,n,heads,first,*refs):
    shards=refs[:n]; gain,tok_ref,seen_ref,live_ref=refs[n:n+4]
    fulls=refs[n+4:2*n+4]; gout,tattn,cin,cmixed,cattn,clse=refs[2*n+4:2*n+10]
    rest=refs[2*n+10:]
    k=len(plan)
    owns=rest[:k]; gown,local,send,recv,gsend,grecv,glocal,gv,tin,tw,cw,wsem=rest[k:]
    z,y,x,c=place()
    turn=pl.program_id(0)
    steps=[]
    for i,(w,r0,rn,c0,cn,quarter) in enumerate(plan):
        steps.append(gather_steps(shards[w],fulls[w],owns[i],(pl.ds(r0,rn),pl.ds(c0,cn)),quarter,local.at[i],send.at[i],recv.at[i]))
    groups={}
    for st,entry in zip(steps,plan): groups.setdefault(entry[:3],[]).append(st)
    turns=by_turn([together(m) for m in groups.values()])
    done={w:i+len(steps[0])-1 for i,(w,_,_) in enumerate(groups)}
    gs,gf=gains_steps(gain,gout,gsend,grecv)
    width=tok_ref.shape[1]; G=width//128; e=width//heads
    take=lambda w,dst,i: pltpu.make_async_copy(fulls[w],dst,wsem.at[i])
    for t,fs in enumerate(turns):
        @pl.when(turn==t)
        def _(t=t,fs=fs):
            if t==0: greet(everyone_on_tok())
            for f in fs: f()
            if t==0:
                gs()
                g0=pltpu.make_async_copy(gain,gown,glocal.at[0]); g0.start(); g0.wait()
                pltpu.make_async_copy(gown,gout.at[z*2+y],glocal.at[1]).start()
            if t==2:
                pltpu.make_async_copy(gown,gout.at[z*2+y],glocal.at[1]).wait()
                gf()
                g2=pltpu.make_async_copy(gout,gv,glocal.at[2]); g2.start(); g2.wait()
            if t==3: scaled_norm(tok_ref[...],gv,0,tin)
            if t==4: scaled_norm(seen_ref[...],gv,2,cin)
            if t==done[0]:
                take(0,tw,0).start(); take(0,tw,0).wait()
            if t==done[4]:
                take(4,cw,1).start(); take(4,cw,1).wait()
    def block(ref,part,g): return ref[:,:,:,:,:,pl.ds(pl.multiple_of((part*G+g)*128,128),128)].reshape(width,128)
    @pl.when((turn>=first)&(turn<first+G))
    def _():
        g=turn-first
        q,key,v=[dot(tin[...],block(tw,part,g)).astype(BF) for part in range(3)]
        o,_=attend_group(q,key,v,e,None,1280)
        tattn[:,pl.ds(pl.multiple_of(g*128,128),128)]=o
    later=first+G
    each=G//(len(turns)-later)
    @pl.when(turn>=later)
    def _():
        live=live_ref[...]!=0
        for j in range(each):
            g=(turn-later)*each+j
            parts=[dot(cin[...],block(cw,part,g)).astype(BF) for part in range(3)]
            for part in range(3):
                cmixed[:,pl.ds(pl.multiple_of((part*G+g)*128,128),128)]=parts[part]
            o,lse=attend_group(*parts,e,live,1280)
            cattn[:,pl.ds(pl.multiple_of(g*128,128),128)]=o
            clse[g]=lse

def gather_and_attend(shards,gains,tokens,seen,live,heads,plan,cid):
    n=len(shards); k=len(plan)
    views=[s.reshape(2,2,s.shape[0]//4,s.shape[1]) for s in shards]
    outs=[jax.ShapeDtypeStruct((4,2,2,2,s.shape[0]//4,s.shape[1]),s.dtype) for s in shards]
    outs.append(jax.ShapeDtypeStruct((8,)+gains.shape,gains.dtype))
    (L,width),slots=tokens.shape,seen.shape[0]
    G=width//128
    extra=[((L,width),BF),((slots,width),BF),((slots,3*width),BF),((slots,width),BF),((G,heads//G,slots),F32)]
    outs+=[jax.ShapeDtypeStruct(s,d) for s,d in extra]
    whole=lambda s: pl.BlockSpec(s,lambda t: (0,)*len(s))
    owns=[pltpu.VMEM(((rn,cn) if q else (2,rn,cn)),BF) for (w,r0,rn,c0,cn,q) in plan]
    S=pltpu.SemaphoreType.DMA
    turns=len({entry[:3] for entry in plan})+4
    scratch=owns+[pltpu.VMEM(gains.shape,BF),S((k,2)),S((k,6)),S((k,6)),S((7,)),S((7,)),S((3,)),
        pltpu.VMEM((8,)+gains.shape,BF),pltpu.VMEM((L,width),BF),pltpu.VMEM(outs[0].shape,BF),pltpu.VMEM(outs[4].shape,BF),S((2,))]
    first=turns-G-4
    res=pl.pallas_call(functools.partial(ag_kernel,plan,n,heads,first),grid=(turns,),out_shape=outs,
        in_specs=[ANY]*(n+1)+[whole(tokens.shape),whole(seen.shape),whole(live.shape)],
        out_specs=[ANY]*(n+1)+[whole(s) for s,_ in extra],scratch_shapes=scratch,
        compiler_params=pltpu.CompilerParams(collective_id=cid,has_side_effects=True,vmem_limit_bytes=60<<20),name="gather_and_attend")(*views,gains,tokens,seen,live)
    return [o.reshape(8*s.shape[0],s.shape[1]) for o,s in zip(res[:n],shards)],res[n],res[n+1:]

def reduce_steps(grad, out, rn, rows, bufs, order, everywhere, local, send, recv):
    z,y,x,c=place()
    M,C,A,B,Z,T=bufs
    def rcopy(i,src,dst,dev):
        return pltpu.make_async_remote_copy(src_ref=src,dst_ref=dst,send_sem=send.at[i],recv_sem=recv.at[i],device_id=dev,device_id_type=MESH)
    xfirst=order=="xy"
    side={"x":peer(z,y,1-x,c),"y":peer(z,1-y,x,c)}
    first,second=order
    load=lambda: pltpu.make_async_copy(grad.at[:,:,:,c,rows],M,local.at[0])
    cc=lambda: rcopy(0,grad.at[:,:,:,1-c,rows],C,side_c)
    side_c=peer(z,y,x,1-c)
    ac=lambda: rcopy(1,M.at[:,:,1-x] if xfirst else M.at[:,1-y],A,side[first])
    bc=lambda: rcopy(2,M.at[:,1-y,x] if xfirst else M.at[:,y,1-x],B,side[second])
    zc=lambda k: rcopy(2+k,M.at[(z+k)%4,y,x],Z.at[k-1],peer((z+k)%4,y,x,c))
    def add(target,source):
        target[...]=(target[...].astype(F32)+source[...].astype(F32)).astype(BF)
    def s0():
        cc().start(); load().start()
    def s1():
        load().wait(); cc().wait_recv()
        @pl.loop(0,16)
        def _(i):
            at=(i//4,(i//2)%2,i%2)
            add(M.at[at],C.at[at])
        ac().start()
    def s2():
        ac().wait_recv()
        @pl.loop(0,8)
        def _(i):
            if xfirst: add(M.at[i//2,i%2,x],A.at[i//2,i%2])
            else: add(M.at[i//2,y,i%2],A.at[i//2,i%2])
        bc().start()
    def s3():
        bc().wait_recv()
        @pl.loop(0,4)
        def _(i):
            add(M.at[i,y,x],B.at[i])
        for k in (2,1,3): zc(k).start()
    if everywhere:
        home=out.at[z,y,x,c,rows]
        spread=[]
        for k in (1,2,3):
            spread.append((5+k,lambda o,k=k:(T,out.at[z,y,x,c,rows] if o else out.at[(z+4-k)%4,y,x,c,rows],peer((z+k)%4,y,x,c))))
        sy=(9,lambda o:(out.at[:,y,x,c,rows],out.at[:,y if o else 1-y,x,c,rows],side["y"]))
        sx=(10,lambda o:(out.at[:,:,x,c,rows],out.at[:,:,x if o else 1-x,c,rows],side["x"]))
        if xfirst: stages=[spread,[sy],[sx]]
        else:
            sx=(9,lambda o:(out.at[:,y,x,c,rows],out.at[:,y,x if o else 1-x,c,rows],side["x"]))
            sy=(10,lambda o:(out.at[:,y,:,c,rows],out.at[:,y if o else 1-y,:,c,rows],side["y"]))
            stages=[spread,[sx],[sy]]
        stages.append([(11,lambda o:(out.at[:,:,:,c,rows],out.at[:,:,:,c if o else 1-c,rows],side_c))])
    else:
        home=out.at[x,c,rows]
        stages=[[(6,lambda o:(T,out.at[x if o else 1-x,c,rows],side["x"]))],[(7,lambda o:(out.at[:,c,rows],out.at[:,c if o else 1-c,rows],side_c))]]
    def run(entry,o):
        i,f=entry; src,dst,dev=f(o); return rcopy(i,src,dst,dev)
    put=lambda: pltpu.make_async_copy(T,home,local.at[1])
    def s4():
        for k in (1,2,3): zc(k).wait_recv()
        T[...]=(M[z,y,x].astype(F32)+Z[0].astype(F32)+Z[1].astype(F32)+Z[2].astype(F32)).astype(BF)
        put().start()
        for e in stages[0]: run(e,True).start()
    def later(n):
        def s():
            if n==1: put().wait()
            for e in stages[n-1]: run(e,False).wait_recv()
            for e in stages[n]: run(e,True).start()
        return s
    def last():
        for e in stages[-1]: run(e,False).wait_recv()
        cc().wait_send(); ac().wait_send(); bc().wait_send()
        for k in (1,2,3): zc(k).wait_send()
        for st in stages:
            for e in st: run(e,True).wait_send()
    mids=[later(n) for n in range(1,len(stages))]
    if not everywhere: mids=mids+[lambda:None]*2
    return [s0,s1,s2,s3,s4]+mids+[last]

def vector_steps(src,out,bufs,local,send,recv):
    z,y,x,c=place()
    V,R=bufs
    dev=[peer(z,y,x,1-c),peer(z,y,1-x,c),peer(z,1-y,x,c)]+[peer((z+k)%4,y,x,c) for k in (1,2,3)]
    def rc(i): return pltpu.make_async_remote_copy(src_ref=V.at[min(i,3)],dst_ref=R.at[i],send_sem=send.at[i],recv_sem=recv.at[i],device_id=dev[i],device_id_type=MESH)
    load=lambda: pltpu.make_async_copy(src,V.at[0],local.at[0])
    def s0():
        load().start(); load().wait(); rc(0).start()
    def mid(n):
        def s():
            rc(n-1).wait_recv()
            V[n]=V[n-1]+R[n-1]
            if n<3: rc(n).start()
            else:
                for i in (3,4,5): rc(i).start()
        return s
    def fin():
        for i in (3,4,5): rc(i).wait_recv()
        V[4]=V[3]+R[3]+R[4]+R[5]
        cp=pltpu.make_async_copy(V.at[4],out,local.at[1]); cp.start(); cp.wait()
        for i in range(6): rc(i).wait_send()
    nothing=lambda:None
    return [s0,mid(1),mid(2),mid(3),fin,nothing,nothing,nothing,nothing]

def rs_kernel(plan,n,*refs):
    grads=refs[:n]; vec=refs[n]; outs=refs[n+1:2*n+1]; vout=refs[2*n+1]; rest=refs[2*n+2:]
    k=len(plan)
    bufs=[rest[6*i:6*i+6] for i in range(k)]
    V,R,local,send,recv,vlocal,vsend,vrecv=rest[6*k:]
    z,y,x,c=place()
    greet([peer((z+j)%4,y,x,c) for j in (1,2,3)]+[peer(z,1-y,x,c),peer(z,y,1-x,c),peer(z,y,x,1-c)])
    steps=[reduce_steps(grads[w],outs[w],rn,pl.ds(r0,rn),bufs[i],order,ev,local.at[i],send.at[i],recv.at[i]) for i,(w,r0,rn,order,ev,_) in enumerate(plan)]
    steps.append(vector_steps(vec,vout,(V,R),vlocal,vsend,vrecv))
    groups={}
    for st,entry in zip(steps,plan): groups.setdefault(entry[5],[]).append(st)
    groups[plan[0][5]].append(steps[-1])
    groups=[together(m) for m in groups.values()]
    for st in groups: st[0]()
    for f in interleave([st[1:] for st in groups]): f()

def reduce_grads(grads, vec, plan, cid):
    n=len(grads)
    every={w:ev for w,_,_,_,ev,_ in plan}
    views=[g.reshape(4,2,2,2,g.shape[0]//32,g.shape[1]) for g in grads]
    outs=[jax.ShapeDtypeStruct(v.shape if every[w] else v.shape[2:],BF) for w,v in enumerate(views)]
    outs.append(jax.ShapeDtypeStruct(vec.shape,F32))
    scratch=[]
    for (w,r0,rn,order,ev,_) in plan:
        N=grads[w].shape[1]
        scratch+=[pltpu.VMEM((4,2,2,rn,N),BF),pltpu.VMEM((4,2,2,rn,N),BF),pltpu.VMEM((4,2,rn,N),BF),pltpu.VMEM((4,rn,N),BF),pltpu.VMEM((3,rn,N),BF),pltpu.VMEM((rn,N),BF)]
    k=len(plan)
    S=pltpu.SemaphoreType.DMA
    scratch+=[pltpu.VMEM((5,)+vec.shape,F32),pltpu.VMEM((6,)+vec.shape,F32),S((k,2)),S((k,12)),S((k,12)),S((2,)),S((6,)),S((6,))]
    res=pl.pallas_call(functools.partial(rs_kernel,plan,n),out_shape=outs,in_specs=[ANY]*(n+1),out_specs=[ANY]*(n+1),scratch_shapes=scratch,
        compiler_params=pltpu.CompilerParams(collective_id=cid,has_side_effects=True,vmem_limit_bytes=60<<20),name="reduce_grads")(*views,vec)
    flat=[]
    for w,r in enumerate(res[:n]):
        rows=grads[w].shape[0]
        flat.append(r.reshape(rows if every[w] else rows//8,grads[w].shape[1]))
    return flat,res[n]


def gather_plan(shards):
    plan = []
    for w in (0, 4, 1, 2, 3, 6, 7, 5):
        rows, wide = shards[w].shape[0] // 4, shards[w].shape[1]
        rest = (wide // 3 + 64) // 128 * 128
        parts = 1 if wide == shards[w].shape[0] * 8 else 2
        for part in range(parts):
            r0, rn = part * rows // parts, rows // parts
            plan.append((w, r0, rn, 0, wide - rest, True))
            plan.append((w, r0, rn, wide - rest, rest, False))
    return plan


def every_weight(tuned, gains, shards, tokens, seen, live, heads):
    if tuned:
        packed = jnp.pad(jnp.stack(gains), ((0, 12), (0, 0)))
        full, norms, attended = gather_and_attend(
            list(shards), packed, tokens, seen, live, heads, gather_plan(shards), 1
        )
        return tuple(norms[:, i, :].reshape(-1) for i in range(4)) + tuple(full), attended
    full = tuple(lax.all_gather(v, "tok", axis=0, tiled=True) for v in gains + shards)
    target_in = layer_norm(tokens.astype(F32), full[0].astype(F32)).astype(BF)
    target_attn = attn_fwd(product(target_in, full[4]).astype(BF), heads, want_lse=False)[0]
    context_in = layer_norm(seen.astype(F32), full[2].astype(F32)).astype(BF)
    context_mixed = product(context_in, full[8]).astype(BF)
    count = jnp.sum(live, axis=0)
    context_attn, context_lse = attn_fwd(context_mixed, heads, count)
    return full, (target_attn, context_in, context_mixed, context_attn, context_lse)


def every_grad(tuned, context, predict):
    if not tuned:
        parts = [lax.psum_scatter(v, "tok", scatter_dimension=0, tiled=True) for v in context]
        return (
            tuple(lax.psum(v.astype(jnp.bfloat16), "head").astype(jnp.float32) for v in parts),
            lax.psum(predict, ("tok", "head")),
        )
    entry, mask, prenorm, project, outward, midnorm, expand, shrink, endnorm, leave = predict
    model_width, width = entry.shape
    wide = jnp.concatenate([project, outward, expand, leave], axis=1).astype(BF)
    blocks = wide.shape[1] // model_width
    wide = jnp.concatenate(
        [wide[:, i * model_width : (i + 1) * model_width] for i in range(blocks)], axis=0
    )
    tall = jnp.concatenate([entry, shrink], axis=0).astype(BF)
    small = (mask, prenorm, midnorm, endnorm, context[0], context[3])
    line = jnp.concatenate(small)
    vector = jnp.pad(line, (0, -line.shape[0] % 1024)).reshape(-1, 128)
    grads = [context[1], context[2], context[4], context[5]]
    grads = [v.astype(BF) for v in grads] + [wide, tall]
    piece = [v.shape[0] // 32 for v in grads]
    plan = [(4, 0, piece[4], "yx", True, 4), (5, 0, piece[5], "xy", True, 4)]
    for w in (1, 0, 2, 3):
        half = piece[w] // 2
        plan += [(w, 0, half, "xy", False, w), (w, half, half, "yx", False, w)]
    sums, vector = reduce_grads(grads, vector, plan, 2)
    sums = [v.astype(F32) for v in sums]
    line = vector.reshape(-1)
    lines = []
    for v in small:
        lines.append(line[: v.shape[0]])
        line = line[v.shape[0] :]
    share = model_width // lax.axis_size("tok")
    mine = lambda v: lax.dynamic_slice_in_dim(v, lax.axis_index("tok") * share, share)
    wide = jnp.concatenate(
        [sums[4][i * width : (i + 1) * width] for i in range(blocks)], axis=1
    )
    cuts = [0]
    for v in (project, outward, expand, leave):
        cuts.append(cuts[-1] + v.shape[1])
    project, outward, expand, leave = (wide[:, a:b] for a, b in zip(cuts, cuts[1:]))
    return (
        (mine(lines[4]), sums[0], sums[1], mine(lines[5]), sums[2], sums[3]),
        (
            sums[5][:model_width],
            lines[0],
            lines[1],
            project,
            outward,
            lines[2],
            expand,
            sums[5][model_width:],
            lines[3],
            leave,
        ),
    )


def ffn_kernel(mid_ref, gain_ref, expand_ref, shrink_ref, out_ref, normed_ref, sum_ref):
    step = pl.program_id(0)

    @pl.when(step == 0)
    def _():
        normed_ref[...] = layer_norm(mid_ref[...], gain_ref[...]).astype(BF)
        sum_ref[...] = mid_ref[...]

    active = jax.nn.gelu(dot(normed_ref[...], expand_ref[...])).astype(BF)
    sum_ref[...] += dot(active, shrink_ref[...])

    @pl.when(step == pl.num_programs(0) - 1)
    def _():
        out_ref[...] = plain_norm(sum_ref[...])


def target_ffn(mid_rows, gain, expand, shrink, block=1024):
    length, width = mid_rows.shape
    hidden = expand.shape[1]
    whole = pl.BlockSpec((length, width), lambda j: (0, 0))
    return pl.pallas_call(
        ffn_kernel,
        grid=(hidden // block,),
        in_specs=[
            whole,
            pl.BlockSpec((1, width), lambda j: (0, 0)),
            pl.BlockSpec((width, block), lambda j: (0, j)),
            pl.BlockSpec((block, width), lambda j: (j, 0)),
        ],
        out_specs=whole,
        out_shape=jax.ShapeDtypeStruct((length, width), F32),
        scratch_shapes=[pltpu.VMEM((length, width), BF), pltpu.VMEM((length, width), F32)],
        compiler_params=pltpu.CompilerParams(vmem_limit_bytes=60 << 20),
        cost_estimate=pl.CostEstimate(
            flops=4 * length * width * hidden,
            bytes_accessed=8 * length * width + 4 * width * hidden,
            transcendentals=length * hidden,
        ),
        name="target_ffn",
    )(mid_rows, gain.reshape(1, -1), expand, shrink)


def feed_forward(mid_rows, midnorm, expand, shrink):
    mid_wide = mid_rows.astype(jnp.float32)
    normed = layer_norm(mid_wide, midnorm).astype(jnp.bfloat16)
    raised = product(normed, expand)
    active = jax.nn.gelu(raised).astype(jnp.bfloat16)
    output = (mid_wide + product(active, shrink)).astype(jnp.bfloat16)
    return (output, (mid_wide, normed, raised, active))


def feed_forward_back(grad_rows, saved, midnorm, expand, shrink):
    mid_wide, normed, raised, active = saved
    grad_shrink = inner_rows(active, grad_rows)
    grad_active = inner_cols(grad_rows, shrink)
    unused, gelu_pullback = jax.vjp(jax.nn.gelu, raised)
    grad_raised = gelu_pullback(grad_active)[0].astype(jnp.bfloat16)
    grad_expand = inner_rows(normed, grad_raised)
    grad_normed = inner_cols(grad_raised, expand)
    unused, norm_pullback = jax.vjp(layer_norm, mid_wide, midnorm)
    grad_mid, grad_midnorm = norm_pullback(grad_normed)
    grad_total = (grad_rows.astype(jnp.float32) + grad_mid).astype(jnp.bfloat16)
    return (grad_total, (grad_midnorm, grad_expand, grad_shrink))


def shards(
    tokens,
    target_prenorm,
    target_project,
    target_outward,
    target_midnorm,
    target_expand,
    target_shrink,
    context_prenorm,
    context_project,
    context_outward,
    context_midnorm,
    context_expand,
    context_shrink,
    predict_entry,
    mask_token,
    predict_prenorm,
    predict_project,
    predict_outward,
    predict_midnorm,
    predict_expand,
    predict_shrink,
    predict_endnorm,
    predict_exit,
    clip_order,
    visible_count,
):
    clips_here = clip_order.shape[0]
    clip_len = clip_order.shape[1]
    model_width = tokens.shape[1]
    head_devices = lax.axis_size("head")
    lane_index = lax.axis_index("tok")
    head_index = lax.axis_index("head")
    device_index = lane_index * head_devices + head_index
    counts_here = lax.dynamic_slice_in_dim(visible_count, device_index * clips_here, clips_here)
    tuned = lax.axis_size("tok") == 8 and head_devices == 4
    visible_pos = clip_order[:, :VMOST]
    slot_live = jnp.arange(VMOST, dtype=jnp.int32)[None, :] < counts_here[:, None]
    holds = visible_pos[:, :, None] == jnp.arange(clip_len, dtype=jnp.int32)[None, None, :]
    holds = jnp.logical_and(holds, slot_live[:, :, None])
    visible = jnp.any(holds, axis=1)
    slot = jnp.arange(VMOST, dtype=jnp.int32)[None, :, None]
    order_rank = jnp.sum(jnp.where(holds, slot, 0), axis=1)
    token_grid = tokens.reshape(clips_here, clip_len, model_width)
    seen_rows = jnp.einsum(
        "csl,cld->csd", holds.astype(BF), token_grid, preferred_element_type=jnp.float32
    )
    seen_rows = seen_rows.reshape(clips_here * VMOST, model_width)
    seen_low = seen_rows.astype(BF)
    live_column = slot_live.astype(jnp.int32).reshape(-1, 1)
    weights, attended = every_weight(
        tuned,
        (target_prenorm, target_midnorm, context_prenorm, context_midnorm),
        (
            target_project,
            target_outward,
            target_expand,
            target_shrink,
            context_project,
            context_outward,
            context_expand,
            context_shrink,
        ),
        tokens,
        seen_low,
        live_column,
        H,
    )
    target_attn, context_in, context_mixed, context_attn, context_lse = attended
    (
        tgt_prenorm_full,
        tgt_midnorm_full,
        ctx_prenorm_full,
        ctx_midnorm_full,
        tgt_project_full,
        tgt_outward_full,
        tgt_expand_full,
        tgt_shrink_full,
        ctx_project_full,
        ctx_outward_full,
        ctx_expand_full,
        ctx_shrink_full,
    ) = weights
    tokens_wide = tokens.astype(jnp.float32)
    target_mid = tokens_wide + product(target_attn, tgt_outward_full)
    target_out = target_ffn(
        target_mid, tgt_midnorm_full.astype(jnp.float32), tgt_expand_full, tgt_shrink_full
    )
    ctx_prenorm_wide = ctx_prenorm_full.astype(jnp.float32)
    ctx_midnorm_wide = ctx_midnorm_full.astype(jnp.float32)
    context_mid = (seen_rows + product(context_attn, ctx_outward_full)).astype(jnp.bfloat16)
    context_out, ffn_saved = feed_forward(
        context_mid, ctx_midnorm_wide, ctx_expand_full, ctx_shrink_full
    )
    entry_rows = product(context_out, predict_entry).reshape(clips_here, VMOST, -1)
    placed = jnp.take_along_axis(entry_rows, order_rank[:, :, None], axis=1)
    start_rows = jnp.where(
        visible[:, :, None], placed, mask_token.astype(jnp.float32)[None, None, :]
    )
    start_rows = (start_rows + positions(clip_len, PD)[None]).reshape(clips_here * clip_len, PD)
    pred_prenorm_wide = predict_prenorm.astype(jnp.float32)
    pred_midnorm_wide = predict_midnorm.astype(jnp.float32)
    pred_endnorm_wide = predict_endnorm.astype(jnp.float32)
    predict_in = layer_norm(start_rows, pred_prenorm_wide).astype(jnp.bfloat16)
    predict_mixed = product(predict_in, predict_project).astype(jnp.bfloat16)
    predict_attn, predict_lse = attn_fwd(predict_mixed, PH)
    branch_rows = start_rows + product(predict_attn, predict_outward)
    predict_normed = layer_norm(branch_rows, pred_midnorm_wide).astype(jnp.bfloat16)
    predict_raised = product(predict_normed, predict_expand)
    predict_active = jax.nn.gelu(predict_raised).astype(jnp.bfloat16)
    final_rows = branch_rows + product(predict_active, predict_shrink)
    final_in = layer_norm(final_rows, pred_endnorm_wide).astype(jnp.bfloat16)
    predicted = product(final_in, predict_exit)
    differ = predicted - target_out
    hidden_rows = jnp.logical_not(visible).reshape(-1)
    row_error = jnp.mean(smooth_error(differ), axis=1)
    clip_sums = jnp.sum(
        jnp.where(hidden_rows, row_error, 0.0).reshape(clips_here, clip_len), axis=1
    )
    clip_loss = clip_sums / (clip_len - counts_here).astype(jnp.float32)
    slope = jnp.clip(differ / HUBER, -1.0, 1.0)
    grad_predicted = (jnp.where(hidden_rows[:, None], slope, 0.0) / model_width).astype(
        jnp.bfloat16
    )
    grad_exit = inner_rows(final_in, grad_predicted)
    grad_final_in = inner_cols(grad_predicted, predict_exit)
    unused, norm_pullback = jax.vjp(layer_norm, final_rows, pred_endnorm_wide)
    grad_final, grad_endnorm = norm_pullback(grad_final_in)
    grad_second = grad_final.astype(jnp.bfloat16)
    grad_pred_shrink = inner_rows(predict_active, grad_second)
    grad_pred_active = inner_cols(grad_second, predict_shrink)
    unused, gelu_pullback = jax.vjp(jax.nn.gelu, predict_raised)
    grad_pred_raised = gelu_pullback(grad_pred_active)[0].astype(jnp.bfloat16)
    grad_pred_expand = inner_rows(predict_normed, grad_pred_raised)
    grad_pred_normed = inner_cols(grad_pred_raised, predict_expand)
    unused, norm_pullback = jax.vjp(layer_norm, branch_rows, pred_midnorm_wide)
    grad_branch_norm, grad_pred_midnorm = norm_pullback(grad_pred_normed)
    grad_branch = grad_final + grad_branch_norm
    grad_first = grad_branch.astype(jnp.bfloat16)
    grad_pred_outward = inner_rows(predict_attn, grad_first)
    grad_pred_attn = inner_cols(grad_first, predict_outward).astype(jnp.bfloat16)
    grad_pred_mixed = attn_bwd(predict_mixed, predict_attn, predict_lse, grad_pred_attn, PH)
    grad_pred_project = inner_rows(predict_in, grad_pred_mixed)
    grad_pred_in = inner_cols(grad_pred_mixed, predict_project)
    unused, norm_pullback = jax.vjp(layer_norm, start_rows, pred_prenorm_wide)
    grad_start_norm, grad_pred_prenorm = norm_pullback(grad_pred_in)
    grad_start = (grad_branch + grad_start_norm).reshape(clips_here, clip_len, PD)
    grad_mask = jnp.sum(jnp.where(visible[:, :, None], 0.0, grad_start), axis=(0, 1))
    grad_entry_rows = jnp.take_along_axis(grad_start, visible_pos[:, :, None], axis=1)
    grad_entry_rows = jnp.where(slot_live[:, :, None], grad_entry_rows, 0.0)
    grad_entry_rows = grad_entry_rows.reshape(clips_here * VMOST, PD).astype(jnp.bfloat16)
    grad_entry = inner_rows(context_out, grad_entry_rows)
    grad_context_out = inner_cols(grad_entry_rows, predict_entry).astype(jnp.bfloat16)
    back_project, back_outward = ctx_project_full, ctx_outward_full
    back_expand, back_shrink = ctx_expand_full, ctx_shrink_full
    back_prenorm_wide, back_midnorm_wide = ctx_prenorm_wide, ctx_midnorm_wide
    grad_mid, ffn_grads = feed_forward_back(
        grad_context_out, ffn_saved, back_midnorm_wide, back_expand, back_shrink
    )
    grad_ctx_outward = inner_rows(context_attn, grad_mid)
    grad_ctx_attn = inner_cols(grad_mid, back_outward).astype(jnp.bfloat16)
    grad_ctx_mixed = attn_bwd(
        context_mixed, context_attn, context_lse, grad_ctx_attn, H, counts_here
    )
    grad_ctx_project = inner_rows(context_in, grad_ctx_mixed)
    grad_ctx_in = inner_cols(grad_ctx_mixed, back_project)
    unused, norm_pullback = jax.vjp(layer_norm, seen_rows, back_prenorm_wide)
    grad_seen_norm, grad_ctx_prenorm = norm_pullback(grad_ctx_in)
    grad_seen = (grad_mid.astype(jnp.float32) + grad_seen_norm).reshape(
        clips_here, VMOST, model_width
    )
    grad_grid = jnp.take_along_axis(
        grad_seen, order_rank[:, :, None], axis=1
    )
    tokens_grad = jnp.where(visible[:, :, None], grad_grid, 0.0).reshape(
        clips_here * clip_len, model_width
    )
    context_sums, predict_sums = every_grad(
        tuned,
        (
            grad_ctx_prenorm,
            grad_ctx_project,
            grad_ctx_outward,
            ffn_grads[0],
            ffn_grads[1],
            ffn_grads[2],
        ),
        (
            grad_entry,
            grad_mask,
            grad_pred_prenorm,
            grad_pred_project,
            grad_pred_outward,
            grad_pred_midnorm,
            grad_pred_expand,
            grad_pred_shrink,
            grad_endnorm,
            grad_exit,
        ),
    )
    return (
        clip_loss,
        tokens_grad,
        context_sums[0],
        context_sums[1],
        context_sums[2],
        context_sums[3],
        context_sums[4],
        context_sums[5],
        predict_sums[0],
        predict_sums[1],
        predict_sums[2],
        predict_sums[3],
        predict_sums[4],
        predict_sums[5],
        predict_sums[6],
        predict_sums[7],
        predict_sums[8],
        predict_sums[9],
    )


def solution(mesh):
    return jax.shard_map(
        shards,
        mesh=mesh,
        in_specs=(
            P(("tok", "head"), None),
            P("tok"),
            P("tok", None),
            P("tok", None),
            P("tok"),
            P("tok", None),
            P("tok", None),
            P("tok"),
            P("tok", None),
            P("tok", None),
            P("tok"),
            P("tok", None),
            P("tok", None),
            P(),
            P(),
            P(),
            P(),
            P(),
            P(),
            P(),
            P(),
            P(),
            P(),
            P(("tok", "head"), None),
            P(),
        ),
        out_specs=(
            P(("tok", "head")),
            P(("tok", "head"), None),
            P("tok"),
            P("tok", None),
            P("tok", None),
            P("tok"),
            P("tok", None),
            P("tok", None),
            P(),
            P(),
            P(),
            P(),
            P(),
            P(),
            P(),
            P(),
            P(),
            P(),
        ),
        check_vma=False,
    )
```

```python
import functools

import jax
import jax.numpy as jnp
from jax import lax
from jax.experimental import pallas as pl
from jax.experimental.pallas import tpu as pltpu
from jax.sharding import PartitionSpec as P

H = 16
PD = 384
PH = 12
VMOST = 464


EPSILON = 1e-06
HUBER = 0.25


def layer_norm(values, gains):
    center = values - jnp.mean(values, axis=-1, keepdims=True)
    spread = jnp.mean(center * center, axis=-1, keepdims=True)
    return center * lax.rsqrt(spread + EPSILON) * gains


def plain_norm(values):
    center = values - jnp.mean(values, axis=-1, keepdims=True)
    spread = jnp.mean(center * center, axis=-1, keepdims=True)
    return center * lax.rsqrt(spread + EPSILON)


def smooth_error(differ):
    magnitude = jnp.abs(differ)
    return jnp.where(magnitude < HUBER, 0.5 * differ * differ / HUBER, magnitude - 0.5 * HUBER)


def positions(length, breadth, block=32):
    half_width = breadth // 2
    freqs = jnp.exp(-jnp.log(10000.0) * jnp.arange(half_width, dtype=jnp.float32) / half_width)
    coarse = jnp.arange(0, length, block, dtype=jnp.float32)[:, None, None] * freqs
    fine = jnp.arange(block, dtype=jnp.float32)[None, :, None] * freqs
    sines = lax.optimization_barrier((jnp.sin(coarse), jnp.cos(coarse), jnp.sin(fine), jnp.cos(fine)))
    sin_far, cos_far, sin_near, cos_near = sines
    table = jnp.concatenate(
        [sin_far * cos_near + cos_far * sin_near, cos_far * cos_near - sin_far * sin_near], axis=2
    )
    return table.reshape(-1, breadth)[:length]


def product(former, latter):
    return jnp.dot(former, latter, preferred_element_type=jnp.float32)


def inner_rows(former, latter):
    return lax.dot_general(
        former, latter, (((0,), (0,)), ((), ())), preferred_element_type=jnp.float32
    )


def inner_cols(former, latter):
    return lax.dot_general(
        former, latter, (((1,), (1,)), ((), ())), preferred_element_type=jnp.float32
    )


BF=jnp.bfloat16; F32=jnp.float32
LOG2E=1.4426950408889634
NT=(((1,),(1,)),((),())); NN=(((1,),(0,)),((),()))
def dot(a,b,dims=NN): return lax.dot_general(a,b,dims,preferred_element_type=F32)
def chunks(n,step):
    return [(i,min(step,n-i)) for i in range(0,n,step)]
def lane_mask(rows,h,e):
    lane=lax.broadcasted_iota(jnp.int32,(rows,128),1)
    return (lane>=h*e)&(lane<(h+1)*e)
def head_rows(values,h,e):
    return jnp.where(lane_mask(values.shape[0],h,e),values,jnp.zeros_like(values))

def attend_group(q_all,k,v,e,live,step):
    L=q_all.shape[0]; per=128//e; c=e**-0.5*LOG2E
    vt=v.T
    results=[]; sums=[]
    for (s0,n) in chunks(L,step):
        outs=[]; lses=[]
        for h in range(per):
            q=head_rows(q_all[s0:s0+n,:],h,e)
            st=dot(k,q,NT)
            if live is not None: st=jnp.where(live,st,-1e30)
            m=jnp.max(st,axis=0,keepdims=True)
            p=jnp.exp2((st-m)*c)
            l=jnp.sum(p,axis=0,keepdims=True)
            outs.append(dot(vt[h*e:(h+1)*e,:],p.astype(BF))*(1.0/l))
            lses.append(m*c+jnp.log2(l))
        results.append(jnp.concatenate(outs,axis=0).T.astype(BF))
        sums.append(jnp.concatenate(lses,axis=0))
    if len(results)==1: return results[0],sums[0]
    return jnp.concatenate(results,axis=0),jnp.concatenate(sums,axis=1)

def fwd_kernel(e,step,masked,want_lse,*refs):
    refs=list(refs)
    count=refs.pop(0) if masked else None
    q_ref,k_ref,v_ref,o_ref=refs[:4]
    L=q_ref.shape[0]
    live=lax.broadcasted_iota(jnp.int32,(L,1),0)<count[0] if masked else None
    o_ref[...],lse=attend_group(q_ref[...],k_ref[...],v_ref[...],e,live,step)
    if want_lse: refs[4][0]=lse

def attn_fwd(mixed,heads,count=None,step=1280,want_lse=True):
    L,w3=mixed.shape; Dm=w3//3; e=Dm//heads; G=Dm//128; per=128//e
    masked=count is not None
    spec=lambda off: pl.BlockSpec((L,128),lambda g,*_:(0,off+g))
    out_shape=[jax.ShapeDtypeStruct((L,Dm),BF)]; out_specs=[pl.BlockSpec((L,128),lambda g,*_:(0,g))]
    if want_lse:
        out_shape.append(jax.ShapeDtypeStruct((G,per,L),F32)); out_specs.append(pl.BlockSpec((1,per,L),lambda g,*_:(g,0,0)))
    gs=pltpu.PrefetchScalarGridSpec(num_scalar_prefetch=1 if masked else 0,grid=(G,),in_specs=[spec(0),spec(G),spec(2*G)],out_specs=out_specs)
    flops=4*heads*L*L*e
    f=pl.pallas_call(functools.partial(fwd_kernel,e,step,masked,want_lse),grid_spec=gs,out_shape=out_shape,
        compiler_params=pltpu.CompilerParams(vmem_limit_bytes=56<<20),
        cost_estimate=pl.CostEstimate(flops=flops,bytes_accessed=L*Dm*8,transcendentals=heads*L*L),name="attn_fwd")
    return f(*((count,) if masked else ()),mixed,mixed,mixed)

def bwd_kernel(e,step,masked,*refs):
    refs=list(refs)
    count=refs.pop(0) if masked else None
    q_ref,k_ref,v_ref,o_ref,do_ref,lse_ref,g_ref,dk_ref,dv_ref=refs
    L=q_ref.shape[0]; per=128//e; c=e**-0.5*LOG2E; f=e**-0.5
    g=pl.program_id(0); G=pl.num_programs(0)
    k=k_ref[...]; v=v_ref[...]
    kt=k.T
    live=None
    if masked:
        live=lax.broadcasted_iota(jnp.int32,(L,1),0)<count[0]
    dk_ref[...]=jnp.zeros_like(dk_ref); dv_ref[...]=jnp.zeros_like(dv_ref)
    cols=lambda part: pl.ds(pl.multiple_of((part*G+g)*128,128),128)
    for (s0,n) in chunks(L,step):
        do_all=do_ref[s0:s0+n,:]; q_all=q_ref[s0:s0+n,:]
        prod=(do_all.astype(F32)*o_ref[s0:s0+n,:].astype(F32)).T
        dqs=[]
        for h in range(per):
            q=head_rows(q_all,h,e); do=head_rows(do_all,h,e)
            delta=jnp.sum(prod[h*e:(h+1)*e,:],axis=0,keepdims=True)
            st=dot(k,q,NT)
            p=jnp.exp2(st*c-lse_ref[0,h:h+1,s0:s0+n])
            if masked: p=jnp.where(live,p,0.0)
            dp=dot(v,do,NT)
            ds=(p*(dp-delta)).astype(BF)
            dv_ref[...]+=dot(p.astype(BF),do)
            dk_ref[...]+=dot(ds,q)
            dqs.append(dot(kt[h*e:(h+1)*e,:],ds))
        g_ref[s0:s0+n,cols(0)]=(jnp.concatenate(dqs,axis=0)*f).T.astype(BF)
    g_ref[:,cols(1)]=(dk_ref[...]*f).astype(BF)
    g_ref[:,cols(2)]=dv_ref[...].astype(BF)

def attn_bwd(mixed,o,lse,do,heads,count=None,step=256):
    L,w3=mixed.shape; Dm=w3//3; e=Dm//heads; G=Dm//128; per=128//e
    masked=count is not None
    spec=lambda off: pl.BlockSpec((L,128),lambda g,*_:(0,off+g))
    gs=pltpu.PrefetchScalarGridSpec(num_scalar_prefetch=1 if masked else 0,grid=(G,),
        in_specs=[spec(0),spec(G),spec(2*G),spec(0),spec(0),pl.BlockSpec((1,per,L),lambda g,*_:(g,0,0))],
        out_specs=pl.BlockSpec((L,w3),lambda g,*_:(0,0)),
        scratch_shapes=[pltpu.VMEM((L,128),F32)]*2)
    return pl.pallas_call(functools.partial(bwd_kernel,e,step,masked),grid_spec=gs,out_shape=jax.ShapeDtypeStruct((L,w3),BF),
        compiler_params=pltpu.CompilerParams(vmem_limit_bytes=56<<20),
        cost_estimate=pl.CostEstimate(flops=10*heads*L*L*e,bytes_accessed=L*Dm*16,transcendentals=heads*L*L),name="attn_bwd")(*((count,) if masked else ()),mixed,mixed,mixed,o,do,lse)


MESH = pl.DeviceIdType.MESH
ANY = pl.BlockSpec(memory_space=pl.ANY)

def place():
    tok=lax.axis_index("tok"); head=lax.axis_index("head")
    return tok//2, tok%2, head//2, head%2

def peer(z,y,x,c): return (z*2+y, x*2+c)

def greet(barrier_peers):
    barrier=pltpu.get_barrier_semaphore()
    for p in barrier_peers:
        pl.semaphore_signal(barrier,inc=1,device_id=p,device_id_type=MESH)
    pl.semaphore_wait(barrier,len(barrier_peers))

def gather_steps(shard, full, own, cut, quarter, local, send, recv):
    z,y,x,c=place()
    xs = x if quarter else slice(None)
    rows, cols = cut
    def rcopy(i,src,dst,dev):
        return pltpu.make_async_remote_copy(src_ref=src,dst_ref=dst,send_sem=send.at[i],recv_sem=recv.at[i],device_id=dev,device_id_type=MESH)
    mine=shard.at[xs,c,rows,cols]
    def load(): return pltpu.make_async_copy(mine,own,local.at[0])
    def put(): return pltpu.make_async_copy(own,full.at[z,y,xs,c,rows,cols],local.at[1])
    def zc(k,out):
        dst=full.at[z,y,xs,c,rows,cols] if out else full.at[(z+4-k)%4,y,xs,c,rows,cols]
        return rcopy(k-1,mine,dst,peer((z+k)%4,y,x,c))
    def yc(out):
        yy=y if out else 1-y
        return rcopy(3,full.at[:,y,xs,c,rows,cols],full.at[:,yy,xs,c,rows,cols],peer(z,1-y,x,c))
    def xc(out):
        xx=x if out else 1-x
        return rcopy(4,full.at[:,:,x,c,rows,cols],full.at[:,:,xx,c,rows,cols],peer(z,y,1-x,c))
    def cc(out):
        cz=c if out else 1-c
        return rcopy(5,full.at[:,:,:,c,rows,cols],full.at[:,:,:,cz,rows,cols],peer(z,y,x,1-c))
    def s0():
        load().start()
        for k in (2,1,3): zc(k,True).start()
    def s1():
        load().wait(); put().start()
        for k in (1,2,3): zc(k,False).wait_recv()
        put().wait()
        yc(True).start()
    def s2():
        yc(False).wait_recv()
        if quarter: xc(True).start()
        else: cc(True).start()
    def s3():
        if quarter:
            xc(False).wait_recv(); cc(True).start()
    def s4():
        cc(False).wait_recv()
        for k in (1,2,3): zc(k,True).wait_send()
        yc(True).wait_send()
        if quarter: xc(True).wait_send()
        cc(True).wait_send()
    return [s0,s1,s2,s3,s4]

def gains_steps(src,out,send,recv):
    z,y,x,c=place()
    def cp(k,outgoing):
        dz,dy=k//2,k%2
        t=z*2+y
        pz=(z+dz)%4; py=(y+dy)%2
        sz=(z+4-dz)%4; sy=(y+2-dy)%2
        dst=out.at[t] if outgoing else out.at[sz*2+sy]
        return pltpu.make_async_remote_copy(src_ref=src,dst_ref=dst,send_sem=send.at[k-1],recv_sem=recv.at[k-1],device_id=peer(pz,py,x,c),device_id_type=MESH)
    def start():
        for k in range(1,8): cp(k,True).start()
    def finish():
        for k in range(1,8): cp(k,False).wait_recv()
        for k in range(1,8): cp(k,True).wait_send()
    return start,finish

def everyone_on_tok():
    z,y,x,c=place()
    peers=[peer((z+k//2)%4,(y+k%2)%2,x,c) for k in range(1,8)]
    return peers+[peer(z,y,1-x,c),peer(z,y,x,1-c)]

def together(members):
    def stage(s):
        def run():
            for m in members: m[s]()
        return run
    return [stage(s) for s in range(len(members[0]))]

def interleave(chunks):
    n=len(chunks); depth=len(chunks[0])
    order=[]
    for t in range(n+depth-1):
        for s in range(depth):
            i=t-s
            if 0<=i<n: order.append(chunks[i][s])
    return order

def by_turn(chunks):
    turns=[[] for _ in range(len(chunks)+len(chunks[0])-1)]
    for i,chunk in enumerate(chunks):
        for s,stage in enumerate(chunk): turns[i+s].append((s,stage))
    return [[stage for _,stage in sorted(t,key=lambda p:p[0])] for t in turns]

def scaled_norm(values,gain_blocks,row,out_ref):
    normed=plain_norm(values.astype(F32))
    for t in range(gain_blocks.shape[0]):
        cols=slice(t*128,(t+1)*128)
        out_ref[:,cols]=(normed[:,cols]*gain_blocks[t,row:row+1,:].astype(F32)).astype(BF)

def ag_kernel(plan,n,heads,*refs):
    shards=refs[:n]; gain,tok_ref,seen_ref,live_ref=refs[n:n+4]
    fulls=refs[n+4:2*n+4]; gout,tout,cin,cmixed,cattn,clse=refs[2*n+4:2*n+10]
    rest=refs[2*n+10:]
    k=len(plan)
    owns=rest[:k]; gown,local,send,recv,gsend,grecv,glocal,gv,tin,tattn,total,pw,ow,ew,sw,wsem=rest[k:]
    z,y,x,c=place()
    turn=pl.program_id(0)
    steps=[]
    for i,(w,r0,rn,c0,cn,quarter) in enumerate(plan):
        steps.append(gather_steps(shards[w],fulls[w],owns[i],(pl.ds(r0,rn),pl.ds(c0,cn)),quarter,local.at[i],send.at[i],recv.at[i]))
    groups={}
    for st,entry in zip(steps,plan): groups.setdefault(entry[:3],[]).append(st)
    turns=by_turn([together(m) for m in groups.values()])
    done={w:i+len(steps[0])-1 for i,(w,_,_) in enumerate(groups)}
    gs,gf=gains_steps(gain,gout,gsend,grecv)
    width=tok_ref.shape[1]; G=width//128; e=width//heads
    first=done[0]+1; outward=first+G//2; dense=done[3]+1; end=len(turns)-1
    blocks=8//(end-dense); block_width=ew.shape[-1]
    assert done[1]<outward and done[4]<outward and done[2]<dense and outward+G==end+1
    take=lambda w,dst,i: pltpu.make_async_copy(fulls[w],dst,wsem.at[i])
    def take_block(j):
        b=(turn-dense)*blocks+j
        cols=pl.ds(pl.multiple_of(b*block_width,128),block_width)
        return (pltpu.make_async_copy(fulls[2].at[:,:,:,:,:,cols],ew.at[j],wsem.at[2+2*j]),
                pltpu.make_async_copy(fulls[3].at[b//2,b%2],sw.at[j],wsem.at[3+2*j]))
    for t,fs in enumerate(turns):
        @pl.when(turn==t)
        def _(t=t,fs=fs):
            if t==0: greet(everyone_on_tok())
            if t==first: take(0,pw,0).start()
            if t==outward:
                take(4,pw,0).start(); take(1,ow,1).start()
            for f in fs: f()
            if t==0:
                gs()
                g0=pltpu.make_async_copy(gain,gown,glocal.at[0]); g0.start(); g0.wait()
                pltpu.make_async_copy(gown,gout.at[z*2+y],glocal.at[1]).start()
            if t==2:
                pltpu.make_async_copy(gown,gout.at[z*2+y],glocal.at[1]).wait()
                gf()
                g2=pltpu.make_async_copy(gout,gv,glocal.at[2]); g2.start(); g2.wait()
            if t==3: scaled_norm(tok_ref[...],gv,0,tin)
            if t==4: scaled_norm(seen_ref[...],gv,2,cin)
            if t==first: take(0,pw,0).wait()
            if t==outward:
                take(4,pw,0).wait(); take(1,ow,1).wait()
                total[...]=tok_ref[...].astype(F32)+dot(tattn[...],ow[...].reshape(width,width))
                scaled_norm(total[...],gv,1,tin)
    def block(part,g): return pw[:,:,:,:,:,pl.ds(pl.multiple_of((part*G+g)*128,128),128)].reshape(width,128)
    @pl.when((turn>=first)&(turn<outward))
    def _():
        @pl.loop(0,2)
        def _(j):
            g=(turn-first)*2+j
            q,key,v=[dot(tin[...],block(part,g)).astype(BF) for part in range(3)]
            o,_=attend_group(q,key,v,e,None,1280)
            tattn[:,pl.ds(pl.multiple_of(g*128,128),128)]=o
    @pl.when(turn>=outward)
    def _():
        g=turn-outward
        parts=[dot(cin[...],block(part,g)).astype(BF) for part in range(3)]
        for part in range(3):
            cmixed[:,pl.ds(pl.multiple_of((part*G+g)*128,128),128)]=parts[part]
        o,lse=attend_group(*parts,e,live_ref[...]!=0,1280)
        cattn[:,pl.ds(pl.multiple_of(g*128,128),128)]=o
        clse[g]=lse
    @pl.when((turn>=dense)&(turn<end))
    def _():
        for j in range(blocks):
            for copy in take_block(j): copy.start()
        for j in range(blocks):
            for copy in take_block(j): copy.wait()
            active=jax.nn.gelu(dot(tin[...],ew[j].reshape(width,block_width))).astype(BF)
            total[...]+=dot(active,sw[j].reshape(block_width,width))
    @pl.when(turn==end)
    def _():
        total[...]=plain_norm(total[...])
        put=pltpu.make_async_copy(total,tout,wsem.at[0]); put.start(); put.wait()

def gather_and_attend(shards,gains,tokens,seen,live,heads,plan,cid):
    n=len(shards); k=len(plan)
    views=[s.reshape(2,2,s.shape[0]//4,s.shape[1]) for s in shards]
    outs=[jax.ShapeDtypeStruct((4,2,2,2,s.shape[0]//4,s.shape[1]),s.dtype) for s in shards]
    outs.append(jax.ShapeDtypeStruct((8,)+gains.shape,gains.dtype))
    (L,width),slots=tokens.shape,seen.shape[0]
    G=width//128
    extra=[((L,width),F32),((slots,width),BF),((slots,3*width),BF),((slots,width),BF),((G,heads//G,slots),F32)]
    outs+=[jax.ShapeDtypeStruct(s,d) for s,d in extra]
    whole=lambda s: pl.BlockSpec(s,lambda t: (0,)*len(s))
    owns=[pltpu.VMEM(((rn,cn) if q else (2,rn,cn)),BF) for (w,r0,rn,c0,cn,q) in plan]
    S=pltpu.SemaphoreType.DMA
    turns=len({entry[:3] for entry in plan})+4
    scratch=owns+[pltpu.VMEM(gains.shape,BF),S((k,2)),S((k,6)),S((k,6)),S((7,)),S((7,)),S((3,)),
        pltpu.VMEM((8,)+gains.shape,BF),pltpu.VMEM((L,width),BF),pltpu.VMEM((L,width),BF),pltpu.VMEM((L,width),F32),
        pltpu.VMEM(outs[0].shape,BF),pltpu.VMEM(outs[1].shape,BF),
        pltpu.VMEM((2,)+outs[2].shape[:-1]+(outs[2].shape[-1]//8,),BF),pltpu.VMEM((2,)+outs[3].shape[2:],BF),S((6,))]
    res=pl.pallas_call(functools.partial(ag_kernel,plan,n,heads),grid=(turns,),out_shape=outs,
        in_specs=[ANY]*(n+1)+[whole(tokens.shape),whole(seen.shape),whole(live.shape)],
        out_specs=[ANY]*(n+2)+[whole(s) for s,_ in extra[1:]],scratch_shapes=scratch,
        compiler_params=pltpu.CompilerParams(collective_id=cid,has_side_effects=True,vmem_limit_bytes=60<<20),name="gather_and_attend")(*views,gains,tokens,seen,live)
    return [o.reshape(8*s.shape[0],s.shape[1]) for o,s in zip(res[:n],shards)],res[n],res[n+1:]

def reduce_steps(grad, out, rn, rows, bufs, order, everywhere, local, send, recv):
    z,y,x,c=place()
    M,C,A,B,Z,T=bufs
    def rcopy(i,src,dst,dev):
        return pltpu.make_async_remote_copy(src_ref=src,dst_ref=dst,send_sem=send.at[i],recv_sem=recv.at[i],device_id=dev,device_id_type=MESH)
    xfirst=order=="xy"
    side={"x":peer(z,y,1-x,c),"y":peer(z,1-y,x,c)}
    first,second=order
    load=lambda: pltpu.make_async_copy(grad.at[:,:,:,c,rows],M,local.at[0])
    cc=lambda: rcopy(0,grad.at[:,:,:,1-c,rows],C,side_c)
    side_c=peer(z,y,x,1-c)
    ac=lambda: rcopy(1,M.at[:,:,1-x] if xfirst else M.at[:,1-y],A,side[first])
    bc=lambda: rcopy(2,M.at[:,1-y,x] if xfirst else M.at[:,y,1-x],B,side[second])
    zc=lambda k: rcopy(2+k,M.at[(z+k)%4,y,x],Z.at[k-1],peer((z+k)%4,y,x,c))
    def add(target,source):
        target[...]=(target[...].astype(F32)+source[...].astype(F32)).astype(BF)
    def s0():
        cc().start(); load().start()
    def s1():
        load().wait(); cc().wait_recv()
        @pl.loop(0,16)
        def _(i):
            at=(i//4,(i//2)%2,i%2)
            add(M.at[at],C.at[at])
        ac().start()
    def s2():
        ac().wait_recv()
        @pl.loop(0,8)
        def _(i):
            if xfirst: add(M.at[i//2,i%2,x],A.at[i//2,i%2])
            else: add(M.at[i//2,y,i%2],A.at[i//2,i%2])
        bc().start()
    def s3():
        bc().wait_recv()
        @pl.loop(0,4)
        def _(i):
            add(M.at[i,y,x],B.at[i])
        for k in (2,1,3): zc(k).start()
    if everywhere:
        home=out.at[z,y,x,c,rows]
        spread=[]
        for k in (1,2,3):
            spread.append((5+k,lambda o,k=k:(T,out.at[z,y,x,c,rows] if o else out.at[(z+4-k)%4,y,x,c,rows],peer((z+k)%4,y,x,c))))
        sy=(9,lambda o:(out.at[:,y,x,c,rows],out.at[:,y if o else 1-y,x,c,rows],side["y"]))
        sx=(10,lambda o:(out.at[:,:,x,c,rows],out.at[:,:,x if o else 1-x,c,rows],side["x"]))
        if xfirst: stages=[spread,[sy],[sx]]
        else:
            sx=(9,lambda o:(out.at[:,y,x,c,rows],out.at[:,y,x if o else 1-x,c,rows],side["x"]))
            sy=(10,lambda o:(out.at[:,y,:,c,rows],out.at[:,y if o else 1-y,:,c,rows],side["y"]))
            stages=[spread,[sx],[sy]]
        stages.append([(11,lambda o:(out.at[:,:,:,c,rows],out.at[:,:,:,c if o else 1-c,rows],side_c))])
    else:
        home=out.at[x,c,rows]
        stages=[[(6,lambda o:(T,out.at[x if o else 1-x,c,rows],side["x"]))],[(7,lambda o:(out.at[:,c,rows],out.at[:,c if o else 1-c,rows],side_c))]]
    def run(entry,o):
        i,f=entry; src,dst,dev=f(o); return rcopy(i,src,dst,dev)
    put=lambda: pltpu.make_async_copy(T,home,local.at[1])
    def s4():
        for k in (1,2,3): zc(k).wait_recv()
        T[...]=(M[z,y,x].astype(F32)+Z[0].astype(F32)+Z[1].astype(F32)+Z[2].astype(F32)).astype(BF)
        put().start()
        for e in stages[0]: run(e,True).start()
    def later(n):
        def s():
            if n==1: put().wait()
            for e in stages[n-1]: run(e,False).wait_recv()
            for e in stages[n]: run(e,True).start()
        return s
    def last():
        for e in stages[-1]: run(e,False).wait_recv()
        cc().wait_send(); ac().wait_send(); bc().wait_send()
        for k in (1,2,3): zc(k).wait_send()
        for st in stages:
            for e in st: run(e,True).wait_send()
    mids=[later(n) for n in range(1,len(stages))]
    if not everywhere: mids=mids+[lambda:None]*2
    return [s0,s1,s2,s3,s4]+mids+[last]

def vector_steps(src,out,bufs,local,send,recv):
    z,y,x,c=place()
    V,R=bufs
    dev=[peer(z,y,x,1-c),peer(z,y,1-x,c),peer(z,1-y,x,c)]+[peer((z+k)%4,y,x,c) for k in (1,2,3)]
    def rc(i): return pltpu.make_async_remote_copy(src_ref=V.at[min(i,3)],dst_ref=R.at[i],send_sem=send.at[i],recv_sem=recv.at[i],device_id=dev[i],device_id_type=MESH)
    load=lambda: pltpu.make_async_copy(src,V.at[0],local.at[0])
    def s0():
        load().start(); load().wait(); rc(0).start()
    def mid(n):
        def s():
            rc(n-1).wait_recv()
            V[n]=V[n-1]+R[n-1]
            if n<3: rc(n).start()
            else:
                for i in (3,4,5): rc(i).start()
        return s
    def fin():
        for i in (3,4,5): rc(i).wait_recv()
        V[4]=V[3]+R[3]+R[4]+R[5]
        cp=pltpu.make_async_copy(V.at[4],out,local.at[1]); cp.start(); cp.wait()
        for i in range(6): rc(i).wait_send()
    nothing=lambda:None
    return [s0,mid(1),mid(2),mid(3),fin,nothing,nothing,nothing,nothing]

def rs_kernel(plan,n,*refs):
    grads=refs[:n]; vec=refs[n]; outs=refs[n+1:2*n+1]; vout=refs[2*n+1]; rest=refs[2*n+2:]
    k=len(plan)
    bufs=[rest[6*i:6*i+6] for i in range(k)]
    V,R,local,send,recv,vlocal,vsend,vrecv=rest[6*k:]
    z,y,x,c=place()
    greet([peer((z+j)%4,y,x,c) for j in (1,2,3)]+[peer(z,1-y,x,c),peer(z,y,1-x,c),peer(z,y,x,1-c)])
    steps=[reduce_steps(grads[w],outs[w],rn,pl.ds(r0,rn),bufs[i],order,ev,local.at[i],send.at[i],recv.at[i]) for i,(w,r0,rn,order,ev,_) in enumerate(plan)]
    steps.append(vector_steps(vec,vout,(V,R),vlocal,vsend,vrecv))
    groups={}
    for st,entry in zip(steps,plan): groups.setdefault(entry[5],[]).append(st)
    groups[plan[0][5]].append(steps[-1])
    groups=[together(m) for m in groups.values()]
    for st in groups: st[0]()
    for f in interleave([st[1:] for st in groups]): f()

def reduce_grads(grads, vec, plan, cid):
    n=len(grads)
    every={w:ev for w,_,_,_,ev,_ in plan}
    views=[g.reshape(4,2,2,2,g.shape[0]//32,g.shape[1]) for g in grads]
    outs=[jax.ShapeDtypeStruct(v.shape if every[w] else v.shape[2:],BF) for w,v in enumerate(views)]
    outs.append(jax.ShapeDtypeStruct(vec.shape,F32))
    scratch=[]
    for (w,r0,rn,order,ev,_) in plan:
        N=grads[w].shape[1]
        scratch+=[pltpu.VMEM((4,2,2,rn,N),BF),pltpu.VMEM((4,2,2,rn,N),BF),pltpu.VMEM((4,2,rn,N),BF),pltpu.VMEM((4,rn,N),BF),pltpu.VMEM((3,rn,N),BF),pltpu.VMEM((rn,N),BF)]
    k=len(plan)
    S=pltpu.SemaphoreType.DMA
    scratch+=[pltpu.VMEM((5,)+vec.shape,F32),pltpu.VMEM((6,)+vec.shape,F32),S((k,2)),S((k,12)),S((k,12)),S((2,)),S((6,)),S((6,))]
    res=pl.pallas_call(functools.partial(rs_kernel,plan,n),out_shape=outs,in_specs=[ANY]*(n+1),out_specs=[ANY]*(n+1),scratch_shapes=scratch,
        compiler_params=pltpu.CompilerParams(collective_id=cid,has_side_effects=True,vmem_limit_bytes=60<<20),name="reduce_grads")(*views,vec)
    flat=[]
    for w,r in enumerate(res[:n]):
        rows=grads[w].shape[0]
        flat.append(r.reshape(rows if every[w] else rows//8,grads[w].shape[1]))
    return flat,res[n]


def gather_plan(shards):
    plan = []
    for w in (0, 4, 1, 2, 3, 6, 7, 5):
        rows, wide = shards[w].shape[0] // 4, shards[w].shape[1]
        rest = (wide // 3 + 64) // 128 * 128
        parts = 1 if wide == shards[w].shape[0] * 8 else 2
        for part in range(parts):
            r0, rn = part * rows // parts, rows // parts
            plan.append((w, r0, rn, 0, wide - rest, True))
            plan.append((w, r0, rn, wide - rest, rest, False))
    return plan


def every_weight(tuned, gains, shards, tokens, seen, live, heads):
    if tuned:
        packed = jnp.pad(jnp.stack(gains), ((0, 12), (0, 0)))
        full, norms, attended = gather_and_attend(
            list(shards), packed, tokens, seen, live, heads, gather_plan(shards), 1
        )
        return tuple(norms[:, i, :].reshape(-1) for i in range(4)) + tuple(full), attended
    full = tuple(lax.all_gather(v, "tok", axis=0, tiled=True) for v in gains + shards)
    target_in = layer_norm(tokens.astype(F32), full[0].astype(F32)).astype(BF)
    target_attn = attn_fwd(product(target_in, full[4]).astype(BF), heads, want_lse=False)[0]
    target_mid = tokens.astype(F32) + product(target_attn, full[5])
    target_out = target_ffn(target_mid, full[1].astype(F32), full[6], full[7])
    context_in = layer_norm(seen.astype(F32), full[2].astype(F32)).astype(BF)
    context_mixed = product(context_in, full[8]).astype(BF)
    count = jnp.sum(live, axis=0)
    context_attn, context_lse = attn_fwd(context_mixed, heads, count)
    return full, (target_out, context_in, context_mixed, context_attn, context_lse)


def every_grad(tuned, context, predict):
    if not tuned:
        parts = [lax.psum_scatter(v, "tok", scatter_dimension=0, tiled=True) for v in context]
        return (
            tuple(lax.psum(v.astype(jnp.bfloat16), "head").astype(jnp.float32) for v in parts),
            lax.psum(predict, ("tok", "head")),
        )
    entry, mask, prenorm, project, outward, midnorm, expand, shrink, endnorm, leave = predict
    model_width, width = entry.shape
    wide = jnp.concatenate([project, outward, expand, leave], axis=1).astype(BF)
    blocks = wide.shape[1] // model_width
    wide = jnp.concatenate(
        [wide[:, i * model_width : (i + 1) * model_width] for i in range(blocks)], axis=0
    )
    tall = jnp.concatenate([entry, shrink], axis=0).astype(BF)
    small = (mask, prenorm, midnorm, endnorm, context[0], context[3])
    line = jnp.concatenate(small)
    vector = jnp.pad(line, (0, -line.shape[0] % 1024)).reshape(-1, 128)
    grads = [context[1], context[2], context[4], context[5]]
    grads = [v.astype(BF) for v in grads] + [wide, tall]
    piece = [v.shape[0] // 32 for v in grads]
    plan = [(4, 0, piece[4], "yx", True, 4), (5, 0, piece[5], "xy", True, 4)]
    for w in (3, 2, 0, 1):
        parts = 2 if piece[w] >= 64 else 1
        rows = piece[w] // (2 * parts)
        for part in range(parts):
            at, key = 2 * part * rows, (w, part)
            plan += [(w, at, rows, "xy", False, key), (w, at + rows, rows, "yx", False, key)]
    sums, vector = reduce_grads(grads, vector, plan, 2)
    sums = [v.astype(F32) for v in sums]
    line = vector.reshape(-1)
    lines = []
    for v in small:
        lines.append(line[: v.shape[0]])
        line = line[v.shape[0] :]
    share = model_width // lax.axis_size("tok")
    mine = lambda v: lax.dynamic_slice_in_dim(v, lax.axis_index("tok") * share, share)
    wide = jnp.concatenate(
        [sums[4][i * width : (i + 1) * width] for i in range(blocks)], axis=1
    )
    cuts = [0]
    for v in (project, outward, expand, leave):
        cuts.append(cuts[-1] + v.shape[1])
    project, outward, expand, leave = (wide[:, a:b] for a, b in zip(cuts, cuts[1:]))
    return (
        (mine(lines[4]), sums[0], sums[1], mine(lines[5]), sums[2], sums[3]),
        (
            sums[5][:model_width],
            lines[0],
            lines[1],
            project,
            outward,
            lines[2],
            expand,
            sums[5][model_width:],
            lines[3],
            leave,
        ),
    )


def ffn_kernel(mid_ref, gain_ref, expand_ref, shrink_ref, out_ref, normed_ref, sum_ref):
    step = pl.program_id(0)

    @pl.when(step == 0)
    def _():
        normed_ref[...] = layer_norm(mid_ref[...], gain_ref[...]).astype(BF)
        sum_ref[...] = mid_ref[...]

    active = jax.nn.gelu(dot(normed_ref[...], expand_ref[...])).astype(BF)
    sum_ref[...] += dot(active, shrink_ref[...])

    @pl.when(step == pl.num_programs(0) - 1)
    def _():
        out_ref[...] = plain_norm(sum_ref[...])


def target_ffn(mid_rows, gain, expand, shrink, block=1024):
    length, width = mid_rows.shape
    hidden = expand.shape[1]
    whole = pl.BlockSpec((length, width), lambda j: (0, 0))
    return pl.pallas_call(
        ffn_kernel,
        grid=(hidden // block,),
        in_specs=[
            whole,
            pl.BlockSpec((1, width), lambda j: (0, 0)),
            pl.BlockSpec((width, block), lambda j: (0, j)),
            pl.BlockSpec((block, width), lambda j: (j, 0)),
        ],
        out_specs=whole,
        out_shape=jax.ShapeDtypeStruct((length, width), F32),
        scratch_shapes=[pltpu.VMEM((length, width), BF), pltpu.VMEM((length, width), F32)],
        compiler_params=pltpu.CompilerParams(vmem_limit_bytes=60 << 20),
        cost_estimate=pl.CostEstimate(
            flops=4 * length * width * hidden,
            bytes_accessed=8 * length * width + 4 * width * hidden,
            transcendentals=length * hidden,
        ),
        name="target_ffn",
    )(mid_rows, gain.reshape(1, -1), expand, shrink)


def feed_forward(mid_rows, midnorm, expand, shrink):
    mid_wide = mid_rows.astype(jnp.float32)
    normed = layer_norm(mid_wide, midnorm).astype(jnp.bfloat16)
    raised = product(normed, expand)
    active = jax.nn.gelu(raised).astype(jnp.bfloat16)
    output = (mid_wide + product(active, shrink)).astype(jnp.bfloat16)
    return (output, (mid_wide, normed, raised, active))


def feed_forward_back(grad_rows, saved, midnorm, expand, shrink):
    mid_wide, normed, raised, active = saved
    grad_shrink = inner_rows(active, grad_rows)
    grad_active = inner_cols(grad_rows, shrink)
    unused, gelu_pullback = jax.vjp(jax.nn.gelu, raised)
    grad_raised = gelu_pullback(grad_active)[0].astype(jnp.bfloat16)
    grad_expand = inner_rows(normed, grad_raised)
    grad_normed = inner_cols(grad_raised, expand)
    unused, norm_pullback = jax.vjp(layer_norm, mid_wide, midnorm)
    grad_mid, grad_midnorm = norm_pullback(grad_normed)
    grad_total = (grad_rows.astype(jnp.float32) + grad_mid).astype(jnp.bfloat16)
    return (grad_total, (grad_midnorm, grad_expand, grad_shrink))


def shards(
    tokens,
    target_prenorm,
    target_project,
    target_outward,
    target_midnorm,
    target_expand,
    target_shrink,
    context_prenorm,
    context_project,
    context_outward,
    context_midnorm,
    context_expand,
    context_shrink,
    predict_entry,
    mask_token,
    predict_prenorm,
    predict_project,
    predict_outward,
    predict_midnorm,
    predict_expand,
    predict_shrink,
    predict_endnorm,
    predict_exit,
    clip_order,
    visible_count,
):
    clips_here = clip_order.shape[0]
    clip_len = clip_order.shape[1]
    model_width = tokens.shape[1]
    head_devices = lax.axis_size("head")
    lane_index = lax.axis_index("tok")
    head_index = lax.axis_index("head")
    device_index = lane_index * head_devices + head_index
    counts_here = lax.dynamic_slice_in_dim(visible_count, device_index * clips_here, clips_here)
    tuned = lax.axis_size("tok") == 8 and head_devices == 4
    visible_pos = clip_order[:, :VMOST]
    slot_live = jnp.arange(VMOST, dtype=jnp.int32)[None, :] < counts_here[:, None]
    holds = visible_pos[:, :, None] == jnp.arange(clip_len, dtype=jnp.int32)[None, None, :]
    holds = jnp.logical_and(holds, slot_live[:, :, None])
    visible = jnp.any(holds, axis=1)
    slot = jnp.arange(VMOST, dtype=jnp.int32)[None, :, None]
    order_rank = jnp.sum(jnp.where(holds, slot, 0), axis=1)
    token_grid = tokens.reshape(clips_here, clip_len, model_width)
    seen_rows = jnp.einsum(
        "csl,cld->csd", holds.astype(BF), token_grid, preferred_element_type=jnp.float32
    )
    seen_rows = seen_rows.reshape(clips_here * VMOST, model_width)
    seen_low = seen_rows.astype(BF)
    live_column = slot_live.astype(jnp.int32).reshape(-1, 1)
    weights, attended = every_weight(
        tuned,
        (target_prenorm, target_midnorm, context_prenorm, context_midnorm),
        (
            target_project,
            target_outward,
            target_expand,
            target_shrink,
            context_project,
            context_outward,
            context_expand,
            context_shrink,
        ),
        tokens,
        seen_low,
        live_column,
        H,
    )
    target_out, context_in, context_mixed, context_attn, context_lse = attended
    ctx_prenorm_full, ctx_midnorm_full = weights[2:4]
    ctx_project_full, ctx_outward_full, ctx_expand_full, ctx_shrink_full = weights[8:]
    ctx_prenorm_wide = ctx_prenorm_full.astype(jnp.float32)
    ctx_midnorm_wide = ctx_midnorm_full.astype(jnp.float32)
    context_mid = (seen_rows + product(context_attn, ctx_outward_full)).astype(jnp.bfloat16)
    context_out, ffn_saved = feed_forward(
        context_mid, ctx_midnorm_wide, ctx_expand_full, ctx_shrink_full
    )
    entry_rows = product(context_out, predict_entry).reshape(clips_here, VMOST, -1)
    placed = jnp.take_along_axis(entry_rows, order_rank[:, :, None], axis=1)
    start_rows = jnp.where(
        visible[:, :, None], placed, mask_token.astype(jnp.float32)[None, None, :]
    )
    start_rows = (start_rows + positions(clip_len, PD)[None]).reshape(clips_here * clip_len, PD)
    pred_prenorm_wide = predict_prenorm.astype(jnp.float32)
    pred_midnorm_wide = predict_midnorm.astype(jnp.float32)
    pred_endnorm_wide = predict_endnorm.astype(jnp.float32)
    predict_in = layer_norm(start_rows, pred_prenorm_wide).astype(jnp.bfloat16)
    predict_mixed = product(predict_in, predict_project).astype(jnp.bfloat16)
    predict_attn, predict_lse = attn_fwd(predict_mixed, PH)
    branch_rows = start_rows + product(predict_attn, predict_outward)
    predict_normed = layer_norm(branch_rows, pred_midnorm_wide).astype(jnp.bfloat16)
    predict_raised = product(predict_normed, predict_expand)
    predict_active = jax.nn.gelu(predict_raised).astype(jnp.bfloat16)
    final_rows = branch_rows + product(predict_active, predict_shrink)
    final_in = layer_norm(final_rows, pred_endnorm_wide).astype(jnp.bfloat16)
    predicted = product(final_in, predict_exit)
    differ = predicted - target_out
    hidden_rows = jnp.logical_not(visible).reshape(-1)
    row_error = jnp.mean(smooth_error(differ), axis=1)
    clip_sums = jnp.sum(
        jnp.where(hidden_rows, row_error, 0.0).reshape(clips_here, clip_len), axis=1
    )
    clip_loss = clip_sums / (clip_len - counts_here).astype(jnp.float32)
    slope = jnp.clip(differ / HUBER, -1.0, 1.0)
    grad_predicted = (jnp.where(hidden_rows[:, None], slope, 0.0) / model_width).astype(
        jnp.bfloat16
    )
    grad_exit = inner_rows(final_in, grad_predicted)
    grad_final_in = inner_cols(grad_predicted, predict_exit)
    unused, norm_pullback = jax.vjp(layer_norm, final_rows, pred_endnorm_wide)
    grad_final, grad_endnorm = norm_pullback(grad_final_in)
    grad_second = grad_final.astype(jnp.bfloat16)
    grad_pred_shrink = inner_rows(predict_active, grad_second)
    grad_pred_active = inner_cols(grad_second, predict_shrink)
    unused, gelu_pullback = jax.vjp(jax.nn.gelu, predict_raised)
    grad_pred_raised = gelu_pullback(grad_pred_active)[0].astype(jnp.bfloat16)
    grad_pred_expand = inner_rows(predict_normed, grad_pred_raised)
    grad_pred_normed = inner_cols(grad_pred_raised, predict_expand)
    unused, norm_pullback = jax.vjp(layer_norm, branch_rows, pred_midnorm_wide)
    grad_branch_norm, grad_pred_midnorm = norm_pullback(grad_pred_normed)
    grad_branch = grad_final + grad_branch_norm
    grad_first = grad_branch.astype(jnp.bfloat16)
    grad_pred_outward = inner_rows(predict_attn, grad_first)
    grad_pred_attn = inner_cols(grad_first, predict_outward).astype(jnp.bfloat16)
    grad_pred_mixed = attn_bwd(predict_mixed, predict_attn, predict_lse, grad_pred_attn, PH)
    grad_pred_project = inner_rows(predict_in, grad_pred_mixed)
    grad_pred_in = inner_cols(grad_pred_mixed, predict_project)
    unused, norm_pullback = jax.vjp(layer_norm, start_rows, pred_prenorm_wide)
    grad_start_norm, grad_pred_prenorm = norm_pullback(grad_pred_in)
    grad_start = (grad_branch + grad_start_norm).reshape(clips_here, clip_len, PD)
    grad_mask = jnp.sum(jnp.where(visible[:, :, None], 0.0, grad_start), axis=(0, 1))
    grad_entry_rows = jnp.take_along_axis(grad_start, visible_pos[:, :, None], axis=1)
    grad_entry_rows = jnp.where(slot_live[:, :, None], grad_entry_rows, 0.0)
    grad_entry_rows = grad_entry_rows.reshape(clips_here * VMOST, PD).astype(jnp.bfloat16)
    grad_entry = inner_rows(context_out, grad_entry_rows)
    grad_context_out = inner_cols(grad_entry_rows, predict_entry).astype(jnp.bfloat16)
    back_project, back_outward = ctx_project_full, ctx_outward_full
    back_expand, back_shrink = ctx_expand_full, ctx_shrink_full
    back_prenorm_wide, back_midnorm_wide = ctx_prenorm_wide, ctx_midnorm_wide
    grad_mid, ffn_grads = feed_forward_back(
        grad_context_out, ffn_saved, back_midnorm_wide, back_expand, back_shrink
    )
    grad_ctx_outward = inner_rows(context_attn, grad_mid)
    grad_ctx_attn = inner_cols(grad_mid, back_outward).astype(jnp.bfloat16)
    grad_ctx_mixed = attn_bwd(
        context_mixed, context_attn, context_lse, grad_ctx_attn, H, counts_here
    )
    grad_ctx_project = inner_rows(context_in, grad_ctx_mixed)
    grad_ctx_in = inner_cols(grad_ctx_mixed, back_project)
    unused, norm_pullback = jax.vjp(layer_norm, seen_rows, back_prenorm_wide)
    grad_seen_norm, grad_ctx_prenorm = norm_pullback(grad_ctx_in)
    grad_seen = (grad_mid.astype(jnp.float32) + grad_seen_norm).reshape(
        clips_here, VMOST, model_width
    )
    grad_grid = jnp.take_along_axis(
        grad_seen, order_rank[:, :, None], axis=1
    )
    tokens_grad = jnp.where(visible[:, :, None], grad_grid, 0.0).reshape(
        clips_here * clip_len, model_width
    )
    context_sums, predict_sums = every_grad(
        tuned,
        (
            grad_ctx_prenorm,
            grad_ctx_project,
            grad_ctx_outward,
            ffn_grads[0],
            ffn_grads[1],
            ffn_grads[2],
        ),
        (
            grad_entry,
            grad_mask,
            grad_pred_prenorm,
            grad_pred_project,
            grad_pred_outward,
            grad_pred_midnorm,
            grad_pred_expand,
            grad_pred_shrink,
            grad_endnorm,
            grad_exit,
        ),
    )
    return (
        clip_loss,
        tokens_grad,
        context_sums[0],
        context_sums[1],
        context_sums[2],
        context_sums[3],
        context_sums[4],
        context_sums[5],
        predict_sums[0],
        predict_sums[1],
        predict_sums[2],
        predict_sums[3],
        predict_sums[4],
        predict_sums[5],
        predict_sums[6],
        predict_sums[7],
        predict_sums[8],
        predict_sums[9],
    )


def solution(mesh):
    return jax.shard_map(
        shards,
        mesh=mesh,
        in_specs=(
            P(("tok", "head"), None),
            P("tok"),
            P("tok", None),
            P("tok", None),
            P("tok"),
            P("tok", None),
            P("tok", None),
            P("tok"),
            P("tok", None),
            P("tok", None),
            P("tok"),
            P("tok", None),
            P("tok", None),
            P(),
            P(),
            P(),
            P(),
            P(),
            P(),
            P(),
            P(),
            P(),
            P(),
            P(("tok", "head"), None),
            P(),
        ),
        out_specs=(
            P(("tok", "head")),
            P(("tok", "head"), None),
            P("tok"),
            P("tok", None),
            P("tok", None),
            P("tok"),
            P("tok", None),
            P("tok", None),
            P(),
            P(),
            P(),
            P(),
            P(),
            P(),
            P(),
            P(),
            P(),
            P(),
        ),
        check_vma=False,
    )
```

```python
import functools

import jax
import jax.numpy as jnp
from jax import lax
from jax.experimental import pallas as pl
from jax.experimental.pallas import tpu as pltpu
from jax.sharding import PartitionSpec as P

H = 16
PD = 384
PH = 12
VMOST = 464


EPSILON = 1e-06
HUBER = 0.25


def layer_norm(values, gains):
    center = values - jnp.mean(values, axis=-1, keepdims=True)
    spread = jnp.mean(center * center, axis=-1, keepdims=True)
    return center * lax.rsqrt(spread + EPSILON) * gains


def plain_norm(values):
    center = values - jnp.mean(values, axis=-1, keepdims=True)
    spread = jnp.mean(center * center, axis=-1, keepdims=True)
    return center * lax.rsqrt(spread + EPSILON)


def smooth_error(differ):
    magnitude = jnp.abs(differ)
    return jnp.where(magnitude < HUBER, 0.5 * differ * differ / HUBER, magnitude - 0.5 * HUBER)


def positions(length, breadth, block=32):
    half_width = breadth // 2
    freqs = jnp.exp(-jnp.log(10000.0) * jnp.arange(half_width, dtype=jnp.float32) / half_width)
    coarse = jnp.arange(0, length, block, dtype=jnp.float32)[:, None, None] * freqs
    fine = jnp.arange(block, dtype=jnp.float32)[None, :, None] * freqs
    sines = lax.optimization_barrier((jnp.sin(coarse), jnp.cos(coarse), jnp.sin(fine), jnp.cos(fine)))
    sin_far, cos_far, sin_near, cos_near = sines
    table = jnp.concatenate(
        [sin_far * cos_near + cos_far * sin_near, cos_far * cos_near - sin_far * sin_near], axis=2
    )
    return table.reshape(-1, breadth)[:length]


def product(former, latter):
    return jnp.dot(former, latter, preferred_element_type=jnp.float32)


def inner_rows(former, latter):
    return lax.dot_general(
        former, latter, (((0,), (0,)), ((), ())), preferred_element_type=jnp.float32
    )


def inner_cols(former, latter):
    return lax.dot_general(
        former, latter, (((1,), (1,)), ((), ())), preferred_element_type=jnp.float32
    )


BF=jnp.bfloat16; F32=jnp.float32
LOG2E=1.4426950408889634
NT=(((1,),(1,)),((),())); NN=(((1,),(0,)),((),()))
def dot(a,b,dims=NN): return lax.dot_general(a,b,dims,preferred_element_type=F32)
def chunks(n,step):
    return [(i,min(step,n-i)) for i in range(0,n,step)]
def lane_mask(rows,h,e):
    lane=lax.broadcasted_iota(jnp.int32,(rows,128),1)
    return (lane>=h*e)&(lane<(h+1)*e)
def head_rows(values,h,e):
    return jnp.where(lane_mask(values.shape[0],h,e),values,jnp.zeros_like(values))

def attend_group(q_all,k,v,e,live,step):
    L=q_all.shape[0]; per=128//e; c=e**-0.5*LOG2E
    vt=v.T
    results=[]; sums=[]
    for (s0,n) in chunks(L,step):
        outs=[]; lses=[]
        for h in range(per):
            q=head_rows(q_all[s0:s0+n,:],h,e)
            st=dot(k,q,NT)
            if live is not None: st=jnp.where(live,st,-1e30)
            m=jnp.max(st,axis=0,keepdims=True)
            p=jnp.exp2((st-m)*c)
            l=jnp.sum(p,axis=0,keepdims=True)
            outs.append(dot(vt[h*e:(h+1)*e,:],p.astype(BF))*(1.0/l))
            lses.append(m*c+jnp.log2(l))
        results.append(jnp.concatenate(outs,axis=0).T.astype(BF))
        sums.append(jnp.concatenate(lses,axis=0))
    if len(results)==1: return results[0],sums[0]
    return jnp.concatenate(results,axis=0),jnp.concatenate(sums,axis=1)

def fwd_kernel(e,step,masked,want_lse,*refs):
    refs=list(refs)
    count=refs.pop(0) if masked else None
    q_ref,k_ref,v_ref,o_ref=refs[:4]
    L=q_ref.shape[0]
    live=lax.broadcasted_iota(jnp.int32,(L,1),0)<count[0] if masked else None
    o_ref[...],lse=attend_group(q_ref[...],k_ref[...],v_ref[...],e,live,step)
    if want_lse: refs[4][0]=lse

def attn_fwd(mixed,heads,count=None,step=1280,want_lse=True):
    L,w3=mixed.shape; Dm=w3//3; e=Dm//heads; G=Dm//128; per=128//e
    masked=count is not None
    spec=lambda off: pl.BlockSpec((L,128),lambda g,*_:(0,off+g))
    out_shape=[jax.ShapeDtypeStruct((L,Dm),BF)]; out_specs=[pl.BlockSpec((L,128),lambda g,*_:(0,g))]
    if want_lse:
        out_shape.append(jax.ShapeDtypeStruct((G,per,L),F32)); out_specs.append(pl.BlockSpec((1,per,L),lambda g,*_:(g,0,0)))
    gs=pltpu.PrefetchScalarGridSpec(num_scalar_prefetch=1 if masked else 0,grid=(G,),in_specs=[spec(0),spec(G),spec(2*G)],out_specs=out_specs)
    flops=4*heads*L*L*e
    f=pl.pallas_call(functools.partial(fwd_kernel,e,step,masked,want_lse),grid_spec=gs,out_shape=out_shape,
        compiler_params=pltpu.CompilerParams(vmem_limit_bytes=56<<20),
        cost_estimate=pl.CostEstimate(flops=flops,bytes_accessed=L*Dm*8,transcendentals=heads*L*L),name="attn_fwd")
    return f(*((count,) if masked else ()),mixed,mixed,mixed)

def bwd_kernel(e,step,masked,*refs):
    refs=list(refs)
    count=refs.pop(0) if masked else None
    q_ref,k_ref,v_ref,o_ref,do_ref,lse_ref,g_ref,dk_ref,dv_ref=refs
    L=q_ref.shape[0]; per=128//e; c=e**-0.5*LOG2E; f=e**-0.5
    g=pl.program_id(0); G=pl.num_programs(0)
    k=k_ref[...]; v=v_ref[...]
    kt=k.T
    live=None
    if masked:
        live=lax.broadcasted_iota(jnp.int32,(L,1),0)<count[0]
    dk_ref[...]=jnp.zeros_like(dk_ref); dv_ref[...]=jnp.zeros_like(dv_ref)
    cols=lambda part: pl.ds(pl.multiple_of((part*G+g)*128,128),128)
    for (s0,n) in chunks(L,step):
        do_all=do_ref[s0:s0+n,:]; q_all=q_ref[s0:s0+n,:]
        prod=(do_all.astype(F32)*o_ref[s0:s0+n,:].astype(F32)).T
        dqs=[]
        for h in range(per):
            q=head_rows(q_all,h,e); do=head_rows(do_all,h,e)
            delta=jnp.sum(prod[h*e:(h+1)*e,:],axis=0,keepdims=True)
            st=dot(k,q,NT)
            p=jnp.exp2(st*c-lse_ref[0,h:h+1,s0:s0+n])
            if masked: p=jnp.where(live,p,0.0)
            dp=dot(v,do,NT)
            ds=(p*(dp-delta)).astype(BF)
            dv_ref[...]+=dot(p.astype(BF),do)
            dk_ref[...]+=dot(ds,q)
            dqs.append(dot(kt[h*e:(h+1)*e,:],ds))
        g_ref[s0:s0+n,cols(0)]=(jnp.concatenate(dqs,axis=0)*f).T.astype(BF)
    g_ref[:,cols(1)]=(dk_ref[...]*f).astype(BF)
    g_ref[:,cols(2)]=dv_ref[...].astype(BF)

def attn_bwd(mixed,o,lse,do,heads,count=None,step=256):
    L,w3=mixed.shape; Dm=w3//3; e=Dm//heads; G=Dm//128; per=128//e
    masked=count is not None
    spec=lambda off: pl.BlockSpec((L,128),lambda g,*_:(0,off+g))
    gs=pltpu.PrefetchScalarGridSpec(num_scalar_prefetch=1 if masked else 0,grid=(G,),
        in_specs=[spec(0),spec(G),spec(2*G),spec(0),spec(0),pl.BlockSpec((1,per,L),lambda g,*_:(g,0,0))],
        out_specs=pl.BlockSpec((L,w3),lambda g,*_:(0,0)),
        scratch_shapes=[pltpu.VMEM((L,128),F32)]*2)
    return pl.pallas_call(functools.partial(bwd_kernel,e,step,masked),grid_spec=gs,out_shape=jax.ShapeDtypeStruct((L,w3),BF),
        compiler_params=pltpu.CompilerParams(vmem_limit_bytes=56<<20),
        cost_estimate=pl.CostEstimate(flops=10*heads*L*L*e,bytes_accessed=L*Dm*16,transcendentals=heads*L*L),name="attn_bwd")(*((count,) if masked else ()),mixed,mixed,mixed,o,do,lse)


MESH = pl.DeviceIdType.MESH
ANY = pl.BlockSpec(memory_space=pl.ANY)

def place():
    tok=lax.axis_index("tok"); head=lax.axis_index("head")
    return tok//2, tok%2, head//2, head%2

def peer(z,y,x,c): return (z*2+y, x*2+c)

def greet(barrier_peers):
    barrier=pltpu.get_barrier_semaphore()
    for p in barrier_peers:
        pl.semaphore_signal(barrier,inc=1,device_id=p,device_id_type=MESH)
    pl.semaphore_wait(barrier,len(barrier_peers))

def gather_steps(shard, full, own, cut, quarter, local, send, recv):
    z,y,x,c=place()
    xs = x if quarter else slice(None)
    rows, cols = cut
    def rcopy(i,src,dst,dev):
        return pltpu.make_async_remote_copy(src_ref=src,dst_ref=dst,send_sem=send.at[i],recv_sem=recv.at[i],device_id=dev,device_id_type=MESH)
    mine=shard.at[xs,c,rows,cols]
    def load(): return pltpu.make_async_copy(mine,own,local.at[0])
    def put(): return pltpu.make_async_copy(own,full.at[z,y,xs,c,rows,cols],local.at[1])
    def zc(k,out):
        dst=full.at[z,y,xs,c,rows,cols] if out else full.at[(z+4-k)%4,y,xs,c,rows,cols]
        return rcopy(k-1,mine,dst,peer((z+k)%4,y,x,c))
    def yc(out):
        yy=y if out else 1-y
        return rcopy(3,full.at[:,y,xs,c,rows,cols],full.at[:,yy,xs,c,rows,cols],peer(z,1-y,x,c))
    def xc(out):
        xx=x if out else 1-x
        return rcopy(4,full.at[:,:,x,c,rows,cols],full.at[:,:,xx,c,rows,cols],peer(z,y,1-x,c))
    def cc(out):
        cz=c if out else 1-c
        return rcopy(5,full.at[:,:,:,c,rows,cols],full.at[:,:,:,cz,rows,cols],peer(z,y,x,1-c))
    def s0():
        load().start()
        for k in (2,1,3): zc(k,True).start()
    def s1():
        load().wait(); put().start()
        for k in (1,2,3): zc(k,False).wait_recv()
        put().wait()
        yc(True).start()
    def s2():
        yc(False).wait_recv()
        if quarter: xc(True).start()
        else: cc(True).start()
    def s3():
        if quarter:
            xc(False).wait_recv(); cc(True).start()
    def s4():
        cc(False).wait_recv()
        for k in (1,2,3): zc(k,True).wait_send()
        yc(True).wait_send()
        if quarter: xc(True).wait_send()
        cc(True).wait_send()
    return [s0,s1,s2,s3,s4]

def gains_steps(src,out,send,recv):
    z,y,x,c=place()
    def cp(k,outgoing):
        dz,dy=k//2,k%2
        t=z*2+y
        pz=(z+dz)%4; py=(y+dy)%2
        sz=(z+4-dz)%4; sy=(y+2-dy)%2
        dst=out.at[t] if outgoing else out.at[sz*2+sy]
        return pltpu.make_async_remote_copy(src_ref=src,dst_ref=dst,send_sem=send.at[k-1],recv_sem=recv.at[k-1],device_id=peer(pz,py,x,c),device_id_type=MESH)
    def start():
        for k in range(1,8): cp(k,True).start()
    def finish():
        for k in range(1,8): cp(k,False).wait_recv()
        for k in range(1,8): cp(k,True).wait_send()
    return start,finish

def everyone_on_tok():
    z,y,x,c=place()
    peers=[peer((z+k//2)%4,(y+k%2)%2,x,c) for k in range(1,8)]
    return peers+[peer(z,y,1-x,c),peer(z,y,x,1-c)]

def together(members):
    def stage(s):
        def run():
            for m in members: m[s]()
        return run
    return [stage(s) for s in range(len(members[0]))]

def interleave(chunks):
    n=len(chunks); depth=len(chunks[0])
    order=[]
    for t in range(n+depth-1):
        for s in range(depth):
            i=t-s
            if 0<=i<n: order.append(chunks[i][s])
    return order

def by_turn(chunks):
    turns=[[] for _ in range(len(chunks)+len(chunks[0])-1)]
    for i,chunk in enumerate(chunks):
        for s,stage in enumerate(chunk): turns[i+s].append((s,stage))
    return [[stage for _,stage in sorted(t,key=lambda p:-p[0])] for t in turns]

def scaled_norm(values,gain_blocks,row,out_ref):
    normed=plain_norm(values.astype(F32))
    for t in range(gain_blocks.shape[0]):
        cols=slice(t*128,(t+1)*128)
        out_ref[:,cols]=(normed[:,cols]*gain_blocks[t,row:row+1,:].astype(F32)).astype(BF)

def ag_kernel(plan,n,heads,*refs):
    shards=refs[:n]; gain,tok_ref,seen_ref,live_ref=refs[n:n+4]
    fulls=refs[n+4:2*n+4]; gout,tout,cin,cmixed,cattn,clse=refs[2*n+4:2*n+10]
    rest=refs[2*n+10:]
    k=len(plan)
    owns=rest[:k]; gown,local,send,recv,gsend,grecv,glocal,gv,tin,tattn,total,pw,ow,ew,sw,wsem=rest[k:]
    z,y,x,c=place()
    turn=pl.program_id(0)
    steps=[]
    for i,(w,r0,rn,c0,cn,quarter) in enumerate(plan):
        steps.append(gather_steps(shards[w],fulls[w],owns[i],(pl.ds(r0,rn),pl.ds(c0,cn)),quarter,local.at[i],send.at[i],recv.at[i]))
    groups={}
    for st,entry in zip(steps,plan): groups.setdefault(entry[:3],[]).append(st)
    turns=by_turn([together(m) for m in groups.values()])
    done={w:i+len(steps[0])-1 for i,(w,_,_) in enumerate(groups)}
    gs,gf=gains_steps(gain,gout,gsend,grecv)
    width=tok_ref.shape[1]; G=width//128; e=width//heads
    first=done[0]+1; outward=first+G//2; dense=outward+1; end=len(turns)-1
    blocks,block_width=2,ew.shape[-1]; finish=dense+8//blocks
    other=end+1-G//2
    assert done[1]<outward and max(done[2],done[3])<dense and outward<done[4]+1<=other and finish<end
    take=lambda w,dst,i: pltpu.make_async_copy(fulls[w],dst,wsem.at[i])
    def take_block(j):
        b=(turn-dense)*blocks+j
        cols=pl.ds(pl.multiple_of(b*block_width,128),block_width)
        return (pltpu.make_async_copy(fulls[2].at[:,:,:,:,:,cols],ew.at[j],wsem.at[2+2*j]),
                pltpu.make_async_copy(fulls[3].at[b//2,b%2],sw.at[j],wsem.at[3+2*j]))
    for t,fs in enumerate(turns):
        @pl.when(turn==t)
        def _(t=t,fs=fs):
            if t==0: greet(everyone_on_tok())
            if t==first: take(0,pw,0).start()
            if t==outward: take(1,ow,1).start()
            if t==done[4]+1: take(4,pw,0).start()
            for f in fs: f()
            if t==0:
                gs()
                g0=pltpu.make_async_copy(gain,gown,glocal.at[0]); g0.start(); g0.wait()
                pltpu.make_async_copy(gown,gout.at[z*2+y],glocal.at[1]).start()
            if t==2:
                pltpu.make_async_copy(gown,gout.at[z*2+y],glocal.at[1]).wait()
                gf()
                g2=pltpu.make_async_copy(gout,gv,glocal.at[2]); g2.start(); g2.wait()
            if t==3: scaled_norm(tok_ref[...],gv,0,tin)
            if t==4: scaled_norm(seen_ref[...],gv,2,cin)
            if t==first: take(0,pw,0).wait()
            if t==outward:
                take(1,ow,1).wait()
                total[...]=tok_ref[...].astype(F32)+dot(tattn[...],ow[...].reshape(width,width))
                scaled_norm(total[...],gv,1,tin)
            if t==done[4]+1: take(4,pw,0).wait()
            if t==finish:
                total[...]=plain_norm(total[...])
                pltpu.make_async_copy(total,tout,wsem.at[1]).start()
            if t==end: pltpu.make_async_copy(total,tout,wsem.at[1]).wait()
    def block(part,g): return pw[:,:,:,:,:,pl.ds(pl.multiple_of((part*G+g)*128,128),128)].reshape(width,128)
    @pl.when((turn>=first)&(turn<outward))
    def _():
        @pl.loop(0,2)
        def _(j):
            g=(turn-first)*2+j
            q,key,v=[dot(tin[...],block(part,g)).astype(BF) for part in range(3)]
            o,_=attend_group(q,key,v,e,None,1280)
            tattn[:,pl.ds(pl.multiple_of(g*128,128),128)]=o
    @pl.when(turn>=other)
    def _():
        live=live_ref[...]!=0
        @pl.loop(0,2)
        def _(j):
            g=(turn-other)*2+j
            parts=[dot(cin[...],block(part,g)).astype(BF) for part in range(3)]
            for part in range(3):
                cmixed[:,pl.ds(pl.multiple_of((part*G+g)*128,128),128)]=parts[part]
            o,lse=attend_group(*parts,e,live,1280)
            cattn[:,pl.ds(pl.multiple_of(g*128,128),128)]=o
            clse[g]=lse
    @pl.when((turn>=dense)&(turn<finish))
    def _():
        for j in range(blocks):
            for copy in take_block(j): copy.start()
        for j in range(blocks):
            for copy in take_block(j): copy.wait()
            active=jax.nn.gelu(dot(tin[...],ew[j].reshape(width,block_width))).astype(BF)
            total[...]+=dot(active,sw[j].reshape(block_width,width))

def gather_and_attend(shards,gains,tokens,seen,live,heads,plan,cid):
    n=len(shards); k=len(plan)
    views=[s.reshape(2,2,s.shape[0]//4,s.shape[1]) for s in shards]
    outs=[jax.ShapeDtypeStruct((4,2,2,2,s.shape[0]//4,s.shape[1]),s.dtype) for s in shards]
    outs.append(jax.ShapeDtypeStruct((8,)+gains.shape,gains.dtype))
    (L,width),slots=tokens.shape,seen.shape[0]
    G=width//128
    extra=[((L,width),F32),((slots,width),BF),((slots,3*width),BF),((slots,width),BF),((G,heads//G,slots),F32)]
    outs+=[jax.ShapeDtypeStruct(s,d) for s,d in extra]
    whole=lambda s: pl.BlockSpec(s,lambda t: (0,)*len(s))
    owns=[pltpu.VMEM(((rn,cn) if q else (2,rn,cn)),BF) for (w,r0,rn,c0,cn,q) in plan]
    S=pltpu.SemaphoreType.DMA
    turns=len({entry[:3] for entry in plan})+4
    scratch=owns+[pltpu.VMEM(gains.shape,BF),S((k,2)),S((k,6)),S((k,6)),S((7,)),S((7,)),S((3,)),
        pltpu.VMEM((8,)+gains.shape,BF),pltpu.VMEM((L,width),BF),pltpu.VMEM((L,width),BF),pltpu.VMEM((L,width),F32),
        pltpu.VMEM(outs[0].shape,BF),pltpu.VMEM(outs[1].shape,BF),
        pltpu.VMEM((2,)+outs[2].shape[:-1]+(outs[2].shape[-1]//8,),BF),pltpu.VMEM((2,)+outs[3].shape[2:],BF),S((6,))]
    res=pl.pallas_call(functools.partial(ag_kernel,plan,n,heads),grid=(turns,),out_shape=outs,
        in_specs=[ANY]*(n+1)+[whole(tokens.shape),whole(seen.shape),whole(live.shape)],
        out_specs=[ANY]*(n+2)+[whole(s) for s,_ in extra[1:]],scratch_shapes=scratch,
        compiler_params=pltpu.CompilerParams(collective_id=cid,has_side_effects=True,vmem_limit_bytes=60<<20),name="gather_and_attend")(*views,gains,tokens,seen,live)
    return [o.reshape(8*s.shape[0],s.shape[1]) for o,s in zip(res[:n],shards)],res[n],res[n+1:]

def reduce_steps(grad, out, rn, rows, bufs, order, everywhere, local, send, recv):
    z,y,x,c=place()
    M,C,A,B,Z,T=bufs
    def rcopy(i,src,dst,dev):
        return pltpu.make_async_remote_copy(src_ref=src,dst_ref=dst,send_sem=send.at[i],recv_sem=recv.at[i],device_id=dev,device_id_type=MESH)
    xfirst=order=="xy"
    side={"x":peer(z,y,1-x,c),"y":peer(z,1-y,x,c)}
    first,second=order
    load=lambda: pltpu.make_async_copy(grad.at[:,:,:,c,rows],M,local.at[0])
    cc=lambda: rcopy(0,grad.at[:,:,:,1-c,rows],C,side_c)
    side_c=peer(z,y,x,1-c)
    ac=lambda: rcopy(1,M.at[:,:,1-x] if xfirst else M.at[:,1-y],A,side[first])
    bc=lambda: rcopy(2,M.at[:,1-y,x] if xfirst else M.at[:,y,1-x],B,side[second])
    zc=lambda k: rcopy(2+k,M.at[(z+k)%4,y,x],Z.at[k-1],peer((z+k)%4,y,x,c))
    def add(target,source):
        target[...]=(target[...].astype(F32)+source[...].astype(F32)).astype(BF)
    def s0():
        cc().start(); load().start()
    def s1():
        load().wait(); cc().wait_recv()
        @pl.loop(0,16)
        def _(i):
            at=(i//4,(i//2)%2,i%2)
            add(M.at[at],C.at[at])
        ac().start()
    def s2():
        ac().wait_recv()
        @pl.loop(0,8)
        def _(i):
            if xfirst: add(M.at[i//2,i%2,x],A.at[i//2,i%2])
            else: add(M.at[i//2,y,i%2],A.at[i//2,i%2])
        bc().start()
    def s3():
        bc().wait_recv()
        @pl.loop(0,4)
        def _(i):
            add(M.at[i,y,x],B.at[i])
        for k in (2,1,3): zc(k).start()
    if everywhere:
        home=out.at[z,y,x,c,rows]
        spread=[]
        for k in (1,2,3):
            spread.append((5+k,lambda o,k=k:(T,out.at[z,y,x,c,rows] if o else out.at[(z+4-k)%4,y,x,c,rows],peer((z+k)%4,y,x,c))))
        sy=(9,lambda o:(out.at[:,y,x,c,rows],out.at[:,y if o else 1-y,x,c,rows],side["y"]))
        sx=(10,lambda o:(out.at[:,:,x,c,rows],out.at[:,:,x if o else 1-x,c,rows],side["x"]))
        if xfirst: stages=[spread,[sy],[sx]]
        else:
            sx=(9,lambda o:(out.at[:,y,x,c,rows],out.at[:,y,x if o else 1-x,c,rows],side["x"]))
            sy=(10,lambda o:(out.at[:,y,:,c,rows],out.at[:,y if o else 1-y,:,c,rows],side["y"]))
            stages=[spread,[sx],[sy]]
        stages.append([(11,lambda o:(out.at[:,:,:,c,rows],out.at[:,:,:,c if o else 1-c,rows],side_c))])
    else:
        home=out.at[x,c,rows]
        stages=[[(6,lambda o:(T,out.at[x if o else 1-x,c,rows],side["x"]))],[(7,lambda o:(out.at[:,c,rows],out.at[:,c if o else 1-c,rows],side_c))]]
    def run(entry,o):
        i,f=entry; src,dst,dev=f(o); return rcopy(i,src,dst,dev)
    put=lambda: pltpu.make_async_copy(T,home,local.at[1])
    def s4():
        for k in (1,2,3): zc(k).wait_recv()
        T[...]=(M[z,y,x].astype(F32)+Z[0].astype(F32)+Z[1].astype(F32)+Z[2].astype(F32)).astype(BF)
        put().start()
        for e in stages[0]: run(e,True).start()
    def later(n):
        def s():
            if n==1: put().wait()
            for e in stages[n-1]: run(e,False).wait_recv()
            for e in stages[n]: run(e,True).start()
        return s
    def last():
        for e in stages[-1]: run(e,False).wait_recv()
        cc().wait_send(); ac().wait_send(); bc().wait_send()
        for k in (1,2,3): zc(k).wait_send()
        for st in stages:
            for e in st: run(e,True).wait_send()
    mids=[later(n) for n in range(1,len(stages))]
    if not everywhere: mids=mids+[lambda:None]*2
    return [s0,s1,s2,s3,s4]+mids+[last]

def vector_steps(src,out,bufs,local,send,recv):
    z,y,x,c=place()
    V,R=bufs
    dev=[peer(z,y,x,1-c),peer(z,y,1-x,c),peer(z,1-y,x,c)]+[peer((z+k)%4,y,x,c) for k in (1,2,3)]
    def rc(i): return pltpu.make_async_remote_copy(src_ref=V.at[min(i,3)],dst_ref=R.at[i],send_sem=send.at[i],recv_sem=recv.at[i],device_id=dev[i],device_id_type=MESH)
    load=lambda: pltpu.make_async_copy(src,V.at[0],local.at[0])
    def s0():
        load().start(); load().wait(); rc(0).start()
    def mid(n):
        def s():
            rc(n-1).wait_recv()
            V[n]=V[n-1]+R[n-1]
            if n<3: rc(n).start()
            else:
                for i in (3,4,5): rc(i).start()
        return s
    def fin():
        for i in (3,4,5): rc(i).wait_recv()
        V[4]=V[3]+R[3]+R[4]+R[5]
        cp=pltpu.make_async_copy(V.at[4],out,local.at[1]); cp.start(); cp.wait()
        for i in range(6): rc(i).wait_send()
    nothing=lambda:None
    return [s0,mid(1),mid(2),mid(3),fin,nothing,nothing,nothing,nothing]

def rs_kernel(plan,n,*refs):
    grads=refs[:n]; vec=refs[n]; outs=refs[n+1:2*n+1]; vout=refs[2*n+1]; rest=refs[2*n+2:]
    k=len(plan)
    bufs=[rest[6*i:6*i+6] for i in range(k)]
    V,R,local,send,recv,vlocal,vsend,vrecv=rest[6*k:]
    z,y,x,c=place()
    greet([peer((z+j)%4,y,x,c) for j in (1,2,3)]+[peer(z,1-y,x,c),peer(z,y,1-x,c),peer(z,y,x,1-c)])
    steps=[reduce_steps(grads[w],outs[w],rn,pl.ds(r0,rn),bufs[i],order,ev,local.at[i],send.at[i],recv.at[i]) for i,(w,r0,rn,order,ev,_) in enumerate(plan)]
    steps.append(vector_steps(vec,vout,(V,R),vlocal,vsend,vrecv))
    groups={}
    for st,entry in zip(steps,plan): groups.setdefault(entry[5],[]).append(st)
    groups[plan[0][5]].append(steps[-1])
    groups=[together(m) for m in groups.values()]
    for st in groups: st[0]()
    for f in interleave([st[1:] for st in groups]): f()

def reduce_grads(grads, vec, plan, cid):
    n=len(grads)
    every={w:ev for w,_,_,_,ev,_ in plan}
    views=[g.reshape(4,2,2,2,g.shape[0]//32,g.shape[1]) for g in grads]
    outs=[jax.ShapeDtypeStruct(v.shape if every[w] else v.shape[2:],BF) for w,v in enumerate(views)]
    outs.append(jax.ShapeDtypeStruct(vec.shape,F32))
    scratch=[]
    for (w,r0,rn,order,ev,_) in plan:
        N=grads[w].shape[1]
        scratch+=[pltpu.VMEM((4,2,2,rn,N),BF),pltpu.VMEM((4,2,2,rn,N),BF),pltpu.VMEM((4,2,rn,N),BF),pltpu.VMEM((4,rn,N),BF),pltpu.VMEM((3,rn,N),BF),pltpu.VMEM((rn,N),BF)]
    k=len(plan)
    S=pltpu.SemaphoreType.DMA
    scratch+=[pltpu.VMEM((5,)+vec.shape,F32),pltpu.VMEM((6,)+vec.shape,F32),S((k,2)),S((k,12)),S((k,12)),S((2,)),S((6,)),S((6,))]
    res=pl.pallas_call(functools.partial(rs_kernel,plan,n),out_shape=outs,in_specs=[ANY]*(n+1),out_specs=[ANY]*(n+1),scratch_shapes=scratch,
        compiler_params=pltpu.CompilerParams(collective_id=cid,has_side_effects=True,vmem_limit_bytes=60<<20),name="reduce_grads")(*views,vec)
    flat=[]
    for w,r in enumerate(res[:n]):
        rows=grads[w].shape[0]
        flat.append(r.reshape(rows if every[w] else rows//8,grads[w].shape[1]))
    return flat,res[n]


def gather_plan(shards):
    plan = []
    for w in (0, 1, 2, 3, 4, 6, 7, 5):
        rows, wide = shards[w].shape[0] // 4, shards[w].shape[1]
        rest = (wide // 3 + 64) // 128 * 128
        parts = 1 if wide == shards[w].shape[0] * 8 else 2
        for part in range(parts):
            r0, rn = part * rows // parts, rows // parts
            plan.append((w, r0, rn, 0, wide - rest, True))
            plan.append((w, r0, rn, wide - rest, rest, False))
    return plan


def every_weight(tuned, gains, shards, tokens, seen, live, heads):
    if tuned:
        packed = jnp.pad(jnp.stack(gains), ((0, 12), (0, 0)))
        full, norms, attended = gather_and_attend(
            list(shards), packed, tokens, seen, live, heads, gather_plan(shards), 1
        )
        return tuple(norms[:, i, :].reshape(-1) for i in range(4)) + tuple(full), attended
    full = tuple(lax.all_gather(v, "tok", axis=0, tiled=True) for v in gains + shards)
    target_in = layer_norm(tokens.astype(F32), full[0].astype(F32)).astype(BF)
    target_attn = attn_fwd(product(target_in, full[4]).astype(BF), heads, want_lse=False)[0]
    target_mid = tokens.astype(F32) + product(target_attn, full[5])
    target_out = target_ffn(target_mid, full[1].astype(F32), full[6], full[7])
    context_in = layer_norm(seen.astype(F32), full[2].astype(F32)).astype(BF)
    context_mixed = product(context_in, full[8]).astype(BF)
    count = jnp.sum(live, axis=0)
    context_attn, context_lse = attn_fwd(context_mixed, heads, count)
    return full, (target_out, context_in, context_mixed, context_attn, context_lse)


def every_grad(tuned, context, predict):
    if not tuned:
        parts = [lax.psum_scatter(v, "tok", scatter_dimension=0, tiled=True) for v in context]
        return (
            tuple(lax.psum(v.astype(jnp.bfloat16), "head").astype(jnp.float32) for v in parts),
            lax.psum(predict, ("tok", "head")),
        )
    entry, mask, prenorm, project, outward, midnorm, expand, shrink, endnorm, leave = predict
    model_width, width = entry.shape
    wide = jnp.concatenate([project, outward, expand, leave], axis=1).astype(BF)
    blocks = wide.shape[1] // model_width
    wide = jnp.concatenate(
        [wide[:, i * model_width : (i + 1) * model_width] for i in range(blocks)], axis=0
    )
    tall = jnp.concatenate([entry, shrink], axis=0).astype(BF)
    small = (mask, prenorm, midnorm, endnorm, context[0], context[3])
    line = jnp.concatenate(small)
    vector = jnp.pad(line, (0, -line.shape[0] % 1024)).reshape(-1, 128)
    grads = [context[1], context[2], context[4], context[5]]
    grads = [v.astype(BF) for v in grads] + [wide, tall]
    piece = [v.shape[0] // 32 for v in grads]
    plan = [(4, 0, piece[4], "yx", True, 4), (5, 0, piece[5], "xy", True, 4)]
    for w in (3, 2, 0, 1):
        parts = 2 if piece[w] >= 64 else 1
        rows = piece[w] // (2 * parts)
        for part in range(parts):
            at, key = 2 * part * rows, (w, part)
            plan += [(w, at, rows, "xy", False, key), (w, at + rows, rows, "yx", False, key)]
    sums, vector = reduce_grads(grads, vector, plan, 2)
    sums = [v.astype(F32) for v in sums]
    line = vector.reshape(-1)
    lines = []
    for v in small:
        lines.append(line[: v.shape[0]])
        line = line[v.shape[0] :]
    share = model_width // lax.axis_size("tok")
    mine = lambda v: lax.dynamic_slice_in_dim(v, lax.axis_index("tok") * share, share)
    wide = jnp.concatenate(
        [sums[4][i * width : (i + 1) * width] for i in range(blocks)], axis=1
    )
    cuts = [0]
    for v in (project, outward, expand, leave):
        cuts.append(cuts[-1] + v.shape[1])
    project, outward, expand, leave = (wide[:, a:b] for a, b in zip(cuts, cuts[1:]))
    return (
        (mine(lines[4]), sums[0], sums[1], mine(lines[5]), sums[2], sums[3]),
        (
            sums[5][:model_width],
            lines[0],
            lines[1],
            project,
            outward,
            lines[2],
            expand,
            sums[5][model_width:],
            lines[3],
            leave,
        ),
    )


def ffn_kernel(mid_ref, gain_ref, expand_ref, shrink_ref, out_ref, normed_ref, sum_ref):
    step = pl.program_id(0)

    @pl.when(step == 0)
    def _():
        normed_ref[...] = layer_norm(mid_ref[...], gain_ref[...]).astype(BF)
        sum_ref[...] = mid_ref[...]

    active = jax.nn.gelu(dot(normed_ref[...], expand_ref[...])).astype(BF)
    sum_ref[...] += dot(active, shrink_ref[...])

    @pl.when(step == pl.num_programs(0) - 1)
    def _():
        out_ref[...] = plain_norm(sum_ref[...])


def target_ffn(mid_rows, gain, expand, shrink, block=1024):
    length, width = mid_rows.shape
    hidden = expand.shape[1]
    whole = pl.BlockSpec((length, width), lambda j: (0, 0))
    return pl.pallas_call(
        ffn_kernel,
        grid=(hidden // block,),
        in_specs=[
            whole,
            pl.BlockSpec((1, width), lambda j: (0, 0)),
            pl.BlockSpec((width, block), lambda j: (0, j)),
            pl.BlockSpec((block, width), lambda j: (j, 0)),
        ],
        out_specs=whole,
        out_shape=jax.ShapeDtypeStruct((length, width), F32),
        scratch_shapes=[pltpu.VMEM((length, width), BF), pltpu.VMEM((length, width), F32)],
        compiler_params=pltpu.CompilerParams(vmem_limit_bytes=60 << 20),
        cost_estimate=pl.CostEstimate(
            flops=4 * length * width * hidden,
            bytes_accessed=8 * length * width + 4 * width * hidden,
            transcendentals=length * hidden,
        ),
        name="target_ffn",
    )(mid_rows, gain.reshape(1, -1), expand, shrink)


def feed_forward(mid_rows, midnorm, expand, shrink):
    mid_wide = mid_rows.astype(jnp.float32)
    normed = layer_norm(mid_wide, midnorm).astype(jnp.bfloat16)
    raised = product(normed, expand)
    active = jax.nn.gelu(raised).astype(jnp.bfloat16)
    output = (mid_wide + product(active, shrink)).astype(jnp.bfloat16)
    return (output, (mid_wide, normed, raised, active))


def feed_forward_back(grad_rows, saved, midnorm, expand, shrink):
    mid_wide, normed, raised, active = saved
    grad_shrink = inner_rows(active, grad_rows)
    grad_active = inner_cols(grad_rows, shrink)
    unused, gelu_pullback = jax.vjp(jax.nn.gelu, raised)
    grad_raised = gelu_pullback(grad_active)[0].astype(jnp.bfloat16)
    grad_expand = inner_rows(normed, grad_raised)
    grad_normed = inner_cols(grad_raised, expand)
    unused, norm_pullback = jax.vjp(layer_norm, mid_wide, midnorm)
    grad_mid, grad_midnorm = norm_pullback(grad_normed)
    grad_total = (grad_rows.astype(jnp.float32) + grad_mid).astype(jnp.bfloat16)
    return (grad_total, (grad_midnorm, grad_expand, grad_shrink))


def shards(
    tokens,
    target_prenorm,
    target_project,
    target_outward,
    target_midnorm,
    target_expand,
    target_shrink,
    context_prenorm,
    context_project,
    context_outward,
    context_midnorm,
    context_expand,
    context_shrink,
    predict_entry,
    mask_token,
    predict_prenorm,
    predict_project,
    predict_outward,
    predict_midnorm,
    predict_expand,
    predict_shrink,
    predict_endnorm,
    predict_exit,
    clip_order,
    visible_count,
):
    clips_here = clip_order.shape[0]
    clip_len = clip_order.shape[1]
    model_width = tokens.shape[1]
    head_devices = lax.axis_size("head")
    lane_index = lax.axis_index("tok")
    head_index = lax.axis_index("head")
    device_index = lane_index * head_devices + head_index
    counts_here = lax.dynamic_slice_in_dim(visible_count, device_index * clips_here, clips_here)
    tuned = lax.axis_size("tok") == 8 and head_devices == 4
    visible_pos = clip_order[:, :VMOST]
    slot_live = jnp.arange(VMOST, dtype=jnp.int32)[None, :] < counts_here[:, None]
    holds = visible_pos[:, :, None] == jnp.arange(clip_len, dtype=jnp.int32)[None, None, :]
    holds = jnp.logical_and(holds, slot_live[:, :, None])
    visible = jnp.any(holds, axis=1)
    slot = jnp.arange(VMOST, dtype=jnp.int32)[None, :, None]
    order_rank = jnp.sum(jnp.where(holds, slot, 0), axis=1)
    token_grid = tokens.reshape(clips_here, clip_len, model_width)
    seen_rows = jnp.einsum(
        "csl,cld->csd", holds.astype(BF), token_grid, preferred_element_type=jnp.float32
    )
    seen_rows = seen_rows.reshape(clips_here * VMOST, model_width)
    seen_low = seen_rows.astype(BF)
    live_column = slot_live.astype(jnp.int32).reshape(-1, 1)
    weights, attended = every_weight(
        tuned,
        (target_prenorm, target_midnorm, context_prenorm, context_midnorm),
        (
            target_project,
            target_outward,
            target_expand,
            target_shrink,
            context_project,
            context_outward,
            context_expand,
            context_shrink,
        ),
        tokens,
        seen_low,
        live_column,
        H,
    )
    target_out, context_in, context_mixed, context_attn, context_lse = attended
    ctx_prenorm_full, ctx_midnorm_full = weights[2:4]
    ctx_project_full, ctx_outward_full, ctx_expand_full, ctx_shrink_full = weights[8:]
    ctx_prenorm_wide = ctx_prenorm_full.astype(jnp.float32)
    ctx_midnorm_wide = ctx_midnorm_full.astype(jnp.float32)
    context_mid = (seen_rows + product(context_attn, ctx_outward_full)).astype(jnp.bfloat16)
    context_out, ffn_saved = feed_forward(
        context_mid, ctx_midnorm_wide, ctx_expand_full, ctx_shrink_full
    )
    entry_rows = product(context_out, predict_entry).reshape(clips_here, VMOST, -1)
    placed = jnp.take_along_axis(entry_rows, order_rank[:, :, None], axis=1)
    start_rows = jnp.where(
        visible[:, :, None], placed, mask_token.astype(jnp.float32)[None, None, :]
    )
    start_rows = (start_rows + positions(clip_len, PD)[None]).reshape(clips_here * clip_len, PD)
    pred_prenorm_wide = predict_prenorm.astype(jnp.float32)
    pred_midnorm_wide = predict_midnorm.astype(jnp.float32)
    pred_endnorm_wide = predict_endnorm.astype(jnp.float32)
    predict_in = layer_norm(start_rows, pred_prenorm_wide).astype(jnp.bfloat16)
    predict_mixed = product(predict_in, predict_project).astype(jnp.bfloat16)
    predict_attn, predict_lse = attn_fwd(predict_mixed, PH)
    branch_rows = start_rows + product(predict_attn, predict_outward)
    predict_normed = layer_norm(branch_rows, pred_midnorm_wide).astype(jnp.bfloat16)
    predict_raised = product(predict_normed, predict_expand)
    predict_active = jax.nn.gelu(predict_raised).astype(jnp.bfloat16)
    final_rows = branch_rows + product(predict_active, predict_shrink)
    final_in = layer_norm(final_rows, pred_endnorm_wide).astype(jnp.bfloat16)
    predicted = product(final_in, predict_exit)
    differ = predicted - target_out
    hidden_rows = jnp.logical_not(visible).reshape(-1)
    row_error = jnp.mean(smooth_error(differ), axis=1)
    clip_sums = jnp.sum(
        jnp.where(hidden_rows, row_error, 0.0).reshape(clips_here, clip_len), axis=1
    )
    clip_loss = clip_sums / (clip_len - counts_here).astype(jnp.float32)
    slope = jnp.clip(differ / HUBER, -1.0, 1.0)
    grad_predicted = (jnp.where(hidden_rows[:, None], slope, 0.0) / model_width).astype(
        jnp.bfloat16
    )
    grad_exit = inner_rows(final_in, grad_predicted)
    grad_final_in = inner_cols(grad_predicted, predict_exit)
    unused, norm_pullback = jax.vjp(layer_norm, final_rows, pred_endnorm_wide)
    grad_final, grad_endnorm = norm_pullback(grad_final_in)
    grad_second = grad_final.astype(jnp.bfloat16)
    grad_pred_shrink = inner_rows(predict_active, grad_second)
    grad_pred_active = inner_cols(grad_second, predict_shrink)
    unused, gelu_pullback = jax.vjp(jax.nn.gelu, predict_raised)
    grad_pred_raised = gelu_pullback(grad_pred_active)[0].astype(jnp.bfloat16)
    grad_pred_expand = inner_rows(predict_normed, grad_pred_raised)
    grad_pred_normed = inner_cols(grad_pred_raised, predict_expand)
    unused, norm_pullback = jax.vjp(layer_norm, branch_rows, pred_midnorm_wide)
    grad_branch_norm, grad_pred_midnorm = norm_pullback(grad_pred_normed)
    grad_branch = grad_final + grad_branch_norm
    grad_first = grad_branch.astype(jnp.bfloat16)
    grad_pred_outward = inner_rows(predict_attn, grad_first)
    grad_pred_attn = inner_cols(grad_first, predict_outward).astype(jnp.bfloat16)
    grad_pred_mixed = attn_bwd(predict_mixed, predict_attn, predict_lse, grad_pred_attn, PH)
    grad_pred_project = inner_rows(predict_in, grad_pred_mixed)
    grad_pred_in = inner_cols(grad_pred_mixed, predict_project)
    unused, norm_pullback = jax.vjp(layer_norm, start_rows, pred_prenorm_wide)
    grad_start_norm, grad_pred_prenorm = norm_pullback(grad_pred_in)
    grad_start = (grad_branch + grad_start_norm).reshape(clips_here, clip_len, PD)
    grad_mask = jnp.sum(jnp.where(visible[:, :, None], 0.0, grad_start), axis=(0, 1))
    grad_entry_rows = jnp.take_along_axis(grad_start, visible_pos[:, :, None], axis=1)
    grad_entry_rows = jnp.where(slot_live[:, :, None], grad_entry_rows, 0.0)
    grad_entry_rows = grad_entry_rows.reshape(clips_here * VMOST, PD).astype(jnp.bfloat16)
    grad_entry = inner_rows(context_out, grad_entry_rows)
    grad_context_out = inner_cols(grad_entry_rows, predict_entry).astype(jnp.bfloat16)
    back_project, back_outward = ctx_project_full, ctx_outward_full
    back_expand, back_shrink = ctx_expand_full, ctx_shrink_full
    back_prenorm_wide, back_midnorm_wide = ctx_prenorm_wide, ctx_midnorm_wide
    grad_mid, ffn_grads = feed_forward_back(
        grad_context_out, ffn_saved, back_midnorm_wide, back_expand, back_shrink
    )
    grad_ctx_outward = inner_rows(context_attn, grad_mid)
    grad_ctx_attn = inner_cols(grad_mid, back_outward).astype(jnp.bfloat16)
    grad_ctx_mixed = attn_bwd(
        context_mixed, context_attn, context_lse, grad_ctx_attn, H, counts_here
    )
    grad_ctx_project = inner_rows(context_in, grad_ctx_mixed)
    grad_ctx_in = inner_cols(grad_ctx_mixed, back_project)
    unused, norm_pullback = jax.vjp(layer_norm, seen_rows, back_prenorm_wide)
    grad_seen_norm, grad_ctx_prenorm = norm_pullback(grad_ctx_in)
    grad_seen = (grad_mid.astype(jnp.float32) + grad_seen_norm).reshape(
        clips_here, VMOST, model_width
    )
    grad_grid = jnp.take_along_axis(
        grad_seen, order_rank[:, :, None], axis=1
    )
    tokens_grad = jnp.where(visible[:, :, None], grad_grid, 0.0).reshape(
        clips_here * clip_len, model_width
    )
    context_sums, predict_sums = every_grad(
        tuned,
        (
            grad_ctx_prenorm,
            grad_ctx_project,
            grad_ctx_outward,
            ffn_grads[0],
            ffn_grads[1],
            ffn_grads[2],
        ),
        (
            grad_entry,
            grad_mask,
            grad_pred_prenorm,
            grad_pred_project,
            grad_pred_outward,
            grad_pred_midnorm,
            grad_pred_expand,
            grad_pred_shrink,
            grad_endnorm,
            grad_exit,
        ),
    )
    return (
        clip_loss,
        tokens_grad,
        context_sums[0],
        context_sums[1],
        context_sums[2],
        context_sums[3],
        context_sums[4],
        context_sums[5],
        predict_sums[0],
        predict_sums[1],
        predict_sums[2],
        predict_sums[3],
        predict_sums[4],
        predict_sums[5],
        predict_sums[6],
        predict_sums[7],
        predict_sums[8],
        predict_sums[9],
    )


def solution(mesh):
    return jax.shard_map(
        shards,
        mesh=mesh,
        in_specs=(
            P(("tok", "head"), None),
            P("tok"),
            P("tok", None),
            P("tok", None),
            P("tok"),
            P("tok", None),
            P("tok", None),
            P("tok"),
            P("tok", None),
            P("tok", None),
            P("tok"),
            P("tok", None),
            P("tok", None),
            P(),
            P(),
            P(),
            P(),
            P(),
            P(),
            P(),
            P(),
            P(),
            P(),
            P(("tok", "head"), None),
            P(),
        ),
        out_specs=(
            P(("tok", "head")),
            P(("tok", "head"), None),
            P("tok"),
            P("tok", None),
            P("tok", None),
            P("tok"),
            P("tok", None),
            P("tok", None),
            P(),
            P(),
            P(),
            P(),
            P(),
            P(),
            P(),
            P(),
            P(),
            P(),
        ),
        check_vma=False,
    )
```

```python
import functools

import jax
import jax.numpy as jnp
from jax import lax
from jax.experimental import pallas as pl
from jax.experimental.pallas import tpu as pltpu
from jax.sharding import PartitionSpec as P

H = 16
PD = 384
PH = 12
VMOST = 464


EPSILON = 1e-06
HUBER = 0.25


def layer_norm(values, gains):
    center = values - jnp.mean(values, axis=-1, keepdims=True)
    spread = jnp.mean(center * center, axis=-1, keepdims=True)
    return center * lax.rsqrt(spread + EPSILON) * gains


def plain_norm(values):
    center = values - jnp.mean(values, axis=-1, keepdims=True)
    spread = jnp.mean(center * center, axis=-1, keepdims=True)
    return center * lax.rsqrt(spread + EPSILON)


def smooth_error(differ):
    magnitude = jnp.abs(differ)
    return jnp.where(magnitude < HUBER, 0.5 * differ * differ / HUBER, magnitude - 0.5 * HUBER)


def positions(length, breadth, block=32):
    half_width = breadth // 2
    freqs = jnp.exp(-jnp.log(10000.0) * jnp.arange(half_width, dtype=jnp.float32) / half_width)
    coarse = jnp.arange(0, length, block, dtype=jnp.float32)[:, None, None] * freqs
    fine = jnp.arange(block, dtype=jnp.float32)[None, :, None] * freqs
    sines = lax.optimization_barrier((jnp.sin(coarse), jnp.cos(coarse), jnp.sin(fine), jnp.cos(fine)))
    sin_far, cos_far, sin_near, cos_near = sines
    table = jnp.concatenate(
        [sin_far * cos_near + cos_far * sin_near, cos_far * cos_near - sin_far * sin_near], axis=2
    )
    return table.reshape(-1, breadth)[:length]


def product(former, latter):
    return jnp.dot(former, latter, preferred_element_type=jnp.float32)


def inner_rows(former, latter):
    return lax.dot_general(
        former, latter, (((0,), (0,)), ((), ())), preferred_element_type=jnp.float32
    )


def inner_cols(former, latter):
    return lax.dot_general(
        former, latter, (((1,), (1,)), ((), ())), preferred_element_type=jnp.float32
    )


BF=jnp.bfloat16; F32=jnp.float32
LOG2E=1.4426950408889634
NT=(((1,),(1,)),((),())); NN=(((1,),(0,)),((),()))
def dot(a,b,dims=NN): return lax.dot_general(a,b,dims,preferred_element_type=F32)
def chunks(n,step):
    return [(i,min(step,n-i)) for i in range(0,n,step)]
def lane_mask(rows,h,e):
    lane=lax.broadcasted_iota(jnp.int32,(rows,128),1)
    return (lane>=h*e)&(lane<(h+1)*e)
def head_rows(values,h,e):
    return jnp.where(lane_mask(values.shape[0],h,e),values,jnp.zeros_like(values))

def attend_group(q_all,k,v,e,live,step):
    L=q_all.shape[0]; per=128//e; c=e**-0.5*LOG2E
    vt=v.T
    results=[]; sums=[]
    for (s0,n) in chunks(L,step):
        outs=[]; lses=[]
        for h in range(per):
            q=head_rows(q_all[s0:s0+n,:],h,e)
            st=dot(k,q,NT)
            if live is not None: st=jnp.where(live,st,-1e30)
            m=jnp.max(st,axis=0,keepdims=True)
            p=jnp.exp2((st-m)*c)
            l=jnp.sum(p,axis=0,keepdims=True)
            outs.append(dot(vt[h*e:(h+1)*e,:],p.astype(BF))*(1.0/l))
            lses.append(m*c+jnp.log2(l))
        results.append(jnp.concatenate(outs,axis=0).T.astype(BF))
        sums.append(jnp.concatenate(lses,axis=0))
    if len(results)==1: return results[0],sums[0]
    return jnp.concatenate(results,axis=0),jnp.concatenate(sums,axis=1)

def fwd_kernel(e,step,masked,want_lse,*refs):
    refs=list(refs)
    count=refs.pop(0) if masked else None
    q_ref,k_ref,v_ref,o_ref=refs[:4]
    L=q_ref.shape[0]
    live=lax.broadcasted_iota(jnp.int32,(L,1),0)<count[0] if masked else None
    o_ref[...],lse=attend_group(q_ref[...],k_ref[...],v_ref[...],e,live,step)
    if want_lse: refs[4][0]=lse

def attn_fwd(mixed,heads,count=None,step=1280,want_lse=True):
    L,w3=mixed.shape; Dm=w3//3; e=Dm//heads; G=Dm//128; per=128//e
    masked=count is not None
    spec=lambda off: pl.BlockSpec((L,128),lambda g,*_:(0,off+g))
    out_shape=[jax.ShapeDtypeStruct((L,Dm),BF)]; out_specs=[pl.BlockSpec((L,128),lambda g,*_:(0,g))]
    if want_lse:
        out_shape.append(jax.ShapeDtypeStruct((G,per,L),F32)); out_specs.append(pl.BlockSpec((1,per,L),lambda g,*_:(g,0,0)))
    gs=pltpu.PrefetchScalarGridSpec(num_scalar_prefetch=1 if masked else 0,grid=(G,),in_specs=[spec(0),spec(G),spec(2*G)],out_specs=out_specs)
    flops=4*heads*L*L*e
    f=pl.pallas_call(functools.partial(fwd_kernel,e,step,masked,want_lse),grid_spec=gs,out_shape=out_shape,
        compiler_params=pltpu.CompilerParams(vmem_limit_bytes=56<<20),
        cost_estimate=pl.CostEstimate(flops=flops,bytes_accessed=L*Dm*8,transcendentals=heads*L*L),name="attn_fwd")
    return f(*((count,) if masked else ()),mixed,mixed,mixed)

def bwd_kernel(e,step,masked,*refs):
    refs=list(refs)
    count=refs.pop(0) if masked else None
    q_ref,k_ref,v_ref,o_ref,do_ref,lse_ref,g_ref,dk_ref,dv_ref=refs
    L=q_ref.shape[0]; per=128//e; c=e**-0.5*LOG2E; f=e**-0.5
    g=pl.program_id(0); G=pl.num_programs(0)
    k=k_ref[...]; v=v_ref[...]
    kt=k.T
    live=None
    if masked:
        live=lax.broadcasted_iota(jnp.int32,(L,1),0)<count[0]
    dk_ref[...]=jnp.zeros_like(dk_ref); dv_ref[...]=jnp.zeros_like(dv_ref)
    cols=lambda part: pl.ds(pl.multiple_of((part*G+g)*128,128),128)
    for (s0,n) in chunks(L,step):
        do_all=do_ref[s0:s0+n,:]; q_all=q_ref[s0:s0+n,:]
        prod=(do_all.astype(F32)*o_ref[s0:s0+n,:].astype(F32)).T
        dqs=[]
        for h in range(per):
            q=head_rows(q_all,h,e); do=head_rows(do_all,h,e)
            delta=jnp.sum(prod[h*e:(h+1)*e,:],axis=0,keepdims=True)
            st=dot(k,q,NT)
            p=jnp.exp2(st*c-lse_ref[0,h:h+1,s0:s0+n])
            if masked: p=jnp.where(live,p,0.0)
            dp=dot(v,do,NT)
            ds=(p*(dp-delta)).astype(BF)
            dv_ref[...]+=dot(p.astype(BF),do)
            dk_ref[...]+=dot(ds,q)
            dqs.append(dot(kt[h*e:(h+1)*e,:],ds))
        g_ref[s0:s0+n,cols(0)]=(jnp.concatenate(dqs,axis=0)*f).T.astype(BF)
    g_ref[:,cols(1)]=(dk_ref[...]*f).astype(BF)
    g_ref[:,cols(2)]=dv_ref[...].astype(BF)

def attn_bwd(mixed,o,lse,do,heads,count=None,step=256):
    L,w3=mixed.shape; Dm=w3//3; e=Dm//heads; G=Dm//128; per=128//e
    masked=count is not None
    spec=lambda off: pl.BlockSpec((L,128),lambda g,*_:(0,off+g))
    gs=pltpu.PrefetchScalarGridSpec(num_scalar_prefetch=1 if masked else 0,grid=(G,),
        in_specs=[spec(0),spec(G),spec(2*G),spec(0),spec(0),pl.BlockSpec((1,per,L),lambda g,*_:(g,0,0))],
        out_specs=pl.BlockSpec((L,w3),lambda g,*_:(0,0)),
        scratch_shapes=[pltpu.VMEM((L,128),F32)]*2)
    return pl.pallas_call(functools.partial(bwd_kernel,e,step,masked),grid_spec=gs,out_shape=jax.ShapeDtypeStruct((L,w3),BF),
        compiler_params=pltpu.CompilerParams(vmem_limit_bytes=56<<20),
        cost_estimate=pl.CostEstimate(flops=10*heads*L*L*e,bytes_accessed=L*Dm*16,transcendentals=heads*L*L),name="attn_bwd")(*((count,) if masked else ()),mixed,mixed,mixed,o,do,lse)


MESH = pl.DeviceIdType.MESH
ANY = pl.BlockSpec(memory_space=pl.ANY)

def place():
    tok=lax.axis_index("tok"); head=lax.axis_index("head")
    return tok//2, tok%2, head//2, head%2

def peer(z,y,x,c): return (z*2+y, x*2+c)

def greet(barrier_peers):
    barrier=pltpu.get_barrier_semaphore()
    for p in barrier_peers:
        pl.semaphore_signal(barrier,inc=1,device_id=p,device_id_type=MESH)
    pl.semaphore_wait(barrier,len(barrier_peers))

def gather_steps(shard, full, own, cut, quarter, local, send, recv):
    z,y,x,c=place()
    xs = x if quarter else slice(None)
    rows, cols = cut
    def rcopy(i,src,dst,dev):
        return pltpu.make_async_remote_copy(src_ref=src,dst_ref=dst,send_sem=send.at[i],recv_sem=recv.at[i],device_id=dev,device_id_type=MESH)
    mine=shard.at[xs,c,rows,cols]
    def load(): return pltpu.make_async_copy(mine,own,local.at[0])
    def put(): return pltpu.make_async_copy(own,full.at[z,y,xs,c,rows,cols],local.at[1])
    def zc(k,out):
        dst=full.at[z,y,xs,c,rows,cols] if out else full.at[(z+4-k)%4,y,xs,c,rows,cols]
        return rcopy(k-1,mine,dst,peer((z+k)%4,y,x,c))
    def yc(out):
        yy=y if out else 1-y
        return rcopy(3,full.at[:,y,xs,c,rows,cols],full.at[:,yy,xs,c,rows,cols],peer(z,1-y,x,c))
    def xc(out):
        xx=x if out else 1-x
        return rcopy(4,full.at[:,:,x,c,rows,cols],full.at[:,:,xx,c,rows,cols],peer(z,y,1-x,c))
    def cc(out):
        cz=c if out else 1-c
        return rcopy(5,full.at[:,:,:,c,rows,cols],full.at[:,:,:,cz,rows,cols],peer(z,y,x,1-c))
    def s0():
        load().start()
        for k in (2,1,3): zc(k,True).start()
    def s1():
        load().wait(); put().start()
        for k in (1,2,3): zc(k,False).wait_recv()
        put().wait()
        yc(True).start()
    def s2():
        yc(False).wait_recv()
        if quarter: xc(True).start()
        else: cc(True).start()
    def s3():
        if quarter:
            xc(False).wait_recv(); cc(True).start()
    def s4():
        cc(False).wait_recv()
        for k in (1,2,3): zc(k,True).wait_send()
        yc(True).wait_send()
        if quarter: xc(True).wait_send()
        cc(True).wait_send()
    return [s0,s1,s2,s3,s4]

def gains_steps(src,out,send,recv):
    z,y,x,c=place()
    def cp(k,outgoing):
        dz,dy=k//2,k%2
        t=z*2+y
        pz=(z+dz)%4; py=(y+dy)%2
        sz=(z+4-dz)%4; sy=(y+2-dy)%2
        dst=out.at[t] if outgoing else out.at[sz*2+sy]
        return pltpu.make_async_remote_copy(src_ref=src,dst_ref=dst,send_sem=send.at[k-1],recv_sem=recv.at[k-1],device_id=peer(pz,py,x,c),device_id_type=MESH)
    def start():
        for k in range(1,8): cp(k,True).start()
    def finish():
        for k in range(1,8): cp(k,False).wait_recv()
        for k in range(1,8): cp(k,True).wait_send()
    return start,finish

def everyone_on_tok():
    z,y,x,c=place()
    peers=[peer((z+k//2)%4,(y+k%2)%2,x,c) for k in range(1,8)]
    return peers+[peer(z,y,1-x,c),peer(z,y,x,1-c)]

def together(members):
    def stage(s):
        def run():
            for m in members: m[s]()
        return run
    return [stage(s) for s in range(len(members[0]))]

def interleave(chunks):
    n=len(chunks); depth=len(chunks[0])
    order=[]
    for t in range(n+depth-1):
        for s in range(depth):
            i=t-s
            if 0<=i<n: order.append(chunks[i][s])
    return order

def by_turn(chunks):
    turns=[[] for _ in range(len(chunks)+len(chunks[0])-1)]
    for i,chunk in enumerate(chunks):
        for s,stage in enumerate(chunk): turns[i+s].append((s,stage))
    return [[stage for _,stage in sorted(t,key=lambda p:-p[0])] for t in turns]

def scaled_norm(values,gain_blocks,row,out_ref):
    normed=plain_norm(values.astype(F32))
    for t in range(gain_blocks.shape[0]):
        cols=slice(t*128,(t+1)*128)
        out_ref[:,cols]=(normed[:,cols]*gain_blocks[t,row:row+1,:].astype(F32)).astype(BF)

def ag_kernel(plan,n,heads,*refs):
    shards=refs[:n]; gain,tok_ref,seen_ref,live_ref=refs[n:n+4]
    fulls=refs[n+4:2*n+4]; gout,tout,cin,cmixed,cattn,clse=refs[2*n+4:2*n+10]
    rest=refs[2*n+10:]
    k=len(plan)
    owns=rest[:k]; gown,local,send,recv,gsend,grecv,glocal,gv,tin,tattn,total,pw,ow,ew,sw,wsem=rest[k:]
    z,y,x,c=place()
    turn=pl.program_id(0)
    steps=[]
    for i,(w,r0,rn,c0,cn,quarter) in enumerate(plan):
        steps.append(gather_steps(shards[w],fulls[w],owns[i],(pl.ds(r0,rn),pl.ds(c0,cn)),quarter,local.at[i],send.at[i],recv.at[i]))
    groups={}
    for st,entry in zip(steps,plan): groups.setdefault(entry[:3],[]).append(st)
    turns=by_turn([together(m) for m in groups.values()])
    done={w:i+len(steps[0])-1 for i,(w,_,_) in enumerate(groups)}
    gs,gf=gains_steps(gain,gout,gsend,grecv)
    width=tok_ref.shape[1]; G=width//128; e=width//heads
    first=done[0]+1; outward=first+G//2; dense=outward+1; end=len(turns)-1
    blocks,block_width=2,ew.shape[-1]; finish=dense+8//blocks
    other=end+1-G//2
    assert done[1]<outward and max(done[2],done[3])<dense and outward<done[4]+1<=other and finish<end
    take=lambda w,dst,i: pltpu.make_async_copy(fulls[w],dst,wsem.at[i])
    def take_block(j):
        b=(turn-dense)*blocks+j
        cols=pl.ds(pl.multiple_of(b*block_width,128),block_width)
        return (pltpu.make_async_copy(fulls[2].at[:,:,:,:,:,cols],ew.at[j],wsem.at[2+2*j]),
                pltpu.make_async_copy(fulls[3].at[b//2,b%2],sw.at[j],wsem.at[3+2*j]))
    @pl.when((turn>=dense)&(turn<finish))
    def _():
        for j in range(blocks):
            for copy in take_block(j): copy.start()
    for t,fs in enumerate(turns):
        @pl.when(turn==t)
        def _(t=t,fs=fs):
            if t==0: greet(everyone_on_tok())
            if t==first: take(0,pw,0).start()
            if t==outward: take(1,ow,1).start()
            if t==done[4]+1: take(4,pw,0).start()
            for f in fs: f()
            if t==0:
                gs()
                g0=pltpu.make_async_copy(gain,gown,glocal.at[0]); g0.start(); g0.wait()
                pltpu.make_async_copy(gown,gout.at[z*2+y],glocal.at[1]).start()
            if t==2:
                pltpu.make_async_copy(gown,gout.at[z*2+y],glocal.at[1]).wait()
                gf()
                g2=pltpu.make_async_copy(gout,gv,glocal.at[2]); g2.start(); g2.wait()
            if t==3: scaled_norm(tok_ref[...],gv,0,tin)
            if t==4: scaled_norm(seen_ref[...],gv,2,cin)
            if t==first: take(0,pw,0).wait()
            if t==outward:
                take(1,ow,1).wait()
                total[...]=tok_ref[...].astype(F32)+dot(tattn[...],ow[...].reshape(width,width))
                scaled_norm(total[...],gv,1,tin)
            if t==done[4]+1: take(4,pw,0).wait()
            if t==finish:
                total[...]=plain_norm(total[...])
                pltpu.make_async_copy(total,tout,wsem.at[1]).start()
            if t==end: pltpu.make_async_copy(total,tout,wsem.at[1]).wait()
    def pair(rows,g):
        columns=lambda part: pl.ds(pl.multiple_of((part*G+g)*128,128),256)
        return [dot(rows,pw[:,:,:,:,:,columns(part)].reshape(width,256)).astype(BF) for part in range(3)]
    @pl.when((turn>=first)&(turn<outward))
    def _():
        g=(turn-first)*2
        parts=pair(tin[...],g)
        for j in range(2):
            o,_=attend_group(*[p[:,j*128:(j+1)*128] for p in parts],e,None,1280)
            tattn[:,pl.ds(pl.multiple_of((g+j)*128,128),128)]=o
    @pl.when(turn>=other)
    def _():
        g=(turn-other)*2
        live=live_ref[...]!=0
        parts=pair(cin[...],g)
        for part in range(3):
            cmixed[:,pl.ds(pl.multiple_of((part*G+g)*128,128),256)]=parts[part]
        for j in range(2):
            o,lse=attend_group(*[p[:,j*128:(j+1)*128] for p in parts],e,live,1280)
            cattn[:,pl.ds(pl.multiple_of((g+j)*128,128),128)]=o
            clse[g+j]=lse
    @pl.when((turn>=dense)&(turn<finish))
    def _():
        for j in range(blocks):
            for copy in take_block(j): copy.wait()
            active=jax.nn.gelu(dot(tin[...],ew[j].reshape(width,block_width))).astype(BF)
            total[...]+=dot(active,sw[j].reshape(block_width,width))

def gather_and_attend(shards,gains,tokens,seen,live,heads,plan,cid):
    n=len(shards); k=len(plan)
    views=[s.reshape(2,2,s.shape[0]//4,s.shape[1]) for s in shards]
    outs=[jax.ShapeDtypeStruct((4,2,2,2,s.shape[0]//4,s.shape[1]),s.dtype) for s in shards]
    outs.append(jax.ShapeDtypeStruct((8,)+gains.shape,gains.dtype))
    (L,width),slots=tokens.shape,seen.shape[0]
    G=width//128
    extra=[((L,width),F32),((slots,width),BF),((slots,3*width),BF),((slots,width),BF),((G,heads//G,slots),F32)]
    outs+=[jax.ShapeDtypeStruct(s,d) for s,d in extra]
    whole=lambda s: pl.BlockSpec(s,lambda t: (0,)*len(s))
    owns=[pltpu.VMEM(((rn,cn) if q else (2,rn,cn)),BF) for (w,r0,rn,c0,cn,q) in plan]
    S=pltpu.SemaphoreType.DMA
    turns=len({entry[:3] for entry in plan})+4
    scratch=owns+[pltpu.VMEM(gains.shape,BF),S((k,2)),S((k,6)),S((k,6)),S((7,)),S((7,)),S((3,)),
        pltpu.VMEM((8,)+gains.shape,BF),pltpu.VMEM((L,width),BF),pltpu.VMEM((L,width),BF),pltpu.VMEM((L,width),F32),
        pltpu.VMEM(outs[0].shape,BF),pltpu.VMEM(outs[1].shape,BF),
        pltpu.VMEM((2,)+outs[2].shape[:-1]+(outs[2].shape[-1]//8,),BF),pltpu.VMEM((2,)+outs[3].shape[2:],BF),S((6,))]
    res=pl.pallas_call(functools.partial(ag_kernel,plan,n,heads),grid=(turns,),out_shape=outs,
        in_specs=[ANY]*(n+1)+[whole(tokens.shape),whole(seen.shape),whole(live.shape)],
        out_specs=[ANY]*(n+2)+[whole(s) for s,_ in extra[1:]],scratch_shapes=scratch,
        compiler_params=pltpu.CompilerParams(collective_id=cid,has_side_effects=True,vmem_limit_bytes=60<<20),name="gather_and_attend")(*views,gains,tokens,seen,live)
    return [o.reshape(8*s.shape[0],s.shape[1]) for o,s in zip(res[:n],shards)],res[n],res[n+1:]

def reduce_steps(grad, out, rn, rows, bufs, order, everywhere, local, send, recv):
    z,y,x,c=place()
    M,C,A,B,Z,T=bufs
    def rcopy(i,src,dst,dev):
        return pltpu.make_async_remote_copy(src_ref=src,dst_ref=dst,send_sem=send.at[i],recv_sem=recv.at[i],device_id=dev,device_id_type=MESH)
    xfirst=order=="xy"
    side={"x":peer(z,y,1-x,c),"y":peer(z,1-y,x,c)}
    first,second=order
    load=lambda: pltpu.make_async_copy(grad.at[:,:,:,c,rows],M,local.at[0])
    cc=lambda: rcopy(0,grad.at[:,:,:,1-c,rows],C,side_c)
    side_c=peer(z,y,x,1-c)
    ac=lambda: rcopy(1,M.at[:,:,1-x] if xfirst else M.at[:,1-y],A,side[first])
    bc=lambda: rcopy(2,M.at[:,1-y,x] if xfirst else M.at[:,y,1-x],B,side[second])
    zc=lambda k: rcopy(2+k,M.at[(z+k)%4,y,x],Z.at[k-1],peer((z+k)%4,y,x,c))
    def add(target,source):
        target[...]=(target[...].astype(F32)+source[...].astype(F32)).astype(BF)
    def s0():
        cc().start(); load().start()
    def s1():
        load().wait(); cc().wait_recv()
        @pl.loop(0,16)
        def _(i):
            at=(i//4,(i//2)%2,i%2)
            add(M.at[at],C.at[at])
        ac().start()
    def s2():
        ac().wait_recv()
        @pl.loop(0,8)
        def _(i):
            if xfirst: add(M.at[i//2,i%2,x],A.at[i//2,i%2])
            else: add(M.at[i//2,y,i%2],A.at[i//2,i%2])
        bc().start()
    def s3():
        bc().wait_recv()
        @pl.loop(0,4)
        def _(i):
            add(M.at[i,y,x],B.at[i])
        for k in (2,1,3): zc(k).start()
    if everywhere:
        home=out.at[z,y,x,c,rows]
        spread=[]
        for k in (1,2,3):
            spread.append((5+k,lambda o,k=k:(T,out.at[z,y,x,c,rows] if o else out.at[(z+4-k)%4,y,x,c,rows],peer((z+k)%4,y,x,c))))
        sy=(9,lambda o:(out.at[:,y,x,c,rows],out.at[:,y if o else 1-y,x,c,rows],side["y"]))
        sx=(10,lambda o:(out.at[:,:,x,c,rows],out.at[:,:,x if o else 1-x,c,rows],side["x"]))
        if xfirst: stages=[spread,[sy],[sx]]
        else:
            sx=(9,lambda o:(out.at[:,y,x,c,rows],out.at[:,y,x if o else 1-x,c,rows],side["x"]))
            sy=(10,lambda o:(out.at[:,y,:,c,rows],out.at[:,y if o else 1-y,:,c,rows],side["y"]))
            stages=[spread,[sx],[sy]]
        stages.append([(11,lambda o:(out.at[:,:,:,c,rows],out.at[:,:,:,c if o else 1-c,rows],side_c))])
    else:
        home=out.at[x,c,rows]
        stages=[[(6,lambda o:(T,out.at[x if o else 1-x,c,rows],side["x"]))],[(7,lambda o:(out.at[:,c,rows],out.at[:,c if o else 1-c,rows],side_c))]]
    def run(entry,o):
        i,f=entry; src,dst,dev=f(o); return rcopy(i,src,dst,dev)
    put=lambda: pltpu.make_async_copy(T,home,local.at[1])
    def s4():
        for k in (1,2,3): zc(k).wait_recv()
        T[...]=(M[z,y,x].astype(F32)+Z[0].astype(F32)+Z[1].astype(F32)+Z[2].astype(F32)).astype(BF)
        put().start()
        for e in stages[0]: run(e,True).start()
    def later(n):
        def s():
            if n==1: put().wait()
            for e in stages[n-1]: run(e,False).wait_recv()
            for e in stages[n]: run(e,True).start()
        return s
    def last():
        for e in stages[-1]: run(e,False).wait_recv()
        cc().wait_send(); ac().wait_send(); bc().wait_send()
        for k in (1,2,3): zc(k).wait_send()
        for st in stages:
            for e in st: run(e,True).wait_send()
    mids=[later(n) for n in range(1,len(stages))]
    if not everywhere: mids=mids+[lambda:None]*2
    return [s0,s1,s2,s3,s4]+mids+[last]

def vector_steps(src,out,bufs,local,send,recv):
    z,y,x,c=place()
    V,R=bufs
    dev=[peer(z,y,x,1-c),peer(z,y,1-x,c),peer(z,1-y,x,c)]+[peer((z+k)%4,y,x,c) for k in (1,2,3)]
    def rc(i): return pltpu.make_async_remote_copy(src_ref=V.at[min(i,3)],dst_ref=R.at[i],send_sem=send.at[i],recv_sem=recv.at[i],device_id=dev[i],device_id_type=MESH)
    load=lambda: pltpu.make_async_copy(src,V.at[0],local.at[0])
    def s0():
        load().start(); load().wait(); rc(0).start()
    def mid(n):
        def s():
            rc(n-1).wait_recv()
            V[n]=V[n-1]+R[n-1]
            if n<3: rc(n).start()
            else:
                for i in (3,4,5): rc(i).start()
        return s
    def fin():
        for i in (3,4,5): rc(i).wait_recv()
        V[4]=V[3]+R[3]+R[4]+R[5]
        cp=pltpu.make_async_copy(V.at[4],out,local.at[1]); cp.start(); cp.wait()
        for i in range(6): rc(i).wait_send()
    nothing=lambda:None
    return [s0,mid(1),mid(2),mid(3),fin,nothing,nothing,nothing,nothing]

def rs_kernel(plan,n,*refs):
    grads=refs[:n]; vec=refs[n]; outs=refs[n+1:2*n+1]; vout=refs[2*n+1]; rest=refs[2*n+2:]
    k=len(plan)
    bufs=[rest[6*i:6*i+6] for i in range(k)]
    V,R,local,send,recv,vlocal,vsend,vrecv=rest[6*k:]
    z,y,x,c=place()
    greet([peer((z+j)%4,y,x,c) for j in (1,2,3)]+[peer(z,1-y,x,c),peer(z,y,1-x,c),peer(z,y,x,1-c)])
    steps=[reduce_steps(grads[w],outs[w],rn,pl.ds(r0,rn),bufs[i],order,ev,local.at[i],send.at[i],recv.at[i]) for i,(w,r0,rn,order,ev,_) in enumerate(plan)]
    steps.append(vector_steps(vec,vout,(V,R),vlocal,vsend,vrecv))
    groups={}
    for st,entry in zip(steps,plan): groups.setdefault(entry[5],[]).append(st)
    groups[plan[0][5]].append(steps[-1])
    groups=[together(m) for m in groups.values()]
    for st in groups: st[0]()
    for f in interleave([st[1:] for st in groups]): f()

def reduce_grads(grads, vec, plan, cid):
    n=len(grads)
    every={w:ev for w,_,_,_,ev,_ in plan}
    views=[g.reshape(4,2,2,2,g.shape[0]//32,g.shape[1]) for g in grads]
    outs=[jax.ShapeDtypeStruct(v.shape if every[w] else v.shape[2:],BF) for w,v in enumerate(views)]
    outs.append(jax.ShapeDtypeStruct(vec.shape,F32))
    scratch=[]
    for (w,r0,rn,order,ev,_) in plan:
        N=grads[w].shape[1]
        scratch+=[pltpu.VMEM((4,2,2,rn,N),BF),pltpu.VMEM((4,2,2,rn,N),BF),pltpu.VMEM((4,2,rn,N),BF),pltpu.VMEM((4,rn,N),BF),pltpu.VMEM((3,rn,N),BF),pltpu.VMEM((rn,N),BF)]
    k=len(plan)
    S=pltpu.SemaphoreType.DMA
    scratch+=[pltpu.VMEM((5,)+vec.shape,F32),pltpu.VMEM((6,)+vec.shape,F32),S((k,2)),S((k,12)),S((k,12)),S((2,)),S((6,)),S((6,))]
    res=pl.pallas_call(functools.partial(rs_kernel,plan,n),out_shape=outs,in_specs=[ANY]*(n+1),out_specs=[ANY]*(n+1),scratch_shapes=scratch,
        compiler_params=pltpu.CompilerParams(collective_id=cid,has_side_effects=True,vmem_limit_bytes=60<<20),name="reduce_grads")(*views,vec)
    flat=[]
    for w,r in enumerate(res[:n]):
        rows=grads[w].shape[0]
        flat.append(r.reshape(rows if every[w] else rows//8,grads[w].shape[1]))
    return flat,res[n]


def gather_plan(shards):
    plan = []
    for w in (0, 1, 2, 3, 4, 6, 7, 5):
        rows, wide = shards[w].shape[0] // 4, shards[w].shape[1]
        rest = (wide // 3 + 64) // 128 * 128
        parts = 1 if wide == shards[w].shape[0] * 8 else 2
        for part in range(parts):
            r0, rn = part * rows // parts, rows // parts
            plan.append((w, r0, rn, 0, wide - rest, True))
            plan.append((w, r0, rn, wide - rest, rest, False))
    return plan


def every_weight(tuned, gains, shards, tokens, seen, live, heads):
    if tuned:
        packed = jnp.pad(jnp.stack(gains), ((0, 12), (0, 0)))
        full, norms, attended = gather_and_attend(
            list(shards), packed, tokens, seen, live, heads, gather_plan(shards), 1
        )
        return tuple(norms[:, i, :].reshape(-1) for i in range(4)) + tuple(full), attended
    full = tuple(lax.all_gather(v, "tok", axis=0, tiled=True) for v in gains + shards)
    target_in = layer_norm(tokens.astype(F32), full[0].astype(F32)).astype(BF)
    target_attn = attn_fwd(product(target_in, full[4]).astype(BF), heads, want_lse=False)[0]
    target_mid = tokens.astype(F32) + product(target_attn, full[5])
    target_out = target_ffn(target_mid, full[1].astype(F32), full[6], full[7])
    context_in = layer_norm(seen.astype(F32), full[2].astype(F32)).astype(BF)
    context_mixed = product(context_in, full[8]).astype(BF)
    count = jnp.sum(live, axis=0)
    context_attn, context_lse = attn_fwd(context_mixed, heads, count)
    return full, (target_out, context_in, context_mixed, context_attn, context_lse)


def every_grad(tuned, context, predict):
    if not tuned:
        parts = [lax.psum_scatter(v, "tok", scatter_dimension=0, tiled=True) for v in context]
        return (
            tuple(lax.psum(v.astype(jnp.bfloat16), "head").astype(jnp.float32) for v in parts),
            lax.psum(predict, ("tok", "head")),
        )
    entry, mask, prenorm, project, outward, midnorm, expand, shrink, endnorm, leave = predict
    model_width, width = entry.shape
    wide = jnp.concatenate([project, outward, expand, leave], axis=1).astype(BF)
    blocks = wide.shape[1] // model_width
    wide = jnp.concatenate(
        [wide[:, i * model_width : (i + 1) * model_width] for i in range(blocks)], axis=0
    )
    tall = jnp.concatenate([entry, shrink], axis=0).astype(BF)
    small = (mask, prenorm, midnorm, endnorm, context[0], context[3])
    line = jnp.concatenate(small)
    vector = jnp.pad(line, (0, -line.shape[0] % 1024)).reshape(-1, 128)
    grads = [context[1], context[2], context[4], context[5]]
    grads = [v.astype(BF) for v in grads] + [wide, tall]
    piece = [v.shape[0] // 32 for v in grads]
    plan = [(4, 0, piece[4], "yx", True, 4), (5, 0, piece[5], "xy", True, 4)]
    for w in (3, 2, 0, 1):
        parts = 2 if piece[w] >= 64 else 1
        rows = piece[w] // (2 * parts)
        for part in range(parts):
            at, key = 2 * part * rows, (w, part)
            plan += [(w, at, rows, "xy", False, key), (w, at + rows, rows, "yx", False, key)]
    sums, vector = reduce_grads(grads, vector, plan, 2)
    sums = [v.astype(F32) for v in sums]
    line = vector.reshape(-1)
    lines = []
    for v in small:
        lines.append(line[: v.shape[0]])
        line = line[v.shape[0] :]
    share = model_width // lax.axis_size("tok")
    mine = lambda v: lax.dynamic_slice_in_dim(v, lax.axis_index("tok") * share, share)
    wide = jnp.concatenate(
        [sums[4][i * width : (i + 1) * width] for i in range(blocks)], axis=1
    )
    cuts = [0]
    for v in (project, outward, expand, leave):
        cuts.append(cuts[-1] + v.shape[1])
    project, outward, expand, leave = (wide[:, a:b] for a, b in zip(cuts, cuts[1:]))
    return (
        (mine(lines[4]), sums[0], sums[1], mine(lines[5]), sums[2], sums[3]),
        (
            sums[5][:model_width],
            lines[0],
            lines[1],
            project,
            outward,
            lines[2],
            expand,
            sums[5][model_width:],
            lines[3],
            leave,
        ),
    )


def ffn_kernel(mid_ref, gain_ref, expand_ref, shrink_ref, out_ref, normed_ref, sum_ref):
    step = pl.program_id(0)

    @pl.when(step == 0)
    def _():
        normed_ref[...] = layer_norm(mid_ref[...], gain_ref[...]).astype(BF)
        sum_ref[...] = mid_ref[...]

    active = jax.nn.gelu(dot(normed_ref[...], expand_ref[...])).astype(BF)
    sum_ref[...] += dot(active, shrink_ref[...])

    @pl.when(step == pl.num_programs(0) - 1)
    def _():
        out_ref[...] = plain_norm(sum_ref[...])


def target_ffn(mid_rows, gain, expand, shrink, block=1024):
    length, width = mid_rows.shape
    hidden = expand.shape[1]
    whole = pl.BlockSpec((length, width), lambda j: (0, 0))
    return pl.pallas_call(
        ffn_kernel,
        grid=(hidden // block,),
        in_specs=[
            whole,
            pl.BlockSpec((1, width), lambda j: (0, 0)),
            pl.BlockSpec((width, block), lambda j: (0, j)),
            pl.BlockSpec((block, width), lambda j: (j, 0)),
        ],
        out_specs=whole,
        out_shape=jax.ShapeDtypeStruct((length, width), F32),
        scratch_shapes=[pltpu.VMEM((length, width), BF), pltpu.VMEM((length, width), F32)],
        compiler_params=pltpu.CompilerParams(vmem_limit_bytes=60 << 20),
        cost_estimate=pl.CostEstimate(
            flops=4 * length * width * hidden,
            bytes_accessed=8 * length * width + 4 * width * hidden,
            transcendentals=length * hidden,
        ),
        name="target_ffn",
    )(mid_rows, gain.reshape(1, -1), expand, shrink)


def feed_forward(mid_rows, midnorm, expand, shrink):
    mid_wide = mid_rows.astype(jnp.float32)
    normed = layer_norm(mid_wide, midnorm).astype(jnp.bfloat16)
    raised = product(normed, expand)
    active = jax.nn.gelu(raised).astype(jnp.bfloat16)
    output = (mid_wide + product(active, shrink)).astype(jnp.bfloat16)
    return (output, (mid_wide, normed, raised, active))


def feed_forward_back(grad_rows, saved, midnorm, expand, shrink):
    mid_wide, normed, raised, active = saved
    grad_shrink = inner_rows(active, grad_rows)
    grad_active = inner_cols(grad_rows, shrink)
    unused, gelu_pullback = jax.vjp(jax.nn.gelu, raised)
    grad_raised = gelu_pullback(grad_active)[0].astype(jnp.bfloat16)
    grad_expand = inner_rows(normed, grad_raised)
    grad_normed = inner_cols(grad_raised, expand)
    unused, norm_pullback = jax.vjp(layer_norm, mid_wide, midnorm)
    grad_mid, grad_midnorm = norm_pullback(grad_normed)
    grad_total = (grad_rows.astype(jnp.float32) + grad_mid).astype(jnp.bfloat16)
    return (grad_total, (grad_midnorm, grad_expand, grad_shrink))


def shards(
    tokens,
    target_prenorm,
    target_project,
    target_outward,
    target_midnorm,
    target_expand,
    target_shrink,
    context_prenorm,
    context_project,
    context_outward,
    context_midnorm,
    context_expand,
    context_shrink,
    predict_entry,
    mask_token,
    predict_prenorm,
    predict_project,
    predict_outward,
    predict_midnorm,
    predict_expand,
    predict_shrink,
    predict_endnorm,
    predict_exit,
    clip_order,
    visible_count,
):
    clips_here = clip_order.shape[0]
    clip_len = clip_order.shape[1]
    model_width = tokens.shape[1]
    head_devices = lax.axis_size("head")
    lane_index = lax.axis_index("tok")
    head_index = lax.axis_index("head")
    device_index = lane_index * head_devices + head_index
    counts_here = lax.dynamic_slice_in_dim(visible_count, device_index * clips_here, clips_here)
    tuned = lax.axis_size("tok") == 8 and head_devices == 4
    visible_pos = clip_order[:, :VMOST]
    slot_live = jnp.arange(VMOST, dtype=jnp.int32)[None, :] < counts_here[:, None]
    holds = visible_pos[:, :, None] == jnp.arange(clip_len, dtype=jnp.int32)[None, None, :]
    holds = jnp.logical_and(holds, slot_live[:, :, None])
    visible = jnp.any(holds, axis=1)
    slot = jnp.arange(VMOST, dtype=jnp.int32)[None, :, None]
    order_rank = jnp.sum(jnp.where(holds, slot, 0), axis=1)
    token_grid = tokens.reshape(clips_here, clip_len, model_width)
    seen_rows = jnp.einsum(
        "csl,cld->csd", holds.astype(BF), token_grid, preferred_element_type=jnp.float32
    )
    seen_rows = seen_rows.reshape(clips_here * VMOST, model_width)
    seen_low = seen_rows.astype(BF)
    live_column = slot_live.astype(jnp.int32).reshape(-1, 1)
    weights, attended = every_weight(
        tuned,
        (target_prenorm, target_midnorm, context_prenorm, context_midnorm),
        (
            target_project,
            target_outward,
            target_expand,
            target_shrink,
            context_project,
            context_outward,
            context_expand,
            context_shrink,
        ),
        tokens,
        seen_low,
        live_column,
        H,
    )
    target_out, context_in, context_mixed, context_attn, context_lse = attended
    ctx_prenorm_full, ctx_midnorm_full = weights[2:4]
    ctx_project_full, ctx_outward_full, ctx_expand_full, ctx_shrink_full = weights[8:]
    ctx_prenorm_wide = ctx_prenorm_full.astype(jnp.float32)
    ctx_midnorm_wide = ctx_midnorm_full.astype(jnp.float32)
    context_mid = (seen_rows + product(context_attn, ctx_outward_full)).astype(jnp.bfloat16)
    context_out, ffn_saved = feed_forward(
        context_mid, ctx_midnorm_wide, ctx_expand_full, ctx_shrink_full
    )
    entry_rows = product(context_out, predict_entry).reshape(clips_here, VMOST, -1)
    placed = jnp.take_along_axis(entry_rows, order_rank[:, :, None], axis=1)
    start_rows = jnp.where(
        visible[:, :, None], placed, mask_token.astype(jnp.float32)[None, None, :]
    )
    start_rows = (start_rows + positions(clip_len, PD)[None]).reshape(clips_here * clip_len, PD)
    pred_prenorm_wide = predict_prenorm.astype(jnp.float32)
    pred_midnorm_wide = predict_midnorm.astype(jnp.float32)
    pred_endnorm_wide = predict_endnorm.astype(jnp.float32)
    predict_in = layer_norm(start_rows, pred_prenorm_wide).astype(jnp.bfloat16)
    predict_mixed = product(predict_in, predict_project).astype(jnp.bfloat16)
    predict_attn, predict_lse = attn_fwd(predict_mixed, PH)
    branch_rows = start_rows + product(predict_attn, predict_outward)
    predict_normed = layer_norm(branch_rows, pred_midnorm_wide).astype(jnp.bfloat16)
    predict_raised = product(predict_normed, predict_expand)
    predict_active = jax.nn.gelu(predict_raised).astype(jnp.bfloat16)
    final_rows = branch_rows + product(predict_active, predict_shrink)
    final_in = layer_norm(final_rows, pred_endnorm_wide).astype(jnp.bfloat16)
    predicted = product(final_in, predict_exit)
    differ = predicted - target_out
    hidden_rows = jnp.logical_not(visible).reshape(-1)
    row_error = jnp.mean(smooth_error(differ), axis=1)
    clip_sums = jnp.sum(
        jnp.where(hidden_rows, row_error, 0.0).reshape(clips_here, clip_len), axis=1
    )
    clip_loss = clip_sums / (clip_len - counts_here).astype(jnp.float32)
    slope = jnp.clip(differ / HUBER, -1.0, 1.0)
    grad_predicted = (jnp.where(hidden_rows[:, None], slope, 0.0) / model_width).astype(
        jnp.bfloat16
    )
    grad_exit = inner_rows(final_in, grad_predicted)
    grad_final_in = inner_cols(grad_predicted, predict_exit)
    unused, norm_pullback = jax.vjp(layer_norm, final_rows, pred_endnorm_wide)
    grad_final, grad_endnorm = norm_pullback(grad_final_in)
    grad_second = grad_final.astype(jnp.bfloat16)
    grad_pred_shrink = inner_rows(predict_active, grad_second)
    grad_pred_active = inner_cols(grad_second, predict_shrink)
    unused, gelu_pullback = jax.vjp(jax.nn.gelu, predict_raised)
    grad_pred_raised = gelu_pullback(grad_pred_active)[0].astype(jnp.bfloat16)
    grad_pred_expand = inner_rows(predict_normed, grad_pred_raised)
    grad_pred_normed = inner_cols(grad_pred_raised, predict_expand)
    unused, norm_pullback = jax.vjp(layer_norm, branch_rows, pred_midnorm_wide)
    grad_branch_norm, grad_pred_midnorm = norm_pullback(grad_pred_normed)
    grad_branch = grad_final + grad_branch_norm
    grad_first = grad_branch.astype(jnp.bfloat16)
    grad_pred_outward = inner_rows(predict_attn, grad_first)
    grad_pred_attn = inner_cols(grad_first, predict_outward).astype(jnp.bfloat16)
    grad_pred_mixed = attn_bwd(predict_mixed, predict_attn, predict_lse, grad_pred_attn, PH)
    grad_pred_project = inner_rows(predict_in, grad_pred_mixed)
    grad_pred_in = inner_cols(grad_pred_mixed, predict_project)
    unused, norm_pullback = jax.vjp(layer_norm, start_rows, pred_prenorm_wide)
    grad_start_norm, grad_pred_prenorm = norm_pullback(grad_pred_in)
    grad_start = (grad_branch + grad_start_norm).reshape(clips_here, clip_len, PD)
    grad_mask = jnp.sum(jnp.where(visible[:, :, None], 0.0, grad_start), axis=(0, 1))
    grad_entry_rows = jnp.take_along_axis(grad_start, visible_pos[:, :, None], axis=1)
    grad_entry_rows = jnp.where(slot_live[:, :, None], grad_entry_rows, 0.0)
    grad_entry_rows = grad_entry_rows.reshape(clips_here * VMOST, PD).astype(jnp.bfloat16)
    grad_entry = inner_rows(context_out, grad_entry_rows)
    grad_context_out = inner_cols(grad_entry_rows, predict_entry).astype(jnp.bfloat16)
    back_project, back_outward = ctx_project_full, ctx_outward_full
    back_expand, back_shrink = ctx_expand_full, ctx_shrink_full
    back_prenorm_wide, back_midnorm_wide = ctx_prenorm_wide, ctx_midnorm_wide
    grad_mid, ffn_grads = feed_forward_back(
        grad_context_out, ffn_saved, back_midnorm_wide, back_expand, back_shrink
    )
    grad_ctx_outward = inner_rows(context_attn, grad_mid)
    grad_ctx_attn = inner_cols(grad_mid, back_outward).astype(jnp.bfloat16)
    grad_ctx_mixed = attn_bwd(
        context_mixed, context_attn, context_lse, grad_ctx_attn, H, counts_here
    )
    grad_ctx_project = inner_rows(context_in, grad_ctx_mixed)
    grad_ctx_in = inner_cols(grad_ctx_mixed, back_project)
    unused, norm_pullback = jax.vjp(layer_norm, seen_rows, back_prenorm_wide)
    grad_seen_norm, grad_ctx_prenorm = norm_pullback(grad_ctx_in)
    grad_seen = (grad_mid.astype(jnp.float32) + grad_seen_norm).reshape(
        clips_here, VMOST, model_width
    )
    grad_grid = jnp.take_along_axis(
        grad_seen, order_rank[:, :, None], axis=1
    )
    tokens_grad = jnp.where(visible[:, :, None], grad_grid, 0.0).reshape(
        clips_here * clip_len, model_width
    )
    context_sums, predict_sums = every_grad(
        tuned,
        (
            grad_ctx_prenorm,
            grad_ctx_project,
            grad_ctx_outward,
            ffn_grads[0],
            ffn_grads[1],
            ffn_grads[2],
        ),
        (
            grad_entry,
            grad_mask,
            grad_pred_prenorm,
            grad_pred_project,
            grad_pred_outward,
            grad_pred_midnorm,
            grad_pred_expand,
            grad_pred_shrink,
            grad_endnorm,
            grad_exit,
        ),
    )
    return (
        clip_loss,
        tokens_grad,
        context_sums[0],
        context_sums[1],
        context_sums[2],
        context_sums[3],
        context_sums[4],
        context_sums[5],
        predict_sums[0],
        predict_sums[1],
        predict_sums[2],
        predict_sums[3],
        predict_sums[4],
        predict_sums[5],
        predict_sums[6],
        predict_sums[7],
        predict_sums[8],
        predict_sums[9],
    )


def solution(mesh):
    return jax.shard_map(
        shards,
        mesh=mesh,
        in_specs=(
            P(("tok", "head"), None),
            P("tok"),
            P("tok", None),
            P("tok", None),
            P("tok"),
            P("tok", None),
            P("tok", None),
            P("tok"),
            P("tok", None),
            P("tok", None),
            P("tok"),
            P("tok", None),
            P("tok", None),
            P(),
            P(),
            P(),
            P(),
            P(),
            P(),
            P(),
            P(),
            P(),
            P(),
            P(("tok", "head"), None),
            P(),
        ),
        out_specs=(
            P(("tok", "head")),
            P(("tok", "head"), None),
            P("tok"),
            P("tok", None),
            P("tok", None),
            P("tok"),
            P("tok", None),
            P("tok", None),
            P(),
            P(),
            P(),
            P(),
            P(),
            P(),
            P(),
            P(),
            P(),
            P(),
        ),
        check_vma=False,
    )
```
